32 devices in a mesh: src: 2 (over x), space: 16 (over z, y, core).
Axes of the slice: x: 2, y: 2, z: 4, core: 2. Of those that a mesh axis runs over, the one named last changes fastest.
Arguments:
- adjoint_source: float32 [2, 6, 64, 64, 128], P('src', None, 'space'), may hold values from -6 to 6
- forward_field: bfloat16 [2, 6, 64, 64, 128], P('src', None, 'space'), may hold values from -6 to 6
- medium: float32 [2, 64, 64, 128], P(None, 'space'), may hold values from 0.3 to 3
- plane_map: int32 [64, 64], P('space'), may hold values from 0 to 15, as said below
- depth: int32 [2, 64, 64], P('src', 'space'), may hold values from 1 to 128
- rough: float32 [9, 16, 32, 128], P(None, 'space'), may hold values from 0.2 to 1
Outputs:
- gradient: float32 [16, 32, 128], P('space')
The draws below stay inside these ranges and needn't reach their ends.
Inputs may be any that keep to these rules, and one draw needn't show every extreme that they name: plane_map[x, y] differs from x // 4 by at most 2.
All inputs are finite; a program needn't handle non-finite values.
Results may differ from the reference program's by a relative error of at most 0.0003.
Values sent between devices are 32-bit elements; how exact they have to be, the bound alone decides.
No kernel may reach another device: no remote copies, remote signals or barrier semaphores. Data moves between devices by JAX's collectives and lax.ppermute only.
A program may use at most 64 MiB of HBM per device.

```python
import math
import jax
import jax.numpy as jnp
from jax import lax

CX = 4
NY = 64
NZ = 128
SWEEPS = 4
REACH = 2
SOURCES = 2
NX = 64
IX = 16
IY = 32


def draw_plane_map(key, part):
    column = lax.iota(jnp.int32, NY)[None, :]
    base = (lax.iota(jnp.int32, NX) // CX)[:, None]
    jitter = jax.random.randint(key, (NX, NY), -REACH, REACH + 1)
    jitter = jnp.where(column == 0, REACH, jnp.where(column == 1, -REACH, jitter))
    return jnp.clip(base + jitter, 0, IX - 1).astype(jnp.int32)


def touch_ends(entries, own_key, smallest, largest):
    place = [jax.random.randint(jax.random.fold_in(own_key, axis), (), 0, length) for axis, length in enumerate(entries.shape)]
    longest = entries.shape.index(max(entries.shape))
    neighbour = place[:longest] + [(place[longest] + 1) % entries.shape[longest]] + place[longest + 1:]
    return entries.at[tuple(place)].set(smallest).at[tuple(neighbour)].set(largest)


def levels(key, dims, shards, low, largest):
    level = 1.0
    for axis_at, parts in shards:
        steps = jax.random.uniform(jax.random.fold_in(jax.random.fold_in(key, 6), axis_at), (parts,), jnp.float32, low / len(shards), largest / len(shards))
        level = level * jnp.repeat(jnp.exp(steps), dims[axis_at] // parts).reshape((-1,) + (1,) * (len(dims) - 1 - axis_at))
    return level


def centred(stream_key, shape, deviation, most, cuts=(), kind=jnp.bfloat16):
    level = levels(stream_key, shape, cuts, -0.22, 0.18) if cuts else 1.0
    array = jax.random.normal(stream_key, shape, jnp.float32) * deviation * level
    return jnp.minimum(jnp.maximum(array, -most), most).astype(kind)


def setup_inputs(seed: int = 0) -> dict:
    key_list = jax.random.split(jax.random.key(seed), 7)
    return {
        "adjoint_source": centred(key_list[0], (SOURCES, 6, NX, NY, NZ), 1.0, 6.0, ((0, 2), (2, 16)), jnp.float32),
        "forward_field": centred(key_list[1], (SOURCES, 6, NX, NY, NZ), 1.0, 6.0, ((0, 2), (2, 16))),
        "medium": jnp.clip(jnp.exp(math.log(3.0) - 2.3025851 * jax.random.uniform(key_list[2], (2, NX, NY, NZ), jnp.float32) ** levels(key_list[2], (2, NX, NY, NZ), ((1, 16),), -0.2, 0.2)), 0.3, 3.0),
        "plane_map": draw_plane_map(jax.random.fold_in(key_list[6], 71), 0),
        "depth": touch_ends(jax.random.randint(key_list[4], (SOURCES, NX, NY), 1, NZ + 1), jax.random.fold_in(key_list[4], 1), 1, NZ).astype(jnp.int32),
        "rough": jnp.clip(jnp.exp(math.log(1.0) - 1.609438 * jax.random.uniform(key_list[5], (9, IX, IY, NZ), jnp.float32) ** levels(key_list[5], (9, IX, IY, NZ), ((1, 16),), -0.2, 0.2)), 0.2, 1.0),
    }


sweep_steps = (0.323, 1.658, 0.422, 0.752)


def ahead_rows(value):
    return jnp.concatenate([value[..., 1:, :], jnp.zeros_like(value[..., :1, :])], axis=-2)


def ahead_depth(value):
    return jnp.concatenate([value[..., 1:], jnp.zeros_like(value[..., :1])], axis=-1)


def behind_rows(value):
    return jnp.concatenate([jnp.zeros_like(value[..., :1, :]), value[..., :-1, :]], axis=-2) - value


def behind_depth(value):
    return jnp.concatenate([jnp.zeros_like(value[..., :1]), value[..., :-1]], axis=-1) - value


def lower_planes(value):
    return value[..., :-1, :, :]


def upper_planes(value):
    return value[..., 1:, :, :]


def step_planes(value):
    return value[..., 1:, :, :] - value[..., :-1, :, :]


def back_planes(value):
    return value[..., :-1, :, :] - value[..., 1:, :, :]


def curl_curl(padded, inside):
    shape = padded.shape
    planes = shape[-3]
    split = padded.reshape(shape[:-4] + (2, 3) + shape[-3:])
    field_x = split[..., 0, :, :, :]
    field_y = split[..., 1, :, :, :]
    field_z = split[..., 2, :, :, :]
    front = inside[:-1][:, None, None]
    curl_x = (ahead_rows(lower_planes(field_z)) - lower_planes(field_z)) - (ahead_depth(lower_planes(field_y)) - lower_planes(field_y))
    curl_y = (ahead_depth(lower_planes(field_x)) - lower_planes(field_x)) - step_planes(field_z)
    curl_z = step_planes(field_y) - (ahead_rows(lower_planes(field_x)) - lower_planes(field_x))
    curl_x = curl_x * front
    curl_y = curl_y * front
    curl_z = curl_z * front
    out_x = behind_depth(upper_planes(curl_y)) - behind_rows(upper_planes(curl_z))
    out_y = back_planes(curl_z) - behind_depth(upper_planes(curl_x))
    out_z = behind_rows(upper_planes(curl_x)) - back_planes(curl_y)
    stacked = jnp.stack([out_x, out_y, out_z], axis=-4)
    return stacked.reshape(shape[:-4] + (6, planes - 2) + shape[-2:])


def sweep(padded, source, mass_real, mass_imag, inside, weight):
    image = curl_curl(padded, inside)
    center = padded[..., 1:-1, :, :]
    real_part = center[..., 0:3, :, :, :]
    imag_part = center[..., 3:6, :, :, :]
    applied = jnp.concatenate([
        image[..., 0:3, :, :, :] + mass_real * real_part - mass_imag * imag_part,
        image[..., 3:6, :, :, :] + mass_real * imag_part + mass_imag * real_part], axis=-4)
    residual = source - applied
    diagonal = 4.0 + mass_real
    return (center + weight * residual / diagonal) * inside[1:-1][:, None, None]


def edge_parts(adjoint, saved):
    saved_wide = saved.astype(jnp.float32)
    moment = saved_wide[..., 0:3, :, :, :] * adjoint[..., 3:6, :, :, :] + saved_wide[..., 3:6, :, :, :] * adjoint[..., 0:3, :, :, :]
    moment_x = moment[..., 0, :, :, :]
    moment_y = moment[..., 1, :, :, :]
    moment_z = moment[..., 2, :, :, :]
    part_x = moment_x + ahead_depth(moment_x)
    part_x = part_x + ahead_rows(part_x)
    part_y = moment_y + ahead_depth(moment_y)
    part_z = moment_z + ahead_rows(moment_z)
    return part_x, part_y, part_z


def transposed_smooth(summed, rough):
    rows_in = summed.shape[-2]
    depth_in = summed.shape[-1]
    total = jnp.zeros_like(summed)
    for vertical in range(3):
        for lateral in range(3):
            product = rough[vertical * 3 + lateral] * summed
            padded = jnp.pad(product, ((0, 0), (1, 1), (1, 1)))
            total = total + padded[:, 2 - vertical:2 - vertical + rows_in, 2 - lateral:2 - lateral + depth_in]
    return total


def reference(adjoint_source, forward_field, medium, plane_map, depth, rough):
    mass_real = medium[0][None]
    mass_imag = medium[1][None]
    inside = jnp.concatenate([jnp.zeros((1,), jnp.float32), jnp.ones((NX,), jnp.float32), jnp.zeros((1,), jnp.float32)])

    def one_source(group):
        source, saved, level = group
        adjoint = sweep_steps[0] * source / (4.0 + mass_real)
        for sweep_index in range(1, SWEEPS):
            padded = jnp.pad(adjoint, ((0, 0), (1, 1), (0, 0), (0, 0)))
            adjoint = sweep(padded, source, mass_real, mass_imag, inside, sweep_steps[sweep_index])
        part_x, part_y, part_z = edge_parts(adjoint, saved)
        next_y = jnp.concatenate([part_y[1:], jnp.zeros_like(part_y[:1])], axis=0)
        next_z = jnp.concatenate([part_z[1:], jnp.zeros_like(part_z[:1])], axis=0)
        cell = 0.25 * (part_x + (part_y + next_y) + (part_z + next_z))
        keep = (lax.iota(jnp.int32, NZ)[None, None, :] < level[:, :, None]).astype(jnp.float32)
        return cell * keep

    cells = lax.map(one_source, (adjoint_source, forward_field, depth))
    local = jnp.sum(cells, axis=0)
    segment = (plane_map * IY + (lax.iota(jnp.int32, NY) // 2)[None, :]).astype(jnp.int32)
    summed = jax.ops.segment_sum(local.reshape(NX * NY, NZ), segment.reshape(NX * NY), num_segments=IX * IY)
    summed = summed.reshape(IX, IY, NZ)
    return transposed_smooth(summed, rough)
```

```python
import functools

import jax
import jax.numpy as jnp
from jax import lax
from jax.experimental import pallas as pl
from jax.experimental.pallas import tpu as pltpu
from jax.sharding import PartitionSpec as P

SWEEPS = 4
REACH = 2

sweep_steps = (0.323, 1.658, 0.422, 0.752)

PAD = 8
ROWS = 16


def lane_of(width):
    return lax.broadcasted_iota(jnp.int32, (ROWS, width), 1)


def ahead(value, lane):
    width = value.shape[-1]
    return jnp.where(lane == width - 1, 0.0, pltpu.roll(value, width - 1, 1))


def behind(value, lane):
    return jnp.where(lane == 0, 0.0, pltpu.roll(value, 1, 1))


def rows_at(ref, index, row, shift=0):
    return ref[index + (pl.ds(PAD + row + shift, ROWS), slice(None))]


def put(ref, index, row, value):
    ref[index + (pl.ds(PAD + row, ROWS), slice(None))] = value


def clear_pads(ref):
    rows = ref.shape[-2]
    lead = ref.shape[:-2]
    zero = jnp.zeros((PAD, ref.shape[-1]), jnp.float32)
    for flat in range(functools.reduce(lambda a, b: a * b, lead, 1)):
        index = []
        rest = flat
        for size in reversed(lead):
            index.insert(0, rest % size)
            rest //= size
        ref[tuple(index) + (pl.ds(0, PAD), slice(None))] = zero
        ref[tuple(index) + (pl.ds(rows - PAD, PAD), slice(None))] = zero


def chunks(total):
    return range(0, total, ROWS)


def curl(field, ahead_of, row, lane):
    out = []
    for part in (0, 3):
        ex, ey, ez = field(part, 0), field(part + 1, 0), field(part + 2, 0)
        hx = (field(part + 2, 1) - ez) - (ahead(ey, lane) - ey)
        hy = (ahead(ex, lane) - ex) - (ahead_of(part + 2) - ez)
        hz = (ahead_of(part + 1) - ey) - (field(part, 1) - ex)
        out += [hx, hy, hz]
    return out


def curl_back(held, before, lane):
    out = []
    for part in (0, 3):
        hx, hy, hz = held(part, 0), held(part + 1, 0), held(part + 2, 0)
        ox = (behind(hy, lane) - hy) - (held(part + 2, -1) - hz)
        oy = (before(part + 2) - hz) - (behind(hx, lane) - hx)
        oz = (held(part, -1) - hx) - (before(part + 1) - hy)
        out += [ox, oy, oz]
    return out


def updated(center, image, source, real, imag, scale):
    out = []
    for c in range(3):
        applied = image[c] + real * center[c] - imag * center[c + 3]
        out.append(center[c] + scale * (source[c] - applied))
    for c in range(3):
        applied = image[c + 3] + real * center[c + 3] + imag * center[c]
        out.append(center[c + 3] + scale * (source[c + 3] - applied))
    return out


def edge_sums(field, lane):
    out = []
    for part in (0, 3):
        ex = field(part, 0)
        out.append(field(part + 1, 0) + (field(part, 1) - ex))
        out.append(field(part + 2, 0) + (ahead(ex, lane) - ex))
    return out


def sweep_slab(state, held, result, source_ref, medium_ref, scale_ref, weight, low, high, first_scale, planes, rows, lane, wanted=None):
    wanted = range(planes) if wanted is None else wanted
    needed = sorted({i for w in wanted for i in (w - 1, w)})
    for i in needed:
        for row in chunks(rows):
            if i < 0:
                for part in (0, 3):
                    gy, gz = low(part, row)
                    ey, ez = rows_at(state, (part + 1, 0), row), rows_at(state, (part + 2, 0), row)
                    put(held, (part + 1, 0), row, first_scale * (gz - ez))
                    put(held, (part + 2, 0), row, first_scale * (ey - gy))
                continue

            def ahead_of(c, i=i, row=row):
                if i + 1 < planes:
                    return rows_at(state, (c, i + 1), row)
                return high(c, row)

            values = curl(lambda c, s: rows_at(state, (c, i), row, s), ahead_of, row, lane)
            for c in range(6):
                put(held, (c, i + 1), row, values[c])
    for i in wanted:
        for row in chunks(rows):
            image = curl_back(
                lambda c, s: rows_at(held, (c, i + 1), row, s), lambda c: rows_at(held, (c, i), row), lane
            )
            here = pl.ds(row, ROWS)
            new = updated(
                [rows_at(state, (c, i), row) for c in range(6)],
                image,
                [source_ref[0, c, i, here, :] for c in range(6)],
                medium_ref[0, i, here, :],
                medium_ref[1, i, here, :],
                weight * scale_ref[i, here, :],
            )
            for c in range(6):
                put(result, (c, i), row, new[c])


def first_sweep(source_ref, medium_ref, scale_ref, state, planes, rows):
    for i in range(planes):
        for row in chunks(rows):
            here = pl.ds(row, ROWS)
            scale = 1.0 / (4.0 + medium_ref[0, i, here, :])
            scale_ref[i, here, :] = scale
            for c in range(6):
                put(state, (c, i), row, sweep_steps[0] * source_ref[0, c, i, here, :] * scale)


def send_kernel(source_ref, medium_ref, meta_ref, pair_ref, chip_ref, scale_ref, one, two, held):
    planes, rows, width = medium_ref.shape[1:]
    lane = lane_of(width)
    index = lax.axis_index("space")
    odd = lax.rem(index, 2) == 1
    first_scale = jnp.where(index == 0, 0.0, 1.0)
    for ref in (one, two, held):
        clear_pads(ref)
    first_sweep(source_ref, medium_ref, scale_ref, one, planes, rows)

    def emit(slot, row, below, above):
        here = pl.ds(slot * rows + row, ROWS)
        pair_ref[here, :] = jnp.where(odd, below, above)
        chip_ref[here, :] = jnp.where(odd, above, below)

    def emit_level(level, state):
        for row in chunks(rows):
            sums = edge_sums(lambda c, s: rows_at(state, (c, planes - 1), row, s), lane)
            bottom = [rows_at(state, (c, 0), row) for c in (1, 2, 4, 5)]
            for k in range(4):
                emit(4 * level + k, row, bottom[k], sums[k])

    def zero(c, row):
        return 0.0

    def zeros(part, row):
        return 0.0, 0.0

    emit_level(0, one)
    for row in chunks(rows):
        here = pl.ds(row, ROWS)
        for k in range(2):
            emit(12 + k, row, medium_ref[k, 0, here, :], medium_ref[k, planes - 1, here, :])
    meta = pl.ds(14 * rows, 8)
    pair_ref[meta, :] = meta_ref[...]
    chip_ref[meta, :] = meta_ref[...]
    sweep_slab(one, held, two, source_ref, medium_ref, scale_ref, sweep_steps[1], zeros, zero, first_scale, planes, rows, lane)
    emit_level(1, two)
    sweep_slab(
        two, held, one, source_ref, medium_ref, scale_ref, sweep_steps[2], zeros, zero, first_scale, planes, rows, lane,
        wanted=sorted({0, planes - 1}),
    )
    emit_level(2, one)


def window_kernel(
    source_ref, medium_ref, saved_ref, keep_ref, offset_ref, edge_ref, pair_ref, chip_ref,
    send_ref, stay_ref, scale_ref, one, two, held, delta_low, delta_high, delta_two, window, moment,
):
    planes, rows, width = medium_ref.shape[1:]
    lane = lane_of(width)
    index = lax.axis_index("space")
    odd = lax.rem(index, 2) == 1
    first_scale = jnp.where(index == 0, 0.0, 1.0)
    last_scale = jnp.where(index == lax.axis_size("space") - 1, 0.0, 1.0)
    for ref in (one, two, held, delta_low, delta_high, moment):
        clear_pads(ref)
    first_sweep(source_ref, medium_ref, scale_ref, one, planes, rows)

    def from_below(slot, row):
        here = pl.ds(slot * rows + row, ROWS)
        return jnp.where(odd, pair_ref[here, :], chip_ref[here, :])

    def from_above(slot, row):
        here = pl.ds(slot * rows + row, ROWS)
        return jnp.where(odd, chip_ref[here, :], pair_ref[here, :])

    for row in chunks(rows):
        sums = edge_sums(lambda c, s: rows_at(one, (c, planes - 1), row, s), lane)
        scale = (sweep_steps[1] * last_scale) / (4.0 + from_above(12, row))
        for k, c in enumerate((1, 2, 4, 5)):
            put(delta_high, (c,), row, scale * sums[k])
        scale = sweep_steps[1] / (4.0 + from_below(12, row))
        for part in (0, 3):
            ey, ez = rows_at(one, (part + 1, 0), row), rows_at(one, (part + 2, 0), row)
            put(delta_low, (part + 1,), row, scale * ey)
            put(delta_low, (part + 2,), row, scale * ez)
            put(delta_low, (part,), row, scale * ((behind(ez, lane) - ez) + (rows_at(one, (part + 1, 0), row, -1) - ey)))

    where_yz = {1: 0, 2: 1, 4: 2, 5: 3}
    sweep_slab(
        one, held, two, source_ref, medium_ref, scale_ref, sweep_steps[1],
        lambda part, row: (from_below(2 * (part // 3), row), from_below(2 * (part // 3) + 1, row)),
        lambda c, row: from_above(where_yz[c], row),
        first_scale, planes, rows, lane,
    )

    none = [0.0] * 6
    for row in chunks(rows):
        values = curl(
            lambda c, s: rows_at(delta_low, (c,), row, s), lambda c: rows_at(two, (c, 0), row), row, lane
        )
        for c in range(6):
            put(held, (c, 0), row, values[c])
    for row in chunks(rows):
        before = {1: -rows_at(delta_low, (2,), row), 2: rows_at(delta_low, (1,), row),
                  4: -rows_at(delta_low, (5,), row), 5: rows_at(delta_low, (4,), row)}
        image = curl_back(lambda c, s: rows_at(held, (c, 0), row, s), lambda c: before[c], lane)
        real, imag = from_below(12, row), from_below(13, row)
        new = updated(
            [rows_at(delta_low, (c,), row) for c in range(6)], image, none, real, imag, sweep_steps[2] / (4.0 + real)
        )
        for c in range(6):
            put(delta_two, (c,), row, new[c])
    for row in chunks(rows):
        for part in (0, 3):
            ey, ez = rows_at(delta_high, (part + 1,), row), rows_at(delta_high, (part + 2,), row)
            put(held, (part, 1), row, (rows_at(delta_high, (part + 2,), row, 1) - ez) - (ahead(ey, lane) - ey))
    for row in chunks(rows):
        sums = edge_sums(lambda c, s: rows_at(two, (c, planes - 1), row, s), lane)
        real, imag = from_above(12, row), from_above(13, row)
        scale = (sweep_steps[2] * last_scale) / (4.0 + real)
        center, image = {}, {}
        for part in (0, 3):
            ey, ez = rows_at(delta_high, (part + 1,), row), rows_at(delta_high, (part + 2,), row)
            hx = rows_at(held, (part, 1), row)
            k = 2 * (part // 3)
            center[part + 1], center[part + 2] = ey, ez
            image[part + 1] = 2.0 * ey - sums[k] - (behind(hx, lane) - hx)
            image[part + 2] = (rows_at(held, (part, 1), row, -1) - hx) - sums[k + 1] + 2.0 * ez
        for k, c in enumerate((1, 2)):
            value = center[c] - scale * (image[c] + real * center[c] - imag * center[c + 3])
            delta_two[6 + k, pl.ds(PAD + row, ROWS), :] = value
            value = center[c + 3] - scale * (image[c + 3] + real * center[c + 3] + imag * center[c])
            delta_two[8 + k, pl.ds(PAD + row, ROWS), :] = value

    def low_of(level, deltas):
        def low(part, row):
            k = 4 * level + 2 * (part // 3)
            ex = rows_at(deltas, (part,), row)
            gy = from_below(k, row) + rows_at(deltas, (part + 1,), row) + (rows_at(deltas, (part,), row, 1) - ex)
            gz = from_below(k + 1, row) + rows_at(deltas, (part + 2,), row) + (ahead(ex, lane) - ex)
            return gy, gz
        return low

    sweep_slab(
        two, held, one, source_ref, medium_ref, scale_ref, sweep_steps[2],
        low_of(1, delta_low),
        lambda c, row: from_above(4 + where_yz[c], row) + rows_at(delta_high, (c,), row),
        first_scale, planes, rows, lane,
    )
    for c in range(6):
        delta_two[c, pl.ds(PAD + rows, PAD), :] = jnp.zeros((PAD, width), jnp.float32)
    sweep_slab(
        one, held, two, source_ref, medium_ref, scale_ref, sweep_steps[3],
        low_of(2, delta_two),
        lambda c, row: from_above(8 + where_yz[c], row) + rows_at(delta_two, (6 + where_yz[c],), row),
        first_scale, planes, rows, lane,
    )

    for i in range(planes):
        for row in chunks(rows):
            here = pl.ds(row, ROWS)
            for c in range(3):
                real = saved_ref[0, c, i, here, :].astype(jnp.float32)
                imag = saved_ref[0, c + 3, i, here, :].astype(jnp.float32)
                value = real * rows_at(two, (c + 3, i), row) + imag * rows_at(two, (c, i), row)
                if c < 2:
                    value = value + ahead(value, lane)
                put(moment, (c, i), row, value)
    for row in chunks(rows):
        here = pl.ds(row, ROWS)
        sums = [0.0] * (2 * REACH + 2)

        def add(value, offset, low):
            for k in range(2 * REACH + 1):
                slot = k + low
                sums[slot] = sums[slot] + jnp.where(offset == float(slot - REACH - 1), value, 0.0)

        def side(i):
            return rows_at(moment, (1, i), row) + (rows_at(moment, (2, i), row) + rows_at(moment, (2, i), row, 1))

        lower = side(0)
        add(edge_ref[0, here, :] * lower, edge_ref[1, here, :], 0)
        for i in range(planes):
            cell = rows_at(moment, (0, i), row) + rows_at(moment, (0, i), row, 1) + lower
            if i + 1 < planes:
                lower = side(i + 1)
                cell = cell + lower
            add(keep_ref[i, here, :] * cell, offset_ref[i, here, :], 1)
        for k in range(2 * REACH + 2):
            window[k, here, :] = sums[k]
    for k in range(2 * REACH + 2):
        both = window[k, pl.ds(0, rows // 2, stride=2), :] + window[k, pl.ds(1, rows // 2, stride=2), :]
        if k % 2 == 0:
            send_ref[k // 2] = both
        else:
            stay_ref[k // 2] = both


def vmem():
    return pl.BlockSpec(memory_space=pltpu.VMEM)


def call(kernel, out_shape, scratch, arguments, name):
    return pl.pallas_call(
        kernel,
        out_shape=[jax.ShapeDtypeStruct(s, jnp.float32) for s in out_shape],
        in_specs=[vmem()] * len(arguments),
        out_specs=[vmem()] * len(out_shape),
        scratch_shapes=[pltpu.VMEM(s, jnp.float32) for s in scratch],
        compiler_params=pltpu.CompilerParams(vmem_limit_bytes=24 << 20),
        name=name,
    )(*arguments)


def core_swap(value):
    size = lax.axis_size("space")
    return lax.ppermute(value, "space", [(i, i ^ 1) for i in range(size)])


def chip_swap(value):
    size = lax.axis_size("space")
    pairs = []
    for i in range(1, size - 1, 2):
        pairs += [(i, i + 1), (i + 1, i)]
    return lax.ppermute(value, "space", pairs)


def sum_over_groups(value):
    size = lax.axis_size("src")
    if size & (size - 1):
        return lax.psum(value, "src")
    step = 1
    while step < size:
        value = value + lax.ppermute(value, "src", [(i, i ^ step) for i in range(size)])
        step *= 2
    return value


def gather_owned(send, stay):
    size = lax.axis_size("space")
    index = lax.axis_index("space")
    odd = lax.rem(index, 2) == 1
    other = core_swap(send)
    far = jnp.where(odd, other[0], 0.0)
    below = stay[0] + jnp.where(odd, other[1], other[0])
    here = stay[1] + jnp.where(odd, other[2], other[1])
    above = stay[2] + jnp.where(odd, 0.0, other[2])
    chip = index // 2
    upward = lax.rem(chip, 2) == 0
    chips = size // 2
    inner, outer = [], []
    for c in range(chips):
        for core in range(2):
            if c ^ 1 < chips:
                inner.append((2 * c + core, 2 * (c ^ 1) + core))
            partner = ((c + 1) ^ 1) - 1
            if 0 <= partner < chips:
                outer.append((2 * c + core, 2 * partner + core))
    from_outer = lax.ppermute(jnp.where(upward, below, above), "space", outer)
    from_inner = lax.ppermute(jnp.where(upward, above, below), "space", inner)
    from_far = lax.ppermute(far, "space", [(i, i - 4) for i in range(5, size, 2)])
    return here + from_outer + from_inner + from_far


def transposed_smooth(summed, rough):
    rows_in = summed.shape[-2]
    depth_in = summed.shape[-1]
    total = jnp.zeros_like(summed)
    for vertical in range(3):
        for lateral in range(3):
            product = rough[vertical * 3 + lateral] * summed
            padded = jnp.pad(product, ((0, 0), (1, 1), (1, 1)))
            total = (
                total
                + padded[
                    :, 2 - vertical : 2 - vertical + rows_in, 2 - lateral : 2 - lateral + depth_in
                ]
            )
    return total


def shards(adjoint_source, forward_field, medium, plane_map, depth, rough):
    planes, rows, width = medium.shape[1:]
    index = lax.axis_index("space")
    levels = depth[0].astype(jnp.float32)
    owners = plane_map.astype(jnp.float32)
    meta = jnp.zeros((8, width), jnp.float32)
    meta = meta.at[0, :rows].set(levels[planes - 1]).at[1, :rows].set(owners[planes - 1])
    state = (6, planes, rows + 2 * PAD, width)
    held = (6, planes + 1, rows + 2 * PAD, width)
    message = (14 * rows + 8, width)
    pair, chip = call(
        send_kernel,
        [message, message],
        [(planes, rows, width), state, state, held],
        (adjoint_source, medium, meta),
        "send",
    )
    chip = chip_swap(chip)
    pair = core_swap(pair)
    here = index.astype(jnp.float32)
    position = lax.broadcasted_iota(jnp.int32, (planes, rows, width), 2).astype(jnp.float32)
    keep = jnp.where(position < levels[:, :, None], 0.25, 0.0)
    offset = jnp.broadcast_to((owners - here)[:, :, None], (planes, rows, width))
    below = jnp.where(lax.rem(index, 2) == 1, pair[14 * rows :], chip[14 * rows :])
    edge = jnp.stack(
        [
            jnp.where(position[0] < below[0, :rows, None], 0.25, 0.0),
            jnp.broadcast_to((below[1, :rows] - here)[:, None], (rows, width)),
        ]
    )
    plane = (rows + 2 * PAD, width)
    send, stay = call(
        window_kernel,
        [(REACH + 1, rows // 2, width), (REACH + 1, rows // 2, width)],
        [
            (planes, rows, width), state, state, held, (6,) + plane, (6,) + plane, (10,) + plane,
            (2 * REACH + 2, rows, width), (3, planes) + plane,
        ],
        (adjoint_source, medium, forward_field, keep, offset, edge, pair, chip),
        "window",
    )
    total = sum_over_groups(gather_owned(send, stay))
    return transposed_smooth(total[None], rough)


def solution(mesh):
    in_specs = (
        P("src", None, "space", None, None),
        P("src", None, "space", None, None),
        P(None, "space", None, None),
        P("space", None),
        P("src", "space", None),
        P(None, "space", None, None),
    )
    out_specs = P("space", None, None)
    return jax.shard_map(shards, mesh=mesh, in_specs=in_specs, out_specs=out_specs, check_vma=False)
```

```python
import functools

import jax
import jax.numpy as jnp
from jax import lax
from jax.experimental import pallas as pl
from jax.experimental.pallas import tpu as pltpu
from jax.sharding import PartitionSpec as P


REACH = 2

sweep_steps = (0.323, 1.658, 0.422, 0.752)

PAD = 8
ROWS = 16


def lane_of(width):
    return lax.broadcasted_iota(jnp.int32, (ROWS, width), 1)


def ahead(value, lane):
    width = value.shape[-1]
    return jnp.where(lane == width - 1, 0.0, pltpu.roll(value, width - 1, 1))


def behind(value, lane):
    return jnp.where(lane == 0, 0.0, pltpu.roll(value, 1, 1))


def rows_at(ref, index, row, shift=0):
    return ref[index + (pl.ds(PAD + row + shift, ROWS), slice(None))]


def put(ref, index, row, value):
    ref[index + (pl.ds(PAD + row, ROWS), slice(None))] = value


def clear_pads(ref):
    rows = ref.shape[-2]
    lead = ref.shape[:-2]
    zero = jnp.zeros((PAD, ref.shape[-1]), jnp.float32)
    for flat in range(functools.reduce(lambda a, b: a * b, lead, 1)):
        index = []
        rest = flat
        for size in reversed(lead):
            index.insert(0, rest % size)
            rest //= size
        ref[tuple(index) + (pl.ds(0, PAD), slice(None))] = zero
        ref[tuple(index) + (pl.ds(rows - PAD, PAD), slice(None))] = zero


def chunks(total):
    return range(0, total, ROWS)


def curl(field, ahead_of, lane):
    out = []
    for part in (0, 3):
        ex, ey, ez = field(part, 0), field(part + 1, 0), field(part + 2, 0)
        hx = (field(part + 2, 1) - ez) - (ahead(ey, lane) - ey)
        hy = (ahead(ex, lane) - ex) - (ahead_of(part + 2) - ez)
        hz = (ahead_of(part + 1) - ey) - (field(part, 1) - ex)
        out += [hx, hy, hz]
    return out


def curl_back(held, before, lane):
    out = []
    for part in (0, 3):
        hx, hy, hz = held(part, 0), held(part + 1, 0), held(part + 2, 0)
        ox = (behind(hy, lane) - hy) - (held(part + 2, -1) - hz)
        oy = (before(part + 2) - hz) - (behind(hx, lane) - hx)
        oz = (held(part, -1) - hx) - (before(part + 1) - hy)
        out += [ox, oy, oz]
    return out


def updated(center, image, source, real, imag, scale):
    out = []
    for c in range(3):
        applied = image[c] + real * center[c] - imag * center[c + 3]
        out.append(center[c] + scale * (source[c] - applied))
    for c in range(3):
        applied = image[c + 3] + real * center[c + 3] + imag * center[c]
        out.append(center[c + 3] + scale * (source[c + 3] - applied))
    return out


def edge_sums(field, lane):
    out = []
    for part in (0, 3):
        ex = field(part, 0)
        out.append(field(part + 1, 0) + (field(part, 1) - ex))
        out.append(field(part + 2, 0) + (ahead(ex, lane) - ex))
    return out


def sweep_slab(state, held, result, source_ref, medium_ref, scale_ref, weight, low, high, first_scale, planes, rows, lane, wanted=None):
    wanted = range(planes) if wanted is None else wanted
    needed = sorted({i for w in wanted for i in (w - 1, w)})
    for i in needed:
        for row in chunks(rows):
            if i < 0:
                for part in (0, 3):
                    gy, gz = low(part, row)
                    ey, ez = rows_at(state, (part + 1, 0), row), rows_at(state, (part + 2, 0), row)
                    put(held, (part + 1, 0), row, first_scale * (gz - ez))
                    put(held, (part + 2, 0), row, first_scale * (ey - gy))
                continue

            def ahead_of(c, i=i, row=row):
                if i + 1 < planes:
                    return rows_at(state, (c, i + 1), row)
                return high(c, row)

            values = curl(lambda c, s: rows_at(state, (c, i), row, s), ahead_of, lane)
            for c in range(6):
                put(held, (c, i + 1), row, values[c])
    for i in wanted:
        for row in chunks(rows):
            image = curl_back(
                lambda c, s: rows_at(held, (c, i + 1), row, s), lambda c: rows_at(held, (c, i), row), lane
            )
            here = pl.ds(row, ROWS)
            new = updated(
                [rows_at(state, (c, i), row) for c in range(6)],
                image,
                [source_ref[0, c, i, here, :] for c in range(6)],
                medium_ref[0, i, here, :],
                medium_ref[1, i, here, :],
                weight * scale_ref[i, here, :],
            )
            for c in range(6):
                put(result, (c, i), row, new[c])


def first_sweep(source_ref, medium_ref, scale_ref, state, planes, rows):
    for i in range(planes):
        for row in chunks(rows):
            here = pl.ds(row, ROWS)
            scale = 1.0 / (4.0 + medium_ref[0, i, here, :])
            scale_ref[i, here, :] = scale
            for c in range(6):
                put(state, (c, i), row, sweep_steps[0] * source_ref[0, c, i, here, :] * scale)


def parity_and_ends():
    index = lax.axis_index("space")
    odd = lax.rem(index, 2) == 1
    first_scale = jnp.where(index == 0, 0.0, 1.0)
    last_scale = jnp.where(index == lax.axis_size("space") - 1, 0.0, 1.0)
    return odd, first_scale, last_scale


def emitter(odd, pair_ref, chip_ref, rows):
    def emit(slot, row, below, above):
        here = pl.ds(slot * rows + row, ROWS)
        pair_ref[here, :] = jnp.where(odd, below, above)
        chip_ref[here, :] = jnp.where(odd, above, below)

    return emit


def emit_level(emit, state, planes, rows, lane):
    for row in chunks(rows):
        sums = edge_sums(lambda c, s: rows_at(state, (c, planes - 1), row, s), lane)
        bottom = [rows_at(state, (c, 0), row) for c in (1, 2, 4, 5)]
        for k in range(4):
            emit(k, row, bottom[k], sums[k])


def start_kernel(
    source_hbm, medium_hbm, depth_hbm, map_hbm, pair_ref, chip_ref, source_ref, medium_ref, meta_ref, top, levels, owners, sems
):
    planes, rows, width = medium_ref.shape[1:]
    lane = lane_of(width)
    odd = parity_and_ends()[0]
    order = [planes - 1, 0] + list(range(1, planes - 1))
    copies = []
    for i in order:
        copies.append(pltpu.make_async_copy(medium_hbm.at[:, i], medium_ref.at[:, i], sems.at[2 * i]))
        copies.append(pltpu.make_async_copy(source_hbm.at[0, :, i], source_ref.at[0, :, i], sems.at[2 * i + 1]))
    copies.append(pltpu.make_async_copy(depth_hbm.at[0], levels, sems.at[2 * planes]))
    copies.append(pltpu.make_async_copy(map_hbm, owners, sems.at[2 * planes + 1]))
    for copy in copies:
        copy.start()
    clear_pads(top)
    emit = emitter(odd, pair_ref, chip_ref, rows)
    last = planes - 1
    for copy in copies[:2]:
        copy.wait()
    for row in chunks(rows):
        here = pl.ds(row, ROWS)
        scale = sweep_steps[0] / (4.0 + medium_ref[0, last, here, :])
        for c in range(6):
            put(top, (c,), row, scale * source_ref[0, c, last, here, :])
    for copy in copies[2:4]:
        copy.wait()
    for row in chunks(rows):
        here = pl.ds(row, ROWS)
        scale = sweep_steps[0] / (4.0 + medium_ref[0, 0, here, :])
        sums = edge_sums(lambda c, s: rows_at(top, (c,), row, s), lane)
        for k, c in enumerate((1, 2, 4, 5)):
            emit(k, row, scale * source_ref[0, c, 0, here, :], sums[k])
        for k in range(2):
            emit(4 + k, row, medium_ref[k, 0, here, :], medium_ref[k, last, here, :])
    for copy in copies[4:]:
        copy.wait()
    meta_ref[...] = jnp.zeros_like(meta_ref)
    meta_ref[pl.ds(0, 1), pl.ds(0, rows)] = levels[pl.ds(last, 1), :].astype(jnp.float32)
    meta_ref[pl.ds(1, 1), pl.ds(0, rows)] = owners[pl.ds(last, 1), :].astype(jnp.float32)


def no_plane(c, row):
    return 0.0


def no_sums(part, row):
    return 0.0, 0.0


def follow_kernel(
    source_ref, medium_ref, meta_ref, pair_ref, chip_ref, pair_two_ref, chip_two_ref, scale_ref, one, two, held
):
    planes, rows, width = medium_ref.shape[1:]
    lane = lane_of(width)
    odd, first_scale, _ = parity_and_ends()
    for ref in (one, two, held):
        clear_pads(ref)
    first_sweep(source_ref, medium_ref, scale_ref, one, planes, rows)
    sweep_slab(
        one, held, two, source_ref, medium_ref, scale_ref, sweep_steps[1], no_sums, no_plane, first_scale,
        planes, rows, lane,
    )
    emit_level(emitter(odd, pair_ref, chip_ref, rows), two, planes, rows, lane)
    for ref in (pair_ref, chip_ref):
        ref[pl.ds(4 * rows, PAD), :] = meta_ref[...]
    sweep_slab(
        two, held, one, source_ref, medium_ref, scale_ref, sweep_steps[2], no_sums, no_plane, first_scale,
        planes, rows, lane, wanted=sorted({0, planes - 1}),
    )
    emit_level(emitter(odd, pair_two_ref, chip_two_ref, rows), one, planes, rows, lane)


def readers(odd, pair_ref, chip_ref, rows):
    def from_below(slot, row):
        here = pl.ds(slot * rows + row, ROWS)
        return jnp.where(odd, pair_ref[here, :], chip_ref[here, :])

    def from_above(slot, row):
        here = pl.ds(slot * rows + row, ROWS)
        return jnp.where(odd, chip_ref[here, :], pair_ref[here, :])

    return from_below, from_above


WHERE_YZ = {1: 0, 2: 1, 4: 2, 5: 3}


def moments(saved_ref, state, moment_ref, i, rows, lane):
    for row in chunks(rows):
        here = pl.ds(row, ROWS)
        for c in range(3):
            real = saved_ref[0, c, i, here, :].astype(jnp.float32)
            imag = saved_ref[0, c + 3, i, here, :].astype(jnp.float32)
            value = real * rows_at(state, (c + 3, i), row) + imag * rows_at(state, (c, i), row)
            if c < 2:
                value = value + ahead(value, lane)
            put(moment_ref, (c, i), row, value)


def middle_kernel(
    source_ref, medium_ref, saved_ref, pair_ref, chip_ref, pair_one_ref, chip_one_ref,
    state_ref, held, extra_ref, moment_ref, one, two, scale_ref, delta_low, delta_high, delta_two,
):
    planes, rows, width = medium_ref.shape[1:]
    lane = lane_of(width)
    odd, first_scale, last_scale = parity_and_ends()
    for ref in (one, two, state_ref, held, delta_low, delta_high, delta_two, moment_ref):
        clear_pads(ref)
    first_sweep(source_ref, medium_ref, scale_ref, one, planes, rows)
    from_below, from_above = readers(odd, pair_ref, chip_ref, rows)

    for row in chunks(rows):
        sums = edge_sums(lambda c, s: rows_at(one, (c, planes - 1), row, s), lane)
        scale = (sweep_steps[1] * last_scale) / (4.0 + from_above(4, row))
        for k, c in enumerate((1, 2, 4, 5)):
            put(delta_high, (c,), row, scale * sums[k])
        scale = sweep_steps[1] / (4.0 + from_below(4, row))
        for part in (0, 3):
            ey, ez = rows_at(one, (part + 1, 0), row), rows_at(one, (part + 2, 0), row)
            put(delta_low, (part + 1,), row, scale * ey)
            put(delta_low, (part + 2,), row, scale * ez)
            put(delta_low, (part,), row, scale * ((behind(ez, lane) - ez) + (rows_at(one, (part + 1, 0), row, -1) - ey)))

    sweep_slab(
        one, held, two, source_ref, medium_ref, scale_ref, sweep_steps[1],
        lambda part, row: (from_below(2 * (part // 3), row), from_below(2 * (part // 3) + 1, row)),
        lambda c, row: from_above(WHERE_YZ[c], row),
        first_scale, planes, rows, lane,
    )

    none = [0.0] * 6
    for row in chunks(rows):
        values = curl(lambda c, s: rows_at(delta_low, (c,), row, s), lambda c: rows_at(two, (c, 0), row), lane)
        for c in range(6):
            put(held, (c, 0), row, values[c])
    for row in chunks(rows):
        before = {1: -rows_at(delta_low, (2,), row), 2: rows_at(delta_low, (1,), row),
                  4: -rows_at(delta_low, (5,), row), 5: rows_at(delta_low, (4,), row)}
        image = curl_back(lambda c, s: rows_at(held, (c, 0), row, s), lambda c: before[c], lane)
        real, imag = from_below(4, row), from_below(5, row)
        new = updated(
            [rows_at(delta_low, (c,), row) for c in range(6)], image, none, real, imag, sweep_steps[2] / (4.0 + real)
        )
        for c in range(6):
            put(delta_two, (c,), row, new[c])
    for row in chunks(rows):
        sums = edge_sums(lambda c, s: rows_at(delta_two, (c,), row, s), lane)
        for k in range(4):
            extra_ref[k, pl.ds(row, ROWS), :] = sums[k]
    for row in chunks(rows):
        for part in (0, 3):
            ey, ez = rows_at(delta_high, (part + 1,), row), rows_at(delta_high, (part + 2,), row)
            put(held, (part, 1), row, (rows_at(delta_high, (part + 2,), row, 1) - ez) - (ahead(ey, lane) - ey))
    for row in chunks(rows):
        here = pl.ds(row, ROWS)
        sums = edge_sums(lambda c, s: rows_at(two, (c, planes - 1), row, s), lane)
        real, imag = from_above(4, row), from_above(5, row)
        scale = (sweep_steps[2] * last_scale) / (4.0 + real)
        center, image = {}, {}
        for part in (0, 3):
            ey, ez = rows_at(delta_high, (part + 1,), row), rows_at(delta_high, (part + 2,), row)
            hx = rows_at(held, (part, 1), row)
            k = 2 * (part // 3)
            center[part + 1], center[part + 2] = ey, ez
            image[part + 1] = 2.0 * ey - sums[k] - (behind(hx, lane) - hx)
            image[part + 2] = (rows_at(held, (part, 1), row, -1) - hx) - sums[k + 1] + 2.0 * ez
        for k, c in enumerate((1, 2)):
            extra_ref[4 + k, here, :] = center[c] - scale * (image[c] + real * center[c] - imag * center[c + 3])
            extra_ref[6 + k, here, :] = center[c + 3] - scale * (
                image[c + 3] + real * center[c + 3] + imag * center[c]
            )

    below_one, above_one = readers(odd, pair_one_ref, chip_one_ref, rows)

    def low(part, row):
        k = 2 * (part // 3)
        ex = rows_at(delta_low, (part,), row)
        gy = below_one(k, row) + rows_at(delta_low, (part + 1,), row) + (rows_at(delta_low, (part,), row, 1) - ex)
        gz = below_one(k + 1, row) + rows_at(delta_low, (part + 2,), row) + (ahead(ex, lane) - ex)
        return gy, gz

    sweep_slab(
        two, held, state_ref, source_ref, medium_ref, scale_ref, sweep_steps[2],
        low, lambda c, row: above_one(WHERE_YZ[c], row) + rows_at(delta_high, (c,), row),
        first_scale, planes, rows, lane,
    )
    inner = range(1, planes - 1)
    sweep_slab(
        state_ref, held, one, source_ref, medium_ref, scale_ref, sweep_steps[3], None, None, first_scale,
        planes, rows, lane, wanted=inner,
    )
    for i in inner:
        moments(saved_ref, one, moment_ref, i, rows, lane)


def window_kernel(
    source_ref, medium_ref, saved_ref, keep_ref, offset_ref, edge_ref, pair_ref, chip_ref, state_ref, held_ref,
    extra_ref, moment_in_ref, send_ref, stay_ref, held, two, scale_ref, moment, window,
):
    planes, rows, width = medium_ref.shape[1:]
    lane = lane_of(width)
    odd, first_scale, _ = parity_and_ends()
    from_below, from_above = readers(odd, pair_ref, chip_ref, rows)
    clear_pads(held)
    clear_pads(moment)
    ends = sorted({0, planes - 1})

    for row in chunks(rows):
        here = pl.ds(row, ROWS)
        for part in (0, 3):
            k = 2 * (part // 3)
            ey, ez = rows_at(state_ref, (part + 1, 0), row), rows_at(state_ref, (part + 2, 0), row)
            gy = from_below(k, row) + extra_ref[k, here, :]
            gz = from_below(k + 1, row) + extra_ref[k + 1, here, :]
            put(held, (part + 1, 0), row, first_scale * (gz - ez))
            put(held, (part + 2, 0), row, first_scale * (ey - gy))
        values = curl(
            lambda c, s: rows_at(state_ref, (c, planes - 1), row, s),
            lambda c: from_above(WHERE_YZ[c], row) + extra_ref[4 + WHERE_YZ[c], here, :],
            lane,
        )
        for c in range(6):
            put(held, (c, 1), row, values[c])
    for i in ends:
        for row in chunks(rows):
            here = pl.ds(row, ROWS)
            if i == planes - 1:
                now = lambda c, s: rows_at(held, (c, 1), row, s)
            else:
                now = lambda c, s: rows_at(held_ref, (c, i + 1), row, s)
            if i == 0:
                before = lambda c: rows_at(held, (c, 0), row)
            else:
                before = lambda c: rows_at(held_ref, (c, i), row)
            image = curl_back(now, before, lane)
            real, imag = medium_ref[0, i, here, :], medium_ref[1, i, here, :]
            new = updated(
                [rows_at(state_ref, (c, i), row) for c in range(6)], image,
                [source_ref[0, c, i, here, :] for c in range(6)], real, imag, sweep_steps[3] / (4.0 + real),
            )
            for c in range(6):
                put(two, (c, i), row, new[c])
        moments(saved_ref, two, moment, i, rows, lane)

    def moment_rows(c, i, row, shift=0):
        return rows_at(moment if i in ends else moment_in_ref, (c, i), row, shift)

    for row in chunks(rows):
        here = pl.ds(row, ROWS)
        sums = [0.0] * (2 * REACH + 2)

        def add(value, offset, low):
            for k in range(2 * REACH + 1):
                slot = k + low
                sums[slot] = sums[slot] + jnp.where(offset == float(slot - REACH - 1), value, 0.0)

        def side(i):
            return moment_rows(1, i, row) + (moment_rows(2, i, row) + moment_rows(2, i, row, 1))

        lower = side(0)
        add(edge_ref[0, here, :] * lower, edge_ref[1, here, :], 0)
        for i in range(planes):
            cell = moment_rows(0, i, row) + moment_rows(0, i, row, 1) + lower
            if i + 1 < planes:
                lower = side(i + 1)
                cell = cell + lower
            add(keep_ref[i, here, :] * cell, offset_ref[i, here, :], 1)
        for k in range(2 * REACH + 2):
            window[k, here, :] = sums[k]
    for k in range(2 * REACH + 2):
        both = window[k, pl.ds(0, rows // 2, stride=2), :] + window[k, pl.ds(1, rows // 2, stride=2), :]
        if k % 2 == 0:
            send_ref[k // 2] = both
        else:
            stay_ref[k // 2] = both


def vmem():
    return pl.BlockSpec(memory_space=pltpu.VMEM)


def call(kernel, out_shape, scratch, arguments, in_specs=None, limit=24 << 20, flops=1 << 20):
    return pl.pallas_call(
        kernel,
        out_shape=[jax.ShapeDtypeStruct(s, jnp.float32) for s in out_shape],
        in_specs=in_specs or [vmem()] * len(arguments),
        out_specs=[vmem()] * len(out_shape),
        scratch_shapes=[s if not isinstance(s, tuple) else pltpu.VMEM(s, jnp.float32) for s in scratch],
        compiler_params=pltpu.CompilerParams(vmem_limit_bytes=limit),
        cost_estimate=pl.CostEstimate(flops=flops, bytes_accessed=1 << 20, transcendentals=0),
    )(*arguments)


def core_swap(value):
    size = lax.axis_size("space")
    return lax.ppermute(value, "space", [(i, i ^ 1) for i in range(size)])


def chip_swap(value):
    size = lax.axis_size("space")
    pairs = []
    for i in range(1, size - 1, 2):
        pairs += [(i, i + 1), (i + 1, i)]
    return lax.ppermute(value, "space", pairs)


def sum_over_groups(value):
    size = lax.axis_size("src")
    if size & (size - 1):
        return lax.psum(value, "src")
    step = 1
    while step < size:
        value = value + lax.ppermute(value, "src", [(i, i ^ step) for i in range(size)])
        step *= 2
    return value


def gather_owned(send, stay):
    size = lax.axis_size("space")
    index = lax.axis_index("space")
    odd = lax.rem(index, 2) == 1
    other = core_swap(send)
    from_far = lax.ppermute(send[0], "space", [(i, i - 3) for i in range(4, size, 2)])
    below = stay[0] + jnp.where(odd, other[1], other[0])
    here = stay[1] + jnp.where(odd, other[2], other[1])
    above = stay[2] + jnp.where(odd, 0.0, other[2])
    chip = index // 2
    upward = lax.rem(chip, 2) == 0
    chips = size // 2
    inner, outer = [], []
    for c in range(chips):
        for core in range(2):
            if c ^ 1 < chips:
                inner.append((2 * c + core, 2 * (c ^ 1) + core))
            partner = ((c + 1) ^ 1) - 1
            if 0 <= partner < chips:
                outer.append((2 * c + core, 2 * partner + core))
    from_outer = lax.ppermute(jnp.where(upward, below, above), "space", outer)
    from_inner = lax.ppermute(jnp.where(upward, above, below), "space", inner)
    return here + from_far + from_outer + from_inner


def transposed_smooth(summed, rough):
    rows_in = summed.shape[-2]
    depth_in = summed.shape[-1]
    total = jnp.zeros_like(summed)
    for vertical in range(3):
        for lateral in range(3):
            product = rough[vertical * 3 + lateral] * summed
            padded = jnp.pad(product, ((0, 0), (1, 1), (1, 1)))
            total = (
                total
                + padded[
                    :, 2 - vertical : 2 - vertical + rows_in, 2 - lateral : 2 - lateral + depth_in
                ]
            )
    return total


def slab(adjoint_source, forward_field, medium, plane_map, depth, rough):
    planes, rows, width = medium.shape[1:]
    index = lax.axis_index("space")
    plane = (rows + 2 * PAD, width)
    state = (6, planes) + plane
    held = (6, planes + 1) + plane
    scale = (planes, rows, width)
    hbm = pl.BlockSpec(memory_space=pltpu.HBM)
    columns = pltpu.VMEM((planes, rows), jnp.int32)
    given = (adjoint_source, medium, depth, plane_map)
    pair, chip, adjoint_source, medium, meta = call(
        start_kernel,
        [(6 * rows, width)] * 2 + [adjoint_source.shape, medium.shape, (PAD, width)],
        [(6,) + plane, columns, columns, pltpu.SemaphoreType.DMA((2 * planes + 2,))],
        tuple(pltpu.with_memory_space_constraint(a, pltpu.HBM) for a in given),
        in_specs=[hbm] * 4,
    )
    chip = chip_swap(chip)
    pair = core_swap(pair)
    pair_one, chip_one, pair_two, chip_two = call(
        follow_kernel,
        [(4 * rows + PAD, width)] * 2 + [(4 * rows, width)] * 2,
        [scale, state, state, held],
        (adjoint_source, medium, meta),
    )
    chip_one = chip_swap(chip_one)
    pair_one = core_swap(pair_one)
    chip_two = chip_swap(chip_two)
    pair_two = core_swap(pair_two)

    here = index.astype(jnp.float32)
    levels = depth[0].astype(jnp.float32)
    owners = plane_map.astype(jnp.float32)
    position = lax.broadcasted_iota(jnp.int32, (planes, rows, width), 2).astype(jnp.float32)
    keep = jnp.where(position < levels[:, :, None], 0.25, 0.0)
    offset = jnp.broadcast_to((owners - here)[:, :, None], (planes, rows, width))
    below = jnp.where(lax.rem(index, 2) == 1, pair_one[4 * rows :], chip_one[4 * rows :])
    edge = jnp.stack(
        [
            jnp.where(position[0] < below[0, :rows, None], 0.25, 0.0),
            jnp.broadcast_to((below[1, :rows] - here)[:, None], (rows, width)),
        ]
    )
    middle, curls, extra, moment = call(
        middle_kernel,
        [state, held, (8, rows, width), (3, planes) + plane],
        [state, state, scale, (6,) + plane, (6,) + plane, (6,) + plane],
        (adjoint_source, medium, forward_field, pair, chip, pair_one, chip_one),
    )
    send, stay = call(
        window_kernel,
        [(REACH + 1, rows // 2, width), (REACH + 1, rows // 2, width)],
        [(6, 2) + plane, state, scale, (3, planes) + plane, (2 * REACH + 2, rows, width)],
        (adjoint_source, medium, forward_field, keep, offset, edge, pair_two, chip_two, middle, curls, extra, moment),
    )
    total = sum_over_groups(gather_owned(send, stay))
    return transposed_smooth(total[None], rough)


def solution(mesh):
    in_specs = (
        P("src", None, "space", None, None),
        P("src", None, "space", None, None),
        P(None, "space", None, None),
        P("space", None),
        P("src", "space", None),
        P(None, "space", None, None),
    )
    out_specs = P("space", None, None)
    return jax.shard_map(slab, mesh=mesh, in_specs=in_specs, out_specs=out_specs, check_vma=False)
```

```python
import functools

import jax
import jax.numpy as jnp
from jax import lax
from jax.experimental import pallas as pl
from jax.experimental.pallas import tpu as pltpu
from jax.sharding import PartitionSpec as P


REACH = 2

sweep_steps = (0.323, 1.658, 0.422, 0.752)

PAD = 8
ROWS = 16


def lane_of(width):
    return lax.broadcasted_iota(jnp.int32, (ROWS, width), 1)


def ahead(value, lane):
    width = value.shape[-1]
    return jnp.where(lane == width - 1, 0.0, pltpu.roll(value, width - 1, 1))


def behind(value, lane):
    return jnp.where(lane == 0, 0.0, pltpu.roll(value, 1, 1))


def rows_at(ref, index, row, shift=0):
    return ref[index + (pl.ds(PAD + row + shift, ROWS), slice(None))]


def put(ref, index, row, value):
    ref[index + (pl.ds(PAD + row, ROWS), slice(None))] = value


def clear_pads(ref):
    rows = ref.shape[-2]
    lead = ref.shape[:-2]
    zero = jnp.zeros((PAD, ref.shape[-1]), jnp.float32)
    for flat in range(functools.reduce(lambda a, b: a * b, lead, 1)):
        index = []
        rest = flat
        for size in reversed(lead):
            index.insert(0, rest % size)
            rest //= size
        ref[tuple(index) + (pl.ds(0, PAD), slice(None))] = zero
        ref[tuple(index) + (pl.ds(rows - PAD, PAD), slice(None))] = zero


def chunks(total):
    return range(0, total, ROWS)


def curl(field, ahead_of, lane):
    out = []
    for part in (0, 3):
        ex, ey, ez = field(part, 0), field(part + 1, 0), field(part + 2, 0)
        hx = (field(part + 2, 1) - ez) - (ahead(ey, lane) - ey)
        hy = (ahead(ex, lane) - ex) - (ahead_of(part + 2) - ez)
        hz = (ahead_of(part + 1) - ey) - (field(part, 1) - ex)
        out += [hx, hy, hz]
    return out


def curl_back(held, before, lane):
    out = []
    for part in (0, 3):
        hx, hy, hz = held(part, 0), held(part + 1, 0), held(part + 2, 0)
        ox = (behind(hy, lane) - hy) - (held(part + 2, -1) - hz)
        oy = (before(part + 2) - hz) - (behind(hx, lane) - hx)
        oz = (held(part, -1) - hx) - (before(part + 1) - hy)
        out += [ox, oy, oz]
    return out


def updated(center, image, source, real, imag, scale):
    out = []
    for c in range(3):
        applied = image[c] + real * center[c] - imag * center[c + 3]
        out.append(center[c] + scale * (source[c] - applied))
    for c in range(3):
        applied = image[c + 3] + real * center[c + 3] + imag * center[c]
        out.append(center[c + 3] + scale * (source[c + 3] - applied))
    return out


def edge_sums(field, lane):
    out = []
    for part in (0, 3):
        ex = field(part, 0)
        out.append(field(part + 1, 0) + (field(part, 1) - ex))
        out.append(field(part + 2, 0) + (ahead(ex, lane) - ex))
    return out


def sweep_slab(state, held, result, source_ref, medium_ref, scale_ref, weight, low, high, first_scale, planes, rows, lane, wanted=None):
    wanted = range(planes) if wanted is None else wanted
    needed = sorted({i for w in wanted for i in (w - 1, w)})
    for i in needed:
        for row in chunks(rows):
            if i < 0:
                for part in (0, 3):
                    gy, gz = low(part, row)
                    ey, ez = rows_at(state, (part + 1, 0), row), rows_at(state, (part + 2, 0), row)
                    put(held, (part + 1, 0), row, first_scale * (gz - ez))
                    put(held, (part + 2, 0), row, first_scale * (ey - gy))
                continue

            def ahead_of(c, i=i, row=row):
                if i + 1 < planes:
                    return rows_at(state, (c, i + 1), row)
                return high(c, row)

            values = curl(lambda c, s: rows_at(state, (c, i), row, s), ahead_of, lane)
            for c in range(6):
                put(held, (c, i + 1), row, values[c])
    for i in wanted:
        for row in chunks(rows):
            image = curl_back(
                lambda c, s: rows_at(held, (c, i + 1), row, s), lambda c: rows_at(held, (c, i), row), lane
            )
            here = pl.ds(row, ROWS)
            new = updated(
                [rows_at(state, (c, i), row) for c in range(6)],
                image,
                [source_ref[0, c, i, here, :] for c in range(6)],
                medium_ref[0, i, here, :],
                medium_ref[1, i, here, :],
                weight * scale_ref[i, here, :],
            )
            for c in range(6):
                put(result, (c, i), row, new[c])


def first_sweep(source_ref, medium_ref, scale_ref, state, planes, rows):
    for i in range(planes):
        for row in chunks(rows):
            here = pl.ds(row, ROWS)
            scale = 1.0 / (4.0 + medium_ref[0, i, here, :])
            scale_ref[i, here, :] = scale
            for c in range(6):
                put(state, (c, i), row, sweep_steps[0] * source_ref[0, c, i, here, :] * scale)


def parity_and_ends():
    index = lax.axis_index("space")
    odd = lax.rem(index, 2) == 1
    first_scale = jnp.where(index == 0, 0.0, 1.0)
    last_scale = jnp.where(index == lax.axis_size("space") - 1, 0.0, 1.0)
    return odd, first_scale, last_scale


def emit_level(emit, state, planes, rows, lane):
    for row in chunks(rows):
        sums = edge_sums(lambda c, s: rows_at(state, (c, planes - 1), row, s), lane)
        bottom = [rows_at(state, (c, 0), row) for c in (1, 2, 4, 5)]
        for k in range(4):
            emit(k, row, bottom[k], sums[k])


def message_rows(slot, row, rows):
    return pl.ds(slot * rows + row, ROWS)


def start_kernel(
    source_hbm, medium_hbm, depth_hbm, map_hbm, chip_ref, source_ref, medium_ref, meta_ref, top, levels, owners, sems
):
    planes, rows, width = medium_ref.shape[1:]
    lane = lane_of(width)
    odd = parity_and_ends()[0]
    order = [planes - 1, 0] + list(range(1, planes - 1))
    copies = []
    for i in order:
        copies.append(pltpu.make_async_copy(medium_hbm.at[:, i], medium_ref.at[:, i], sems.at[2 * i]))
        copies.append(pltpu.make_async_copy(source_hbm.at[0, :, i], source_ref.at[0, :, i], sems.at[2 * i + 1]))
    copies.append(pltpu.make_async_copy(depth_hbm.at[0], levels, sems.at[2 * planes]))
    copies.append(pltpu.make_async_copy(map_hbm, owners, sems.at[2 * planes + 1]))
    for copy in copies:
        copy.start()
    clear_pads(top)
    last = planes - 1

    def emit(slot, row, below, above):
        chip_ref[message_rows(slot, row, rows), :] = jnp.where(odd, above, below)

    for copy in copies[:2]:
        copy.wait()
    for row in chunks(rows):
        here = pl.ds(row, ROWS)
        scale = sweep_steps[0] / (4.0 + medium_ref[0, last, here, :])
        for c in range(6):
            put(top, (c,), row, scale * source_ref[0, c, last, here, :])
    for copy in copies[2:4]:
        copy.wait()
    for row in chunks(rows):
        here = pl.ds(row, ROWS)
        scale = sweep_steps[0] / (4.0 + medium_ref[0, 0, here, :])
        sums = edge_sums(lambda c, s: rows_at(top, (c,), row, s), lane)
        for k, c in enumerate((1, 2, 4, 5)):
            emit(k, row, scale * source_ref[0, c, 0, here, :], sums[k])
        for k in range(2):
            emit(4 + k, row, medium_ref[k, 0, here, :], medium_ref[k, last, here, :])
    for copy in copies[4:]:
        copy.wait()
    meta_ref[...] = jnp.zeros_like(meta_ref)
    meta_ref[pl.ds(0, 1), pl.ds(0, rows)] = levels[pl.ds(last, 1), :].astype(jnp.float32)
    meta_ref[pl.ds(1, 1), pl.ds(0, rows)] = owners[pl.ds(last, 1), :].astype(jnp.float32)


def no_plane(c, row):
    return 0.0


def no_sums(part, row):
    return 0.0, 0.0


def follow_kernel(source_ref, medium_ref, meta_ref, pair_ref, chip_ref, chip_two_ref, scale_ref, one, two, held):
    planes, rows, width = medium_ref.shape[1:]
    lane = lane_of(width)
    odd, first_scale, _ = parity_and_ends()
    for ref in (one, two, held):
        clear_pads(ref)

    def emitter(slots, to_chip):
        def emit(slot, row, below, above):
            pair_ref[message_rows(slots + slot, row, rows), :] = jnp.where(odd, below, above)
            if to_chip is not None:
                to_chip[message_rows(slot, row, rows), :] = jnp.where(odd, above, below)

        return emit

    first_sweep(source_ref, medium_ref, scale_ref, one, planes, rows)
    sweep_slab(
        one, held, two, source_ref, medium_ref, scale_ref, sweep_steps[1], no_sums, no_plane, first_scale,
        planes, rows, lane,
    )
    emit_level(emitter(6, chip_ref), two, planes, rows, lane)
    emit_level(emitter(0, None), one, planes, rows, lane)
    emit = emitter(4, None)
    for row in chunks(rows):
        for k in range(2):
            here = pl.ds(row, ROWS)
            emit(k, row, medium_ref[k, 0, here, :], medium_ref[k, planes - 1, here, :])
    chip_ref[pl.ds(4 * rows, PAD), :] = meta_ref[...]
    pair_ref[pl.ds(14 * rows, PAD), :] = meta_ref[...]
    sweep_slab(
        two, held, one, source_ref, medium_ref, scale_ref, sweep_steps[2], no_sums, no_plane, first_scale,
        planes, rows, lane, wanted=sorted({0, planes - 1}),
    )
    emit_level(emitter(10, chip_two_ref), one, planes, rows, lane)


def readers(odd, pair_ref, chip_ref, rows, first):
    def from_below(slot, row):
        pair, chip = pair_ref[message_rows(first + slot, row, rows), :], chip_ref[message_rows(slot, row, rows), :]
        return jnp.where(odd, pair, chip)

    def from_above(slot, row):
        pair, chip = pair_ref[message_rows(first + slot, row, rows), :], chip_ref[message_rows(slot, row, rows), :]
        return jnp.where(odd, chip, pair)

    return from_below, from_above


WHERE_YZ = {1: 0, 2: 1, 4: 2, 5: 3}


def moments(saved_ref, state, moment_ref, i, rows, lane):
    for row in chunks(rows):
        here = pl.ds(row, ROWS)
        for c in range(3):
            real = saved_ref[0, c, i, here, :].astype(jnp.float32)
            imag = saved_ref[0, c + 3, i, here, :].astype(jnp.float32)
            value = real * rows_at(state, (c + 3, i), row) + imag * rows_at(state, (c, i), row)
            if c < 2:
                value = value + ahead(value, lane)
            put(moment_ref, (c, i), row, value)


def early_kernel(
    source_ref, medium_ref, pair_ref, chip_ref, two, scale_ref, extra_ref, one, held, delta_low, delta_high, delta_two,
):
    planes, rows, width = medium_ref.shape[1:]
    lane = lane_of(width)
    odd, first_scale, last_scale = parity_and_ends()
    for ref in (one, two, held, delta_low, delta_high, delta_two):
        clear_pads(ref)
    first_sweep(source_ref, medium_ref, scale_ref, one, planes, rows)
    from_below, from_above = readers(odd, pair_ref, chip_ref, rows, 0)

    for row in chunks(rows):
        sums = edge_sums(lambda c, s: rows_at(one, (c, planes - 1), row, s), lane)
        scale = (sweep_steps[1] * last_scale) / (4.0 + from_above(4, row))
        for k, c in enumerate((1, 2, 4, 5)):
            put(delta_high, (c,), row, scale * sums[k])
        scale = sweep_steps[1] / (4.0 + from_below(4, row))
        for part in (0, 3):
            ey, ez = rows_at(one, (part + 1, 0), row), rows_at(one, (part + 2, 0), row)
            put(delta_low, (part + 1,), row, scale * ey)
            put(delta_low, (part + 2,), row, scale * ez)
            put(delta_low, (part,), row, scale * ((behind(ez, lane) - ez) + (rows_at(one, (part + 1, 0), row, -1) - ey)))

    sweep_slab(
        one, held, two, source_ref, medium_ref, scale_ref, sweep_steps[1],
        lambda part, row: (from_below(2 * (part // 3), row), from_below(2 * (part // 3) + 1, row)),
        lambda c, row: from_above(WHERE_YZ[c], row),
        first_scale, planes, rows, lane,
    )

    none = [0.0] * 6
    for row in chunks(rows):
        values = curl(lambda c, s: rows_at(delta_low, (c,), row, s), lambda c: rows_at(two, (c, 0), row), lane)
        for c in range(6):
            put(held, (c, 0), row, values[c])
    for row in chunks(rows):
        before = {1: -rows_at(delta_low, (2,), row), 2: rows_at(delta_low, (1,), row),
                  4: -rows_at(delta_low, (5,), row), 5: rows_at(delta_low, (4,), row)}
        image = curl_back(lambda c, s: rows_at(held, (c, 0), row, s), lambda c: before[c], lane)
        real, imag = from_below(4, row), from_below(5, row)
        new = updated(
            [rows_at(delta_low, (c,), row) for c in range(6)], image, none, real, imag, sweep_steps[2] / (4.0 + real)
        )
        for c in range(6):
            put(delta_two, (c,), row, new[c])
    for row in chunks(rows):
        for level, deltas in enumerate((delta_low, delta_two)):
            sums = edge_sums(lambda c, s: rows_at(deltas, (c,), row, s), lane)
            for k in range(4):
                extra_ref[8 * level + k, pl.ds(row, ROWS), :] = sums[k]
        for k, c in enumerate((1, 2, 4, 5)):
            extra_ref[4 + k, pl.ds(row, ROWS), :] = rows_at(delta_high, (c,), row)
    for row in chunks(rows):
        for part in (0, 3):
            ey, ez = rows_at(delta_high, (part + 1,), row), rows_at(delta_high, (part + 2,), row)
            put(held, (part, 1), row, (rows_at(delta_high, (part + 2,), row, 1) - ez) - (ahead(ey, lane) - ey))
    for row in chunks(rows):
        here = pl.ds(row, ROWS)
        sums = edge_sums(lambda c, s: rows_at(two, (c, planes - 1), row, s), lane)
        real, imag = from_above(4, row), from_above(5, row)
        scale = (sweep_steps[2] * last_scale) / (4.0 + real)
        center, image = {}, {}
        for part in (0, 3):
            ey, ez = rows_at(delta_high, (part + 1,), row), rows_at(delta_high, (part + 2,), row)
            hx = rows_at(held, (part, 1), row)
            k = 2 * (part // 3)
            center[part + 1], center[part + 2] = ey, ez
            image[part + 1] = 2.0 * ey - sums[k] - (behind(hx, lane) - hx)
            image[part + 2] = (rows_at(held, (part, 1), row, -1) - hx) - sums[k + 1] + 2.0 * ez
        for k, c in enumerate((1, 2)):
            extra_ref[12 + k, here, :] = center[c] - scale * (image[c] + real * center[c] - imag * center[c + 3])
            extra_ref[14 + k, here, :] = center[c + 3] - scale * (
                image[c + 3] + real * center[c + 3] + imag * center[c]
            )


def middle_kernel(
    source_ref, medium_ref, saved_ref, pair_ref, chip_ref, state_in_ref, scale_ref, extra_ref,
    state_ref, held, moment_ref, one,
):
    planes, rows, width = medium_ref.shape[1:]
    lane = lane_of(width)
    odd, first_scale, _ = parity_and_ends()
    for ref in (one, state_ref, held, moment_ref):
        clear_pads(ref)
    from_below, from_above = readers(odd, pair_ref, chip_ref, rows, 6)

    def low(part, row):
        k = 2 * (part // 3)
        here = pl.ds(row, ROWS)
        return from_below(k, row) + extra_ref[k, here, :], from_below(k + 1, row) + extra_ref[k + 1, here, :]

    def high(c, row):
        return from_above(WHERE_YZ[c], row) + extra_ref[4 + WHERE_YZ[c], pl.ds(row, ROWS), :]

    sweep_slab(
        state_in_ref, held, state_ref, source_ref, medium_ref, scale_ref, sweep_steps[2], low, high, first_scale,
        planes, rows, lane,
    )
    inner = range(1, planes - 1)
    sweep_slab(
        state_ref, held, one, source_ref, medium_ref, scale_ref, sweep_steps[3], None, None, first_scale,
        planes, rows, lane, wanted=inner,
    )
    for i in inner:
        moments(saved_ref, one, moment_ref, i, rows, lane)


def window_kernel(
    source_ref, medium_ref, saved_ref, owner_ref, edge_ref, pair_ref, chip_ref, state_ref, held_ref, scale_ref,
    extra_ref, moment_in_ref, send_ref, stay_ref, held, two, moment, window,
):
    planes, rows, width = medium_ref.shape[1:]
    lane = lane_of(width)
    odd, first_scale, _ = parity_and_ends()
    from_below, from_above = readers(odd, pair_ref, chip_ref, rows, 10)
    clear_pads(held)
    clear_pads(moment)
    ends = sorted({0, planes - 1})

    for row in chunks(rows):
        here = pl.ds(row, ROWS)
        for part in (0, 3):
            k = 2 * (part // 3)
            ey, ez = rows_at(state_ref, (part + 1, 0), row), rows_at(state_ref, (part + 2, 0), row)
            gy = from_below(k, row) + extra_ref[8 + k, here, :]
            gz = from_below(k + 1, row) + extra_ref[9 + k, here, :]
            put(held, (part + 1, 0), row, first_scale * (gz - ez))
            put(held, (part + 2, 0), row, first_scale * (ey - gy))
        values = curl(
            lambda c, s: rows_at(state_ref, (c, planes - 1), row, s),
            lambda c: from_above(WHERE_YZ[c], row) + extra_ref[12 + WHERE_YZ[c], here, :],
            lane,
        )
        for c in range(6):
            put(held, (c, 1), row, values[c])
    for i in ends:
        for row in chunks(rows):
            here = pl.ds(row, ROWS)
            if i == planes - 1:
                now = lambda c, s: rows_at(held, (c, 1), row, s)
            else:
                now = lambda c, s: rows_at(held_ref, (c, i + 1), row, s)
            if i == 0:
                before = lambda c: rows_at(held, (c, 0), row)
            else:
                before = lambda c: rows_at(held_ref, (c, i), row)
            image = curl_back(now, before, lane)
            real, imag = medium_ref[0, i, here, :], medium_ref[1, i, here, :]
            new = updated(
                [rows_at(state_ref, (c, i), row) for c in range(6)], image,
                [source_ref[0, c, i, here, :] for c in range(6)], real, imag, sweep_steps[3] * scale_ref[i, here, :],
            )
            for c in range(6):
                put(two, (c, i), row, new[c])
        moments(saved_ref, two, moment, i, rows, lane)

    def moment_rows(c, i, row, shift=0):
        return rows_at(moment if i in ends else moment_in_ref, (c, i), row, shift)

    for row in chunks(rows):
        here = pl.ds(row, ROWS)
        sums = [0.0] * (2 * REACH + 2)

        def add(value, offset, low):
            for k in range(2 * REACH + 1):
                slot = k + low
                sums[slot] = sums[slot] + jnp.where(offset == float(slot - REACH - 1), value, 0.0)

        def side(i):
            return moment_rows(1, i, row) + (moment_rows(2, i, row) + moment_rows(2, i, row, 1))

        lower = side(0)
        add(lower, edge_ref[here, :], 0)
        for i in range(planes):
            cell = moment_rows(0, i, row) + moment_rows(0, i, row, 1) + lower
            if i + 1 < planes:
                lower = side(i + 1)
                cell = cell + lower
            add(cell, owner_ref[i, here, :], 1)
        for k in range(2 * REACH + 2):
            window[k, here, :] = sums[k]
    for k in range(2 * REACH + 2):
        both = 0.25 * (window[k, pl.ds(0, rows // 2, stride=2), :] + window[k, pl.ds(1, rows // 2, stride=2), :])
        if k % 2 == 0:
            send_ref[k // 2] = both
        else:
            stay_ref[k // 2] = both


def vmem():
    return pl.BlockSpec(memory_space=pltpu.VMEM)


def call(kernel, out_shape, scratch, arguments, in_specs=None, limit=24 << 20, flops=1 << 20):
    return pl.pallas_call(
        kernel,
        out_shape=[jax.ShapeDtypeStruct(s, jnp.float32) for s in out_shape],
        in_specs=in_specs or [vmem()] * len(arguments),
        out_specs=[vmem()] * len(out_shape),
        scratch_shapes=[s if not isinstance(s, tuple) else pltpu.VMEM(s, jnp.float32) for s in scratch],
        compiler_params=pltpu.CompilerParams(vmem_limit_bytes=limit),
        cost_estimate=pl.CostEstimate(flops=flops, bytes_accessed=1 << 20, transcendentals=0),
    )(*arguments)


def core_swap(value):
    size = lax.axis_size("space")
    return lax.ppermute(value, "space", [(i, i ^ 1) for i in range(size)])


def chip_swap(value):
    size = lax.axis_size("space")
    pairs = []
    for i in range(1, size - 1, 2):
        pairs += [(i, i + 1), (i + 1, i)]
    return lax.ppermute(value, "space", pairs)


def sum_over_groups(value):
    size = lax.axis_size("src")
    if size & (size - 1):
        return lax.psum(value, "src")
    step = 1
    while step < size:
        value = value + lax.ppermute(value, "src", [(i, i ^ step) for i in range(size)])
        step *= 2
    return value


def gather_owned(send, stay):
    size = lax.axis_size("space")
    index = lax.axis_index("space")
    odd = lax.rem(index, 2) == 1
    other = core_swap(send)
    below = stay[0] + jnp.where(odd, other[1], other[0])
    here = stay[1] + jnp.where(odd, other[2], other[1])
    above = stay[2] + jnp.where(odd, 0.0, other[2])
    chip = index // 2
    upward = lax.rem(chip, 2) == 0
    chips = size // 2
    inner, outer = [], []
    for c in range(chips):
        for core in range(2):
            if c ^ 1 < chips:
                inner.append((2 * c + core, 2 * (c ^ 1) + core))
            partner = ((c + 1) ^ 1) - 1
            if 0 <= partner < chips:
                outer.append((2 * c + core, 2 * partner + core))
    from_inner = lax.ppermute(jnp.where(upward, above, below), "space", inner)
    from_outer = lax.ppermute(jnp.where(upward, below, above), "space", outer)
    from_far = lax.ppermute(other[0], "space", [(i, i - 4) for i in range(5, size, 2)])
    return here + from_inner + from_outer + from_far


def transposed_smooth(summed, rough):
    rows_in = summed.shape[-2]
    depth_in = summed.shape[-1]
    total = jnp.zeros_like(summed)
    for vertical in range(3):
        for lateral in range(3):
            product = rough[vertical * 3 + lateral] * summed
            padded = jnp.pad(product, ((0, 0), (1, 1), (1, 1)))
            total = (
                total
                + padded[
                    :, 2 - vertical : 2 - vertical + rows_in, 2 - lateral : 2 - lateral + depth_in
                ]
            )
    return total


def slab(adjoint_source, forward_field, medium, plane_map, depth, rough):
    planes, rows, width = medium.shape[1:]
    index = lax.axis_index("space")
    size = lax.axis_size("space") + REACH
    plane = (rows + 2 * PAD, width)
    state = (6, planes) + plane
    held = (6, planes + 1) + plane
    scale = (planes, rows, width)
    hbm = pl.BlockSpec(memory_space=pltpu.HBM)
    columns = pltpu.VMEM((planes, rows), jnp.int32)
    given = (adjoint_source, medium, depth, plane_map)
    chip, adjoint_source, medium, meta = call(
        start_kernel,
        [(6 * rows, width), adjoint_source.shape, medium.shape, (PAD, width)],
        [(6,) + plane, columns, columns, pltpu.SemaphoreType.DMA((2 * planes + 2,))],
        tuple(pltpu.with_memory_space_constraint(a, pltpu.HBM) for a in given),
        in_specs=[hbm] * 4,
    )
    chip = chip_swap(chip)
    pair, chip_one, chip_two = call(
        follow_kernel,
        [(14 * rows + PAD, width), (4 * rows + PAD, width), (4 * rows, width)],
        [scale, state, state, held],
        (adjoint_source, medium, meta),
    )
    chip_one = chip_swap(chip_one)
    chip_two = chip_swap(chip_two)
    pair = core_swap(pair)

    here = index.astype(jnp.float32)
    levels = depth[0].astype(jnp.float32)
    owners = plane_map.astype(jnp.float32)
    position = lax.broadcasted_iota(jnp.int32, (planes, rows, width), 2).astype(jnp.float32)
    outside = float(size)
    owner = jnp.where(position < levels[:, :, None], (owners - here)[:, :, None], outside)
    below = jnp.where(lax.rem(index, 2) == 1, pair[14 * rows :], chip_one[4 * rows :])
    edge = jnp.where(position[0] < below[0, :rows, None], (below[1, :rows] - here)[:, None], outside)
    first, scales, extra = call(
        early_kernel,
        [state, scale, (16, rows, width)],
        [state, held, (6,) + plane, (6,) + plane, (6,) + plane],
        (adjoint_source, medium, pair, chip),
    )
    middle, curls, moment = call(
        middle_kernel,
        [state, held, (3, planes) + plane],
        [state],
        (adjoint_source, medium, forward_field, pair, chip_one, first, scales, extra),
    )
    send, stay = call(
        window_kernel,
        [(REACH + 1, rows // 2, width), (REACH + 1, rows // 2, width)],
        [(6, 2) + plane, state, (3, planes) + plane, (2 * REACH + 2, rows, width)],
        (adjoint_source, medium, forward_field, owner, edge, pair, chip_two, middle, curls, scales, extra, moment),
    )
    total = sum_over_groups(gather_owned(send, stay))
    return transposed_smooth(total[None], rough)


def solution(mesh):
    in_specs = (
        P("src", None, "space", None, None),
        P("src", None, "space", None, None),
        P(None, "space", None, None),
        P("space", None),
        P("src", "space", None),
        P(None, "space", None, None),
    )
    out_specs = P("space", None, None)
    return jax.shard_map(slab, mesh=mesh, in_specs=in_specs, out_specs=out_specs, check_vma=False)
```

```python
import functools

import jax
import jax.numpy as jnp
from jax import lax
from jax.experimental import pallas as pl
from jax.experimental.pallas import tpu as pltpu
from jax.sharding import PartitionSpec as P


REACH = 2

sweep_steps = (0.323, 1.658, 0.422, 0.752)

PAD = 8
ROWS = 16


def lane_of(width):
    return lax.broadcasted_iota(jnp.int32, (ROWS, width), 1)


def ahead(value, lane):
    width = value.shape[-1]
    return jnp.where(lane == width - 1, 0.0, pltpu.roll(value, width - 1, 1))


def behind(value, lane):
    return jnp.where(lane == 0, 0.0, pltpu.roll(value, 1, 1))


def rows_at(ref, index, row, shift=0):
    return ref[index + (pl.ds(PAD + row + shift, ROWS), slice(None))]


def put(ref, index, row, value):
    ref[index + (pl.ds(PAD + row, ROWS), slice(None))] = value


def clear_pads(ref):
    rows = ref.shape[-2]
    lead = ref.shape[:-2]
    zero = jnp.zeros((PAD, ref.shape[-1]), jnp.float32)
    for flat in range(functools.reduce(lambda a, b: a * b, lead, 1)):
        index = []
        rest = flat
        for size in reversed(lead):
            index.insert(0, rest % size)
            rest //= size
        ref[tuple(index) + (pl.ds(0, PAD), slice(None))] = zero
        ref[tuple(index) + (pl.ds(rows - PAD, PAD), slice(None))] = zero


def chunks(total):
    return range(0, total, ROWS)


def curl(field, ahead_of, lane):
    out = []
    for part in (0, 3):
        ex, ey, ez = field(part, 0), field(part + 1, 0), field(part + 2, 0)
        hx = (field(part + 2, 1) - ez) - (ahead(ey, lane) - ey)
        hy = (ahead(ex, lane) - ex) - (ahead_of(part + 2) - ez)
        hz = (ahead_of(part + 1) - ey) - (field(part, 1) - ex)
        out += [hx, hy, hz]
    return out


def curl_back(held, before, lane):
    out = []
    for part in (0, 3):
        hx, hy, hz = held(part, 0), held(part + 1, 0), held(part + 2, 0)
        ox = (behind(hy, lane) - hy) - (held(part + 2, -1) - hz)
        oy = (before(part + 2) - hz) - (behind(hx, lane) - hx)
        oz = (held(part, -1) - hx) - (before(part + 1) - hy)
        out += [ox, oy, oz]
    return out


def updated(center, image, source, real, imag, scale):
    out = []
    for c in range(3):
        applied = image[c] + real * center[c] - imag * center[c + 3]
        out.append(center[c] + scale * (source[c] - applied))
    for c in range(3):
        applied = image[c + 3] + real * center[c + 3] + imag * center[c]
        out.append(center[c + 3] + scale * (source[c + 3] - applied))
    return out


def edge_sums(field, lane):
    out = []
    for part in (0, 3):
        ex = field(part, 0)
        out.append(field(part + 1, 0) + (field(part, 1) - ex))
        out.append(field(part + 2, 0) + (ahead(ex, lane) - ex))
    return out


def sweep_slab(state, held, result, source_ref, medium_ref, scale_ref, weight, low, high, first_scale, planes, rows, lane, wanted=None):
    wanted = range(planes) if wanted is None else wanted
    needed = sorted({i for w in wanted for i in (w - 1, w)})
    for i in needed:
        for row in chunks(rows):
            if i < 0:
                for part in (0, 3):
                    gy, gz = low(part, row)
                    ey, ez = rows_at(state, (part + 1, 0), row), rows_at(state, (part + 2, 0), row)
                    put(held, (part + 1, 0), row, first_scale * (gz - ez))
                    put(held, (part + 2, 0), row, first_scale * (ey - gy))
                continue

            def ahead_of(c, i=i, row=row):
                if i + 1 < planes:
                    return rows_at(state, (c, i + 1), row)
                return high(c, row)

            values = curl(lambda c, s: rows_at(state, (c, i), row, s), ahead_of, lane)
            for c in range(6):
                put(held, (c, i + 1), row, values[c])
    for i in wanted:
        for row in chunks(rows):
            image = curl_back(
                lambda c, s: rows_at(held, (c, i + 1), row, s), lambda c: rows_at(held, (c, i), row), lane
            )
            here = pl.ds(row, ROWS)
            new = updated(
                [rows_at(state, (c, i), row) for c in range(6)],
                image,
                [source_ref[0, c, i, here, :] for c in range(6)],
                medium_ref[0, i, here, :],
                medium_ref[1, i, here, :],
                weight * scale_ref[i, here, :],
            )
            for c in range(6):
                put(result, (c, i), row, new[c])


def first_sweep(source_ref, medium_ref, scale_ref, state, i, rows):
    for row in chunks(rows):
        here = pl.ds(row, ROWS)
        scale = 1.0 / (4.0 + medium_ref[0, i, here, :])
        scale_ref[i, here, :] = scale
        for c in range(6):
            put(state, (c, i), row, sweep_steps[0] * scale * source_ref[0, c, i, here, :])


def parity_and_ends():
    index = lax.axis_index("space")
    odd = lax.rem(index, 2) == 1
    first_scale = jnp.where(index == 0, 0.0, 1.0)
    last_scale = jnp.where(index == lax.axis_size("space") - 1, 0.0, 1.0)
    return odd, first_scale, last_scale


def emit_level(emit, first, state, planes, rows, lane):
    for row in chunks(rows):
        sums = edge_sums(lambda c, s: rows_at(state, (c, planes - 1), row, s), lane)
        bottom = [rows_at(state, (c, 0), row) for c in (1, 2, 4, 5)]
        for k in range(4):
            emit(first + k, row, bottom[k], sums[k])


def message_rows(slot, row, rows):
    return pl.ds(slot * rows + row, ROWS)


def no_plane(c, row):
    return 0.0


def no_sums(part, row):
    return 0.0, 0.0


def start_kernel(
    source_hbm, medium_hbm, depth_hbm, map_hbm, chip_ref, source_ref, medium_ref, scale_ref, two, pair_ref,
    one, held, levels, owners, sems,
):
    planes, rows, width = medium_ref.shape[1:]
    lane = lane_of(width)
    odd, first_scale, _ = parity_and_ends()
    copies = []
    for i in range(planes):
        copies.append(pltpu.make_async_copy(medium_hbm.at[:, i], medium_ref.at[:, i], sems.at[2 * i]))
        copies.append(pltpu.make_async_copy(source_hbm.at[0, :, i], source_ref.at[0, :, i], sems.at[2 * i + 1]))
    columns = [
        pltpu.make_async_copy(depth_hbm.at[0], levels, sems.at[2 * planes]),
        pltpu.make_async_copy(map_hbm, owners, sems.at[2 * planes + 1]),
    ]
    for copy in copies + columns:
        copy.start()
    for ref in (one, two, held):
        clear_pads(ref)

    def emit(slot, row, below, above):
        here = message_rows(slot, row, rows)
        pair_ref[here, :] = jnp.where(odd, below, above)
        chip_ref[here, :] = jnp.where(odd, above, below)

    last = planes - 1
    for i in range(planes):
        copies[2 * i].wait()
        copies[2 * i + 1].wait()
        first_sweep(source_ref, medium_ref, scale_ref, one, i, rows)
    for row in chunks(rows):
        here = pl.ds(row, ROWS)
        for k in range(2):
            emit(4 + k, row, medium_ref[k, 0, here, :], medium_ref[k, last, here, :])
    emit_level(emit, 0, one, planes, rows, lane)
    sweep_slab(
        one, held, two, source_ref, medium_ref, scale_ref, sweep_steps[1], no_sums, no_plane, first_scale,
        planes, rows, lane,
    )
    emit_level(emit, 6, two, planes, rows, lane)
    for copy in columns:
        copy.wait()
    for ref in (pair_ref, chip_ref):
        ref[pl.ds(10 * rows, PAD), :] = jnp.zeros((PAD, width), jnp.float32)
        ref[pl.ds(10 * rows, 1), pl.ds(0, rows)] = levels[pl.ds(last, 1), :].astype(jnp.float32)
        ref[pl.ds(10 * rows + 1, 1), pl.ds(0, rows)] = owners[pl.ds(last, 1), :].astype(jnp.float32)


def follow_kernel(source_ref, medium_ref, scale_ref, two, pair_in_ref, chip_ref, pair_ref, one, held):
    planes, rows, width = medium_ref.shape[1:]
    lane = lane_of(width)
    odd, first_scale, _ = parity_and_ends()
    clear_pads(one)
    clear_pads(held)
    sweep_slab(
        two, held, one, source_ref, medium_ref, scale_ref, sweep_steps[2], no_sums, no_plane, first_scale,
        planes, rows, lane, wanted=sorted({0, planes - 1}),
    )

    def emit(slot, row, below, above):
        here = message_rows(slot, row, rows)
        pair_ref[here, :] = jnp.where(odd, below, above)
        chip_ref[here, :] = jnp.where(odd, above, below)

    emit_level(emit, 0, one, planes, rows, lane)
    pair_ref[pl.ds(4 * rows, 10 * rows + PAD), :] = pair_in_ref[...]


def readers(odd, pair_ref, pair_first, chip_ref, chip_first, rows):
    def both(slot, row):
        pair = pair_ref[message_rows(pair_first + slot, row, rows), :]
        chip = chip_ref[message_rows(chip_first + slot, row, rows), :]
        return pair, chip

    def from_below(slot, row):
        pair, chip = both(slot, row)
        return jnp.where(odd, pair, chip)

    def from_above(slot, row):
        pair, chip = both(slot, row)
        return jnp.where(odd, chip, pair)

    return from_below, from_above


WHERE_YZ = {1: 0, 2: 1, 4: 2, 5: 3}


def moments(saved_ref, state, moment_ref, i, rows, lane):
    for row in chunks(rows):
        here = pl.ds(row, ROWS)
        for c in range(3):
            real = saved_ref[0, c, i, here, :].astype(jnp.float32)
            imag = saved_ref[0, c + 3, i, here, :].astype(jnp.float32)
            value = real * rows_at(state, (c + 3, i), row) + imag * rows_at(state, (c, i), row)
            if c < 2:
                value = value + ahead(value, lane)
            put(moment_ref, (c, i), row, value)


def middle_kernel(
    source_ref, medium_ref, saved_ref, scale_ref, pair_ref, chip_ref,
    state_ref, held, extra_ref, moment_ref, one, two, delta_low, delta_high, delta_two,
):
    planes, rows, width = medium_ref.shape[1:]
    lane = lane_of(width)
    odd, first_scale, last_scale = parity_and_ends()
    for ref in (one, two, state_ref, held, delta_low, delta_high, delta_two, moment_ref):
        clear_pads(ref)
    for i in range(planes):
        for row in chunks(rows):
            here = pl.ds(row, ROWS)
            scale = sweep_steps[0] * scale_ref[i, here, :]
            for c in range(6):
                put(one, (c, i), row, scale * source_ref[0, c, i, here, :])
    from_below, from_above = readers(odd, pair_ref, 4, chip_ref, 0, rows)

    for row in chunks(rows):
        sums = edge_sums(lambda c, s: rows_at(one, (c, planes - 1), row, s), lane)
        scale = (sweep_steps[1] * last_scale) / (4.0 + from_above(4, row))
        for k, c in enumerate((1, 2, 4, 5)):
            put(delta_high, (c,), row, scale * sums[k])
        scale = sweep_steps[1] / (4.0 + from_below(4, row))
        for part in (0, 3):
            ey, ez = rows_at(one, (part + 1, 0), row), rows_at(one, (part + 2, 0), row)
            put(delta_low, (part + 1,), row, scale * ey)
            put(delta_low, (part + 2,), row, scale * ez)
            put(delta_low, (part,), row, scale * ((behind(ez, lane) - ez) + (rows_at(one, (part + 1, 0), row, -1) - ey)))

    sweep_slab(
        one, held, two, source_ref, medium_ref, scale_ref, sweep_steps[1],
        lambda part, row: (from_below(2 * (part // 3), row), from_below(2 * (part // 3) + 1, row)),
        lambda c, row: from_above(WHERE_YZ[c], row),
        first_scale, planes, rows, lane,
    )

    none = [0.0] * 6
    for row in chunks(rows):
        values = curl(lambda c, s: rows_at(delta_low, (c,), row, s), lambda c: rows_at(two, (c, 0), row), lane)
        for c in range(6):
            put(held, (c, 0), row, values[c])
    for row in chunks(rows):
        before = {1: -rows_at(delta_low, (2,), row), 2: rows_at(delta_low, (1,), row),
                  4: -rows_at(delta_low, (5,), row), 5: rows_at(delta_low, (4,), row)}
        image = curl_back(lambda c, s: rows_at(held, (c, 0), row, s), lambda c: before[c], lane)
        real, imag = from_below(4, row), from_below(5, row)
        new = updated(
            [rows_at(delta_low, (c,), row) for c in range(6)], image, none, real, imag, sweep_steps[2] / (4.0 + real)
        )
        for c in range(6):
            put(delta_two, (c,), row, new[c])
    for row in chunks(rows):
        for level, deltas in enumerate((delta_low, delta_two)):
            sums = edge_sums(lambda c, s: rows_at(deltas, (c,), row, s), lane)
            for k in range(4):
                extra_ref[8 * level + k, pl.ds(row, ROWS), :] = sums[k]
        for k, c in enumerate((1, 2, 4, 5)):
            extra_ref[4 + k, pl.ds(row, ROWS), :] = rows_at(delta_high, (c,), row)
    for row in chunks(rows):
        for part in (0, 3):
            ey, ez = rows_at(delta_high, (part + 1,), row), rows_at(delta_high, (part + 2,), row)
            put(held, (part, 1), row, (rows_at(delta_high, (part + 2,), row, 1) - ez) - (ahead(ey, lane) - ey))
    for row in chunks(rows):
        here = pl.ds(row, ROWS)
        sums = edge_sums(lambda c, s: rows_at(two, (c, planes - 1), row, s), lane)
        real, imag = from_above(4, row), from_above(5, row)
        scale = (sweep_steps[2] * last_scale) / (4.0 + real)
        center, image = {}, {}
        for part in (0, 3):
            ey, ez = rows_at(delta_high, (part + 1,), row), rows_at(delta_high, (part + 2,), row)
            hx = rows_at(held, (part, 1), row)
            k = 2 * (part // 3)
            center[part + 1], center[part + 2] = ey, ez
            image[part + 1] = 2.0 * ey - sums[k] - (behind(hx, lane) - hx)
            image[part + 2] = (rows_at(held, (part, 1), row, -1) - hx) - sums[k + 1] + 2.0 * ez
        for k, c in enumerate((1, 2)):
            extra_ref[12 + k, here, :] = center[c] - scale * (image[c] + real * center[c] - imag * center[c + 3])
            extra_ref[14 + k, here, :] = center[c + 3] - scale * (
                image[c + 3] + real * center[c + 3] + imag * center[c]
            )

    below_one, above_one = readers(odd, pair_ref, 10, chip_ref, 6, rows)

    def low(part, row):
        k = 2 * (part // 3)
        here = pl.ds(row, ROWS)
        return below_one(k, row) + extra_ref[k, here, :], below_one(k + 1, row) + extra_ref[k + 1, here, :]

    def high(c, row):
        return above_one(WHERE_YZ[c], row) + extra_ref[4 + WHERE_YZ[c], pl.ds(row, ROWS), :]

    sweep_slab(
        two, held, state_ref, source_ref, medium_ref, scale_ref, sweep_steps[2], low, high, first_scale,
        planes, rows, lane,
    )
    inner = range(1, planes - 1)
    sweep_slab(
        state_ref, held, one, source_ref, medium_ref, scale_ref, sweep_steps[3], None, None, first_scale,
        planes, rows, lane, wanted=inner,
    )
    for i in inner:
        moments(saved_ref, one, moment_ref, i, rows, lane)


def window_kernel(
    source_ref, medium_ref, saved_ref, owner_ref, edge_ref, pair_ref, chip_ref, state_ref, held_ref, scale_ref,
    extra_ref, moment_in_ref, send_ref, stay_ref, held, two, moment, window,
):
    planes, rows, width = medium_ref.shape[1:]
    lane = lane_of(width)
    odd, first_scale, _ = parity_and_ends()
    from_below, from_above = readers(odd, pair_ref, 0, chip_ref, 0, rows)
    clear_pads(held)
    clear_pads(moment)
    ends = sorted({0, planes - 1})

    for row in chunks(rows):
        here = pl.ds(row, ROWS)
        for part in (0, 3):
            k = 2 * (part // 3)
            ey, ez = rows_at(state_ref, (part + 1, 0), row), rows_at(state_ref, (part + 2, 0), row)
            gy = from_below(k, row) + extra_ref[8 + k, here, :]
            gz = from_below(k + 1, row) + extra_ref[9 + k, here, :]
            put(held, (part + 1, 0), row, first_scale * (gz - ez))
            put(held, (part + 2, 0), row, first_scale * (ey - gy))
        values = curl(
            lambda c, s: rows_at(state_ref, (c, planes - 1), row, s),
            lambda c: from_above(WHERE_YZ[c], row) + extra_ref[12 + WHERE_YZ[c], here, :],
            lane,
        )
        for c in range(6):
            put(held, (c, 1), row, values[c])
    for i in ends:
        for row in chunks(rows):
            here = pl.ds(row, ROWS)
            if i == planes - 1:
                now = lambda c, s: rows_at(held, (c, 1), row, s)
            else:
                now = lambda c, s: rows_at(held_ref, (c, i + 1), row, s)
            if i == 0:
                before = lambda c: rows_at(held, (c, 0), row)
            else:
                before = lambda c: rows_at(held_ref, (c, i), row)
            image = curl_back(now, before, lane)
            real, imag = medium_ref[0, i, here, :], medium_ref[1, i, here, :]
            new = updated(
                [rows_at(state_ref, (c, i), row) for c in range(6)], image,
                [source_ref[0, c, i, here, :] for c in range(6)], real, imag, sweep_steps[3] * scale_ref[i, here, :],
            )
            for c in range(6):
                put(two, (c, i), row, new[c])
        moments(saved_ref, two, moment, i, rows, lane)

    def moment_rows(c, i, row, shift=0):
        return rows_at(moment if i in ends else moment_in_ref, (c, i), row, shift)

    for row in chunks(rows):
        here = pl.ds(row, ROWS)
        sums = [0.0] * (2 * REACH + 2)

        def add(value, offset, low):
            for k in range(2 * REACH + 1):
                slot = k + low
                sums[slot] = sums[slot] + jnp.where(offset == float(slot - REACH - 1), value, 0.0)

        def side(i):
            return moment_rows(1, i, row) + (moment_rows(2, i, row) + moment_rows(2, i, row, 1))

        lower = side(0)
        add(lower, edge_ref[here, :], 0)
        for i in range(planes):
            cell = moment_rows(0, i, row) + moment_rows(0, i, row, 1) + lower
            if i + 1 < planes:
                lower = side(i + 1)
                cell = cell + lower
            add(cell, owner_ref[i, here, :], 1)
        for k in range(2 * REACH + 2):
            window[k, here, :] = sums[k]
    for k in range(2 * REACH + 2):
        both = 0.25 * (window[k, pl.ds(0, rows // 2, stride=2), :] + window[k, pl.ds(1, rows // 2, stride=2), :])
        if k % 2 == 0:
            send_ref[k // 2] = both
        else:
            stay_ref[k // 2] = both


def vmem():
    return pl.BlockSpec(memory_space=pltpu.VMEM)


def call(kernel, out_shape, scratch, arguments, in_specs=None, limit=24 << 20, flops=1 << 20):
    return pl.pallas_call(
        kernel,
        out_shape=[jax.ShapeDtypeStruct(s, jnp.float32) for s in out_shape],
        in_specs=in_specs or [vmem()] * len(arguments),
        out_specs=[vmem()] * len(out_shape),
        scratch_shapes=[s if not isinstance(s, tuple) else pltpu.VMEM(s, jnp.float32) for s in scratch],
        compiler_params=pltpu.CompilerParams(vmem_limit_bytes=limit),
        cost_estimate=pl.CostEstimate(flops=flops, bytes_accessed=1 << 20, transcendentals=0),
    )(*arguments)


def core_swap(value):
    size = lax.axis_size("space")
    return lax.ppermute(value, "space", [(i, i ^ 1) for i in range(size)])


def chip_swap(value):
    size = lax.axis_size("space")
    pairs = []
    for i in range(1, size - 1, 2):
        pairs += [(i, i + 1), (i + 1, i)]
    return lax.ppermute(value, "space", pairs)


def sum_over_groups(value):
    size = lax.axis_size("src")
    if size & (size - 1):
        return lax.psum(value, "src")
    step = 1
    while step < size:
        value = value + lax.ppermute(value, "src", [(i, i ^ step) for i in range(size)])
        step *= 2
    return value


def gather_owned(send, stay):
    size = lax.axis_size("space")
    index = lax.axis_index("space")
    odd = lax.rem(index, 2) == 1
    other = core_swap(send)
    below = stay[0] + jnp.where(odd, other[1], other[0])
    here = stay[1] + jnp.where(odd, other[2], other[1])
    above = stay[2] + jnp.where(odd, 0.0, other[2])
    chip = index // 2
    upward = lax.rem(chip, 2) == 0
    chips = size // 2
    inner, outer = [], []
    for c in range(chips):
        for core in range(2):
            if c ^ 1 < chips:
                inner.append((2 * c + core, 2 * (c ^ 1) + core))
            partner = ((c + 1) ^ 1) - 1
            if 0 <= partner < chips:
                outer.append((2 * c + core, 2 * partner + core))
    from_inner = lax.ppermute(jnp.where(upward, above, below), "space", inner)
    from_outer = lax.ppermute(jnp.where(upward, below, above), "space", outer)
    from_far = lax.ppermute(other[0], "space", [(i, i - 4) for i in range(5, size, 2)])
    return here + from_inner + from_outer + from_far


def transposed_smooth(summed, rough):
    rows_in = summed.shape[-2]
    depth_in = summed.shape[-1]
    total = jnp.zeros_like(summed)
    for vertical in range(3):
        for lateral in range(3):
            product = rough[vertical * 3 + lateral] * summed
            padded = jnp.pad(product, ((0, 0), (1, 1), (1, 1)))
            total = (
                total
                + padded[
                    :, 2 - vertical : 2 - vertical + rows_in, 2 - lateral : 2 - lateral + depth_in
                ]
            )
    return total


def slab(adjoint_source, forward_field, medium, plane_map, depth, rough):
    planes, rows, width = medium.shape[1:]
    index = lax.axis_index("space")
    size = lax.axis_size("space") + REACH
    plane = (rows + 2 * PAD, width)
    state = (6, planes) + plane
    held = (6, planes + 1) + plane
    scale = (planes, rows, width)
    hbm = pl.BlockSpec(memory_space=pltpu.HBM)
    columns = pltpu.VMEM((planes, rows), jnp.int32)
    given = (adjoint_source, medium, depth, plane_map)
    first_message, last_message = (10 * rows + PAD, width), (4 * rows, width)
    chip_one, adjoint_source, medium, scales, own, pair = call(
        start_kernel,
        [first_message, adjoint_source.shape, medium.shape, scale, state, first_message],
        [state, held, columns, columns, pltpu.SemaphoreType.DMA((2 * planes + 2,))],
        tuple(pltpu.with_memory_space_constraint(a, pltpu.HBM) for a in given),
        in_specs=[hbm] * 4,
    )
    chip_one = chip_swap(chip_one)
    chip_two, pair = call(
        follow_kernel,
        [last_message, (14 * rows + PAD, width)],
        [state, held],
        (adjoint_source, medium, scales, own, pair),
    )
    pair = core_swap(pair)
    chip_two = chip_swap(chip_two)

    here = index.astype(jnp.float32)
    levels = depth[0].astype(jnp.float32)
    owners = plane_map.astype(jnp.float32)
    position = lax.broadcasted_iota(jnp.int32, (planes, rows, width), 2).astype(jnp.float32)
    outside = float(size)
    owner = jnp.where(position < levels[:, :, None], (owners - here)[:, :, None], outside)
    below = jnp.where(lax.rem(index, 2) == 1, pair[14 * rows :], chip_one[10 * rows :])
    edge = jnp.where(position[0] < below[0, :rows, None], (below[1, :rows] - here)[:, None], outside)
    middle, curls, extra, moment = call(
        middle_kernel,
        [state, held, (16, rows, width), (3, planes) + plane],
        [state, state, (6,) + plane, (6,) + plane, (6,) + plane],
        (adjoint_source, medium, forward_field, scales, pair, chip_one),
    )
    send, stay = call(
        window_kernel,
        [(REACH + 1, rows // 2, width), (REACH + 1, rows // 2, width)],
        [(6, 2) + plane, state, (3, planes) + plane, (2 * REACH + 2, rows, width)],
        (adjoint_source, medium, forward_field, owner, edge, pair, chip_two, middle, curls, scales, extra, moment),
    )
    total = sum_over_groups(gather_owned(send, stay))
    return transposed_smooth(total[None], rough)


def solution(mesh):
    in_specs = (
        P("src", None, "space", None, None),
        P("src", None, "space", None, None),
        P(None, "space", None, None),
        P("space", None),
        P("src", "space", None),
        P(None, "space", None, None),
    )
    out_specs = P("space", None, None)
    return jax.shard_map(slab, mesh=mesh, in_specs=in_specs, out_specs=out_specs, check_vma=False)
```

```python
import functools

import jax
import jax.numpy as jnp
from jax import lax
from jax.experimental import pallas as pl
from jax.experimental.pallas import tpu as pltpu
from jax.sharding import PartitionSpec as P


REACH = 2

sweep_steps = (0.323, 1.658, 0.422, 0.752)

PAD = 8
ROWS = 16


def lane_of(width):
    return lax.broadcasted_iota(jnp.int32, (ROWS, width), 1)


def ahead(value, lane):
    width = value.shape[-1]
    return jnp.where(lane == width - 1, 0.0, pltpu.roll(value, width - 1, 1))


def behind(value, lane):
    return jnp.where(lane == 0, 0.0, pltpu.roll(value, 1, 1))


def rows_at(ref, index, row, shift=0):
    return ref[index + (pl.ds(PAD + row + shift, ROWS), slice(None))]


def put(ref, index, row, value):
    ref[index + (pl.ds(PAD + row, ROWS), slice(None))] = value


def clear_pads(ref):
    rows = ref.shape[-2]
    lead = ref.shape[:-2]
    zero = jnp.zeros((PAD, ref.shape[-1]), jnp.float32)
    for flat in range(functools.reduce(lambda a, b: a * b, lead, 1)):
        index = []
        rest = flat
        for size in reversed(lead):
            index.insert(0, rest % size)
            rest //= size
        ref[tuple(index) + (pl.ds(0, PAD), slice(None))] = zero
        ref[tuple(index) + (pl.ds(rows - PAD, PAD), slice(None))] = zero


def chunks(total):
    return range(0, total, ROWS)


def curl(field, ahead_of, lane):
    out = []
    for part in (0, 3):
        ex, ey, ez = field(part, 0), field(part + 1, 0), field(part + 2, 0)
        hx = (field(part + 2, 1) - ez) - (ahead(ey, lane) - ey)
        hy = (ahead(ex, lane) - ex) - (ahead_of(part + 2) - ez)
        hz = (ahead_of(part + 1) - ey) - (field(part, 1) - ex)
        out += [hx, hy, hz]
    return out


def curl_back(held, before, lane):
    out = []
    for part in (0, 3):
        hx, hy, hz = held(part, 0), held(part + 1, 0), held(part + 2, 0)
        ox = (behind(hy, lane) - hy) - (held(part + 2, -1) - hz)
        oy = (before(part + 2) - hz) - (behind(hx, lane) - hx)
        oz = (held(part, -1) - hx) - (before(part + 1) - hy)
        out += [ox, oy, oz]
    return out


def updated(center, image, base, ratio, real, imag, scale):
    out = []
    for c in range(3):
        applied = image[c] + real * center[c] - imag * center[c + 3]
        out.append(center[c] + ratio * base[c] - scale * applied)
    for c in range(3):
        applied = image[c + 3] + real * center[c + 3] + imag * center[c]
        out.append(center[c + 3] + ratio * base[c + 3] - scale * applied)
    return out


def edge_sums(field, lane):
    out = []
    for part in (0, 3):
        ex = field(part, 0)
        out.append(field(part + 1, 0) + (field(part, 1) - ex))
        out.append(field(part + 2, 0) + (ahead(ex, lane) - ex))
    return out


def sweep_slab(state, held, result, base, medium_ref, scale_ref, weight, low, high, first_scale, planes, rows, lane, wanted=None):
    wanted = range(planes) if wanted is None else wanted
    needed = sorted({i for w in wanted for i in (w - 1, w)})
    for i in needed:
        for row in chunks(rows):
            if i < 0:
                for part in (0, 3):
                    gy, gz = low(part, row)
                    ey, ez = rows_at(state, (part + 1, 0), row), rows_at(state, (part + 2, 0), row)
                    put(held, (part + 1, 0), row, first_scale * (gz - ez))
                    put(held, (part + 2, 0), row, first_scale * (ey - gy))
                continue

            def ahead_of(c, i=i, row=row):
                if i + 1 < planes:
                    return rows_at(state, (c, i + 1), row)
                return high(c, row)

            values = curl(lambda c, s: rows_at(state, (c, i), row, s), ahead_of, lane)
            for c in range(6):
                put(held, (c, i + 1), row, values[c])
    for i in wanted:
        for row in chunks(rows):
            image = curl_back(
                lambda c, s: rows_at(held, (c, i + 1), row, s), lambda c: rows_at(held, (c, i), row), lane
            )
            here = pl.ds(row, ROWS)
            new = updated(
                [rows_at(state, (c, i), row) for c in range(6)],
                image,
                [rows_at(base, (c, i), row) for c in range(6)],
                weight / sweep_steps[0],
                medium_ref[0, i, here, :],
                medium_ref[1, i, here, :],
                weight * scale_ref[i, here, :],
            )
            for c in range(6):
                put(result, (c, i), row, new[c])


def first_sweep(fields, medium_ref, scale_ref, state, i, rows):
    for row in chunks(rows):
        here = pl.ds(row, ROWS)
        scale = 1.0 / (4.0 + medium_ref[0, i, here, :])
        scale_ref[i, here, :] = scale
        for c in range(6):
            put(state, (c, i), row, sweep_steps[0] * scale * fields[c, i, here, :])


def parity_and_ends():
    index = lax.axis_index("space")
    odd = lax.rem(index, 2) == 1
    first_scale = jnp.where(index == 0, 0.0, 1.0)
    last_scale = jnp.where(index == lax.axis_size("space") - 1, 0.0, 1.0)
    return odd, first_scale, last_scale


def emit_level(emit, first, state, planes, rows, lane):
    for row in chunks(rows):
        sums = edge_sums(lambda c, s: rows_at(state, (c, planes - 1), row, s), lane)
        bottom = [rows_at(state, (c, 0), row) for c in (1, 2, 4, 5)]
        for k in range(4):
            emit(first + k, row, bottom[k], sums[k])


def message_rows(slot, row, rows):
    return pl.ds(slot * rows + row, ROWS)


def start_kernel(
    source_hbm, medium_hbm, depth_hbm, map_hbm, chip_ref, medium_ref, scale_ref, one, meta_ref,
    fields, levels, owners, sems,
):
    planes, rows, width = medium_ref.shape[1:]
    lane = lane_of(width)
    odd = parity_and_ends()[0]
    last = planes - 1
    order = [last, 0] + list(range(1, last))
    copies = []
    for i in order:
        copies.append(pltpu.make_async_copy(medium_hbm.at[:, i], medium_ref.at[:, i], sems.at[2 * i]))
        copies.append(pltpu.make_async_copy(source_hbm.at[0, :, i], fields.at[:, i], sems.at[2 * i + 1]))
    columns = [
        pltpu.make_async_copy(depth_hbm.at[0], levels, sems.at[2 * planes]),
        pltpu.make_async_copy(map_hbm, owners, sems.at[2 * planes + 1]),
    ]
    for copy in copies + columns:
        copy.start()
    clear_pads(one)
    meta_ref[...] = jnp.zeros_like(meta_ref)

    def emit(slot, row, below, above):
        chip_ref[message_rows(slot, row, rows), :] = jnp.where(odd, above, below)

    for k, i in enumerate(order):
        copies[2 * k].wait()
        copies[2 * k + 1].wait()
        first_sweep(fields, medium_ref, scale_ref, one, i, rows)
        if k == 1:
            emit_level(emit, 0, one, planes, rows, lane)
            for row in chunks(rows):
                here = pl.ds(row, ROWS)
                for part in range(2):
                    emit(4 + part, row, medium_ref[part, 0, here, :], medium_ref[part, last, here, :])
    for copy in columns:
        copy.wait()
    meta_ref[pl.ds(0, 1), pl.ds(0, rows)] = levels[pl.ds(last, 1), :].astype(jnp.float32)
    meta_ref[pl.ds(1, 1), pl.ds(0, rows)] = owners[pl.ds(last, 1), :].astype(jnp.float32)
    chip_ref[pl.ds(6 * rows, PAD), :] = meta_ref[...]


def no_plane(c, row):
    return 0.0


def no_sums(part, row):
    return 0.0, 0.0


def follow_kernel(medium_ref, scale_ref, one, meta_ref, chip_ref, pair_ref, two, three, held):
    planes, rows, width = medium_ref.shape[1:]
    lane = lane_of(width)
    odd, first_scale, _ = parity_and_ends()
    clear_pads(two)
    clear_pads(three)
    clear_pads(held)

    def emitter(slots, to_chip):
        def emit(slot, row, below, above):
            pair_ref[message_rows(slots + slot, row, rows), :] = jnp.where(odd, below, above)
            if to_chip is not None:
                chip_ref[message_rows(to_chip + slot, row, rows), :] = jnp.where(odd, above, below)

        return emit

    sweep_slab(
        one, held, two, one, medium_ref, scale_ref, sweep_steps[1], no_sums, no_plane, first_scale,
        planes, rows, lane,
    )
    emit_level(emitter(6, 0), 0, two, planes, rows, lane)
    sweep_slab(
        two, held, three, one, medium_ref, scale_ref, sweep_steps[2], no_sums, no_plane, first_scale,
        planes, rows, lane, wanted=sorted({0, planes - 1}),
    )
    emit_level(emitter(10, 4), 0, three, planes, rows, lane)
    emit_level(emitter(0, None), 0, one, planes, rows, lane)
    emit = emitter(4, None)
    for row in chunks(rows):
        for k in range(2):
            here = pl.ds(row, ROWS)
            emit(k, row, medium_ref[k, 0, here, :], medium_ref[k, planes - 1, here, :])
    pair_ref[pl.ds(14 * rows, PAD), :] = meta_ref[...]


def readers(odd, pair_ref, pair_first, chip_ref, chip_first, rows):
    def both(slot, row):
        pair = pair_ref[message_rows(pair_first + slot, row, rows), :]
        chip = chip_ref[message_rows(chip_first + slot, row, rows), :]
        return pair, chip

    def from_below(slot, row):
        pair, chip = both(slot, row)
        return jnp.where(odd, pair, chip)

    def from_above(slot, row):
        pair, chip = both(slot, row)
        return jnp.where(odd, chip, pair)

    return from_below, from_above


WHERE_YZ = {1: 0, 2: 1, 4: 2, 5: 3}


def moments(saved_ref, state, moment_ref, i, rows, lane):
    for row in chunks(rows):
        here = pl.ds(row, ROWS)
        for c in range(3):
            real = saved_ref[0, c, i, here, :].astype(jnp.float32)
            imag = saved_ref[0, c + 3, i, here, :].astype(jnp.float32)
            value = real * rows_at(state, (c + 3, i), row) + imag * rows_at(state, (c, i), row)
            if c < 2:
                value = value + ahead(value, lane)
            put(moment_ref, (c, i), row, value)


def early_kernel(
    medium_ref, scale_ref, one, pair_ref, chip_ref, two, extra_ref, held, delta_low, delta_high, delta_two,
):
    planes, rows, width = medium_ref.shape[1:]
    lane = lane_of(width)
    odd, first_scale, last_scale = parity_and_ends()
    for ref in (two, held, delta_low, delta_high, delta_two):
        clear_pads(ref)
    from_below, from_above = readers(odd, pair_ref, 0, chip_ref, 0, rows)

    for row in chunks(rows):
        sums = edge_sums(lambda c, s: rows_at(one, (c, planes - 1), row, s), lane)
        scale = (sweep_steps[1] * last_scale) / (4.0 + from_above(4, row))
        for k, c in enumerate((1, 2, 4, 5)):
            put(delta_high, (c,), row, scale * sums[k])
        scale = sweep_steps[1] / (4.0 + from_below(4, row))
        for part in (0, 3):
            ey, ez = rows_at(one, (part + 1, 0), row), rows_at(one, (part + 2, 0), row)
            put(delta_low, (part + 1,), row, scale * ey)
            put(delta_low, (part + 2,), row, scale * ez)
            put(delta_low, (part,), row, scale * ((behind(ez, lane) - ez) + (rows_at(one, (part + 1, 0), row, -1) - ey)))

    sweep_slab(
        one, held, two, one, medium_ref, scale_ref, sweep_steps[1],
        lambda part, row: (from_below(2 * (part // 3), row), from_below(2 * (part // 3) + 1, row)),
        lambda c, row: from_above(WHERE_YZ[c], row),
        first_scale, planes, rows, lane,
    )

    none = [0.0] * 6
    for row in chunks(rows):
        values = curl(lambda c, s: rows_at(delta_low, (c,), row, s), lambda c: rows_at(two, (c, 0), row), lane)
        for c in range(6):
            put(held, (c, 0), row, values[c])
    for row in chunks(rows):
        before = {1: -rows_at(delta_low, (2,), row), 2: rows_at(delta_low, (1,), row),
                  4: -rows_at(delta_low, (5,), row), 5: rows_at(delta_low, (4,), row)}
        image = curl_back(lambda c, s: rows_at(held, (c, 0), row, s), lambda c: before[c], lane)
        real, imag = from_below(4, row), from_below(5, row)
        new = updated(
            [rows_at(delta_low, (c,), row) for c in range(6)], image, none, 0.0, real, imag, sweep_steps[2] / (4.0 + real)
        )
        for c in range(6):
            put(delta_two, (c,), row, new[c])
    for row in chunks(rows):
        for level, deltas in enumerate((delta_low, delta_two)):
            sums = edge_sums(lambda c, s: rows_at(deltas, (c,), row, s), lane)
            for k in range(4):
                extra_ref[8 * level + k, pl.ds(row, ROWS), :] = sums[k]
        for k, c in enumerate((1, 2, 4, 5)):
            extra_ref[4 + k, pl.ds(row, ROWS), :] = rows_at(delta_high, (c,), row)
    for row in chunks(rows):
        for part in (0, 3):
            ey, ez = rows_at(delta_high, (part + 1,), row), rows_at(delta_high, (part + 2,), row)
            put(held, (part, 1), row, (rows_at(delta_high, (part + 2,), row, 1) - ez) - (ahead(ey, lane) - ey))
    for row in chunks(rows):
        here = pl.ds(row, ROWS)
        sums = edge_sums(lambda c, s: rows_at(two, (c, planes - 1), row, s), lane)
        real, imag = from_above(4, row), from_above(5, row)
        scale = (sweep_steps[2] * last_scale) / (4.0 + real)
        center, image = {}, {}
        for part in (0, 3):
            ey, ez = rows_at(delta_high, (part + 1,), row), rows_at(delta_high, (part + 2,), row)
            hx = rows_at(held, (part, 1), row)
            k = 2 * (part // 3)
            center[part + 1], center[part + 2] = ey, ez
            image[part + 1] = 2.0 * ey - sums[k] - (behind(hx, lane) - hx)
            image[part + 2] = (rows_at(held, (part, 1), row, -1) - hx) - sums[k + 1] + 2.0 * ez
        for k, c in enumerate((1, 2)):
            extra_ref[12 + k, here, :] = center[c] - scale * (image[c] + real * center[c] - imag * center[c + 3])
            extra_ref[14 + k, here, :] = center[c + 3] - scale * (
                image[c + 3] + real * center[c + 3] + imag * center[c]
            )


def last_kernel(
    base_ref, medium_ref, saved_ref, scale_ref, owner_ref, edge_ref, pair_ref, chip_ref, one, extra_ref,
    send_ref, stay_ref, two, three, held, moment, window,
):
    planes, rows, width = medium_ref.shape[1:]
    lane = lane_of(width)
    odd, first_scale, _ = parity_and_ends()
    for ref in (two, held, moment):
        clear_pads(ref)

    def sweep_with(level, state, result):
        from_below, from_above = readers(odd, pair_ref, 2 + 4 * level, chip_ref, 4 * level - 4, rows)
        first = 8 * level - 8

        def low(part, row):
            k = 2 * (part // 3)
            here = pl.ds(row, ROWS)
            below = from_below(k, row) + extra_ref[first + k, here, :]
            return below, from_below(k + 1, row) + extra_ref[first + k + 1, here, :]

        def high(c, row):
            return from_above(WHERE_YZ[c], row) + extra_ref[first + 4 + WHERE_YZ[c], pl.ds(row, ROWS), :]

        sweep_slab(
            state, held, result, base_ref, medium_ref, scale_ref, sweep_steps[level + 1], low, high, first_scale,
            planes, rows, lane,
        )

    sweep_with(1, one, two)
    sweep_with(2, two, three)
    for i in range(planes):
        moments(saved_ref, three, moment, i, rows, lane)

    def moment_rows(c, i, row, shift=0):
        return rows_at(moment, (c, i), row, shift)

    for row in chunks(rows):
        here = pl.ds(row, ROWS)
        sums = [0.0] * (2 * REACH + 2)

        def add(value, offset, low):
            for k in range(2 * REACH + 1):
                slot = k + low
                sums[slot] = sums[slot] + jnp.where(offset == float(slot - REACH - 1), value, 0.0)

        def side(i):
            return moment_rows(1, i, row) + (moment_rows(2, i, row) + moment_rows(2, i, row, 1))

        lower = side(0)
        add(lower, edge_ref[here, :], 0)
        for i in range(planes):
            cell = moment_rows(0, i, row) + moment_rows(0, i, row, 1) + lower
            if i + 1 < planes:
                lower = side(i + 1)
                cell = cell + lower
            add(cell, owner_ref[i, here, :], 1)
        for k in range(2 * REACH + 2):
            window[k, here, :] = sums[k]
    for k in range(2 * REACH + 2):
        both = 0.25 * (window[k, pl.ds(0, rows // 2, stride=2), :] + window[k, pl.ds(1, rows // 2, stride=2), :])
        if k % 2 == 0:
            send_ref[k // 2] = both
        else:
            stay_ref[k // 2] = both


def vmem():
    return pl.BlockSpec(memory_space=pltpu.VMEM)


def call(kernel, out_shape, scratch, arguments, in_specs=None, limit=24 << 20, flops=1 << 20):
    return pl.pallas_call(
        kernel,
        out_shape=[jax.ShapeDtypeStruct(s, jnp.float32) for s in out_shape],
        in_specs=in_specs or [vmem()] * len(arguments),
        out_specs=[vmem()] * len(out_shape),
        scratch_shapes=[s if not isinstance(s, tuple) else pltpu.VMEM(s, jnp.float32) for s in scratch],
        compiler_params=pltpu.CompilerParams(vmem_limit_bytes=limit),
        cost_estimate=pl.CostEstimate(flops=flops, bytes_accessed=1 << 20, transcendentals=0),
    )(*arguments)


def core_swap(value):
    size = lax.axis_size("space")
    return lax.ppermute(value, "space", [(i, i ^ 1) for i in range(size)])


def chip_swap(value):
    size = lax.axis_size("space")
    pairs = []
    for i in range(1, size - 1, 2):
        pairs += [(i, i + 1), (i + 1, i)]
    return lax.ppermute(value, "space", pairs)


def sum_over_groups(value):
    size = lax.axis_size("src")
    if size & (size - 1):
        return lax.psum(value, "src")
    step = 1
    while step < size:
        value = value + lax.ppermute(value, "src", [(i, i ^ step) for i in range(size)])
        step *= 2
    return value


def gather_owned(send, stay):
    size = lax.axis_size("space")
    index = lax.axis_index("space")
    odd = lax.rem(index, 2) == 1
    other = core_swap(send)
    below = stay[0] + jnp.where(odd, other[1], other[0])
    here = stay[1] + jnp.where(odd, other[2], other[1])
    above = stay[2] + jnp.where(odd, 0.0, other[2])
    chip = index // 2
    upward = lax.rem(chip, 2) == 0
    chips = size // 2
    inner, outer = [], []
    for c in range(chips):
        for core in range(2):
            if c ^ 1 < chips:
                inner.append((2 * c + core, 2 * (c ^ 1) + core))
            partner = ((c + 1) ^ 1) - 1
            if 0 <= partner < chips:
                outer.append((2 * c + core, 2 * partner + core))
    from_inner = lax.ppermute(jnp.where(upward, above, below), "space", inner)
    from_outer = lax.ppermute(jnp.where(upward, below, above), "space", outer)
    from_far = lax.ppermute(other[0], "space", [(i, i - 4) for i in range(5, size, 2)])
    return here + from_inner + from_outer + from_far


def transposed_smooth(summed, rough):
    rows_in = summed.shape[-2]
    depth_in = summed.shape[-1]
    total = jnp.zeros_like(summed)
    for vertical in range(3):
        for lateral in range(3):
            product = rough[vertical * 3 + lateral] * summed
            padded = jnp.pad(product, ((0, 0), (1, 1), (1, 1)))
            total = (
                total
                + padded[
                    :, 2 - vertical : 2 - vertical + rows_in, 2 - lateral : 2 - lateral + depth_in
                ]
            )
    return total


def slab(adjoint_source, forward_field, medium, plane_map, depth, rough):
    planes, rows, width = medium.shape[1:]
    index = lax.axis_index("space")
    size = lax.axis_size("space") + REACH
    plane = (rows + 2 * PAD, width)
    state = (6, planes) + plane
    held = (6, planes + 1) + plane
    scale = (planes, rows, width)
    hbm = pl.BlockSpec(memory_space=pltpu.HBM)
    columns = pltpu.VMEM((planes, rows), jnp.int32)
    given = (adjoint_source, medium, depth, plane_map)
    chip, medium, scales, own, meta = call(
        start_kernel,
        [(6 * rows + PAD, width), medium.shape, scale, state, (PAD, width)],
        [(6, planes, rows, width), columns, columns, pltpu.SemaphoreType.DMA((2 * planes + 2,))],
        tuple(pltpu.with_memory_space_constraint(a, pltpu.HBM) for a in given),
        in_specs=[hbm] * 4,
    )
    chip = chip_swap(chip)
    chip_one, pair = call(
        follow_kernel, [(8 * rows, width), (14 * rows + PAD, width)], [state, state, held], (medium, scales, own, meta)
    )
    chip_one = chip_swap(chip_one)
    pair = core_swap(pair)

    here = index.astype(jnp.float32)
    levels = depth[0].astype(jnp.float32)
    owners = plane_map.astype(jnp.float32)
    position = lax.broadcasted_iota(jnp.int32, (planes, rows, width), 2).astype(jnp.float32)
    outside = float(size)
    owner = jnp.where(position < levels[:, :, None], (owners - here)[:, :, None], outside)
    below = jnp.where(lax.rem(index, 2) == 1, pair[14 * rows :], chip[6 * rows :])
    edge = jnp.where(position[0] < below[0, :rows, None], (below[1, :rows] - here)[:, None], outside)
    first, extra = call(
        early_kernel,
        [state, (16, rows, width)],
        [held, (6,) + plane, (6,) + plane, (6,) + plane],
        (medium, scales, own, pair, chip),
    )
    send, stay = call(
        last_kernel,
        [(REACH + 1, rows // 2, width), (REACH + 1, rows // 2, width)],
        [state, state, held, (3, planes) + plane, (2 * REACH + 2, rows, width)],
        (own, medium, forward_field, scales, owner, edge, pair, chip_one, first, extra),
    )
    total = sum_over_groups(gather_owned(send, stay))
    return transposed_smooth(total[None], rough)


def solution(mesh):
    in_specs = (
        P("src", None, "space", None, None),
        P("src", None, "space", None, None),
        P(None, "space", None, None),
        P("space", None),
        P("src", "space", None),
        P(None, "space", None, None),
    )
    out_specs = P("space", None, None)
    return jax.shard_map(slab, mesh=mesh, in_specs=in_specs, out_specs=out_specs, check_vma=False)
```

```python
import functools

import jax
import jax.numpy as jnp
from jax import lax
from jax.experimental import pallas as pl
from jax.experimental.pallas import tpu as pltpu
from jax.sharding import PartitionSpec as P


REACH = 2

sweep_steps = (0.323, 1.658, 0.422, 0.752)

PAD = 8
ROWS = 16


def lane_of(width):
    return lax.broadcasted_iota(jnp.int32, (ROWS, width), 1)


def ahead(value, lane):
    width = value.shape[-1]
    return jnp.where(lane == width - 1, 0.0, pltpu.roll(value, width - 1, 1))


def behind(value, lane):
    return jnp.where(lane == 0, 0.0, pltpu.roll(value, 1, 1))


def rows_at(ref, index, row, shift=0):
    return ref[index + (pl.ds(PAD + row + shift, ROWS), slice(None))]


def put(ref, index, row, value):
    ref[index + (pl.ds(PAD + row, ROWS), slice(None))] = value


def clear_pads(ref):
    rows = ref.shape[-2]
    lead = ref.shape[:-2]
    zero = jnp.zeros((PAD, ref.shape[-1]), jnp.float32)
    for flat in range(functools.reduce(lambda a, b: a * b, lead, 1)):
        index = []
        rest = flat
        for size in reversed(lead):
            index.insert(0, rest % size)
            rest //= size
        ref[tuple(index) + (pl.ds(0, PAD), slice(None))] = zero
        ref[tuple(index) + (pl.ds(rows - PAD, PAD), slice(None))] = zero


def chunks(total):
    return range(0, total, ROWS)


def curl(field, ahead_of, lane):
    out = []
    for part in (0, 3):
        ex, ey, ez = field(part, 0), field(part + 1, 0), field(part + 2, 0)
        hx = (field(part + 2, 1) - ez) - (ahead(ey, lane) - ey)
        hy = (ahead(ex, lane) - ex) - (ahead_of(part + 2) - ez)
        hz = (ahead_of(part + 1) - ey) - (field(part, 1) - ex)
        out += [hx, hy, hz]
    return out


def curl_back(held, before, lane):
    out = []
    for part in (0, 3):
        hx, hy, hz = held(part, 0), held(part + 1, 0), held(part + 2, 0)
        ox = (behind(hy, lane) - hy) - (held(part + 2, -1) - hz)
        oy = (before(part + 2) - hz) - (behind(hx, lane) - hx)
        oz = (held(part, -1) - hx) - (before(part + 1) - hy)
        out += [ox, oy, oz]
    return out


def updated(center, image, base, ratio, real, imag, scale):
    out = []
    for c in range(3):
        applied = image[c] + real * center[c] - imag * center[c + 3]
        out.append(center[c] + ratio * base[c] - scale * applied)
    for c in range(3):
        applied = image[c + 3] + real * center[c + 3] + imag * center[c]
        out.append(center[c + 3] + ratio * base[c + 3] - scale * applied)
    return out


def edge_sums(field, lane):
    out = []
    for part in (0, 3):
        ex = field(part, 0)
        out.append(field(part + 1, 0) + (field(part, 1) - ex))
        out.append(field(part + 2, 0) + (ahead(ex, lane) - ex))
    return out


def planes_of(ref):
    return lambda c, i, row, shift=0: rows_at(ref, (c, i), row, shift)


def sweep_slab(state, held, result, base, medium_ref, scale_ref, weight, low, high, first_scale, planes, rows, lane, wanted=None):
    wanted = range(planes) if wanted is None else wanted
    needed = sorted({i for w in wanted for i in (w - 1, w)})
    for i in needed:
        for row in chunks(rows):
            if i < 0:
                for part in (0, 3):
                    gy, gz = low(part, row)
                    ey, ez = state(part + 1, 0, row), state(part + 2, 0, row)
                    put(held, (part + 1, 0), row, first_scale * (gz - ez))
                    put(held, (part + 2, 0), row, first_scale * (ey - gy))
                continue

            def ahead_of(c, i=i, row=row):
                if i + 1 < planes:
                    return state(c, i + 1, row)
                return high(c, row)

            values = curl(lambda c, s: state(c, i, row, s), ahead_of, lane)
            for c in range(6):
                put(held, (c, i + 1), row, values[c])
    for i in wanted:
        for row in chunks(rows):
            image = curl_back(
                lambda c, s: rows_at(held, (c, i + 1), row, s), lambda c: rows_at(held, (c, i), row), lane
            )
            here = pl.ds(row, ROWS)
            new = updated(
                [state(c, i, row) for c in range(6)],
                image,
                [rows_at(base, (c, i), row) for c in range(6)],
                weight / sweep_steps[0],
                medium_ref[0, i, here, :],
                medium_ref[1, i, here, :],
                weight * scale_ref[i, here, :],
            )
            for c in range(6):
                put(result, (c, i), row, new[c])


def first_sweep(fields, medium_ref, scale_ref, state, i, rows):
    for row in chunks(rows):
        here = pl.ds(row, ROWS)
        scale = 1.0 / (4.0 + medium_ref[0, i, here, :])
        scale_ref[i, here, :] = scale
        for c in range(6):
            put(state, (c, i), row, sweep_steps[0] * scale * fields[c, i, here, :])


def parity_and_ends():
    index = lax.axis_index("space")
    odd = lax.rem(index, 2) == 1
    first_scale = jnp.where(index == 0, 0.0, 1.0)
    last_scale = jnp.where(index == lax.axis_size("space") - 1, 0.0, 1.0)
    return odd, first_scale, last_scale


def emit_level(emit, first, state, planes, rows, lane):
    for row in chunks(rows):
        sums = edge_sums(lambda c, s: rows_at(state, (c, planes - 1), row, s), lane)
        bottom = [rows_at(state, (c, 0), row) for c in (1, 2, 4, 5)]
        for k in range(4):
            emit(first + k, row, bottom[k], sums[k])


def message_rows(slot, row, rows):
    return pl.ds(slot * rows + row, ROWS)


def start_kernel(
    source_hbm, medium_hbm, depth_hbm, map_hbm, chip_ref, medium_ref, scale_ref, one, meta_ref,
    fields, levels, owners, sems,
):
    planes, rows, width = medium_ref.shape[1:]
    lane = lane_of(width)
    odd = parity_and_ends()[0]
    last = planes - 1
    order = [last, 0] + list(range(1, last))
    copies = []
    for i in order:
        copies.append(pltpu.make_async_copy(medium_hbm.at[:, i], medium_ref.at[:, i], sems.at[2 * i]))
        copies.append(pltpu.make_async_copy(source_hbm.at[0, :, i], fields.at[:, i], sems.at[2 * i + 1]))
    columns = [
        pltpu.make_async_copy(depth_hbm.at[0], levels, sems.at[2 * planes]),
        pltpu.make_async_copy(map_hbm, owners, sems.at[2 * planes + 1]),
    ]
    for copy in copies + columns:
        copy.start()
    clear_pads(one)
    meta_ref[...] = jnp.zeros_like(meta_ref)

    def emit(slot, row, below, above):
        chip_ref[message_rows(slot, row, rows), :] = jnp.where(odd, above, below)

    for k, i in enumerate(order):
        copies[2 * k].wait()
        copies[2 * k + 1].wait()
        first_sweep(fields, medium_ref, scale_ref, one, i, rows)
        if k == 1:
            emit_level(emit, 0, one, planes, rows, lane)
            for row in chunks(rows):
                here = pl.ds(row, ROWS)
                for part in range(2):
                    emit(4 + part, row, medium_ref[part, 0, here, :], medium_ref[part, last, here, :])
    for copy in columns:
        copy.wait()
    meta_ref[pl.ds(0, 1), pl.ds(0, rows)] = levels[pl.ds(last, 1), :].astype(jnp.float32)
    meta_ref[pl.ds(1, 1), pl.ds(0, rows)] = owners[pl.ds(last, 1), :].astype(jnp.float32)
    chip_ref[pl.ds(6 * rows, PAD), :] = meta_ref[...]


def no_plane(c, row):
    return 0.0


def no_sums(part, row):
    return 0.0, 0.0


def follow_kernel(medium_ref, scale_ref, one, meta_ref, chip_ref, pair_ref, two, three, held):
    planes, rows, width = medium_ref.shape[1:]
    lane = lane_of(width)
    odd, first_scale, _ = parity_and_ends()
    clear_pads(two)
    clear_pads(three)
    clear_pads(held)

    def emitter(slots, to_chip):
        def emit(slot, row, below, above):
            pair_ref[message_rows(slots + slot, row, rows), :] = jnp.where(odd, below, above)
            if to_chip is not None:
                chip_ref[message_rows(to_chip + slot, row, rows), :] = jnp.where(odd, above, below)

        return emit

    sweep_slab(
        planes_of(one), held, two, one, medium_ref, scale_ref, sweep_steps[1], no_sums, no_plane, first_scale,
        planes, rows, lane,
    )
    emit_level(emitter(6, 0), 0, two, planes, rows, lane)
    sweep_slab(
        planes_of(two), held, three, one, medium_ref, scale_ref, sweep_steps[2], no_sums, no_plane, first_scale,
        planes, rows, lane, wanted=sorted({0, planes - 1}),
    )
    emit_level(emitter(10, 4), 0, three, planes, rows, lane)
    emit_level(emitter(0, None), 0, one, planes, rows, lane)
    emit = emitter(4, None)
    for row in chunks(rows):
        for k in range(2):
            here = pl.ds(row, ROWS)
            emit(k, row, medium_ref[k, 0, here, :], medium_ref[k, planes - 1, here, :])
    pair_ref[pl.ds(14 * rows, PAD), :] = meta_ref[...]


def readers(odd, pair_ref, pair_first, chip_ref, chip_first, rows):
    def both(slot, row):
        pair = pair_ref[message_rows(pair_first + slot, row, rows), :]
        chip = chip_ref[message_rows(chip_first + slot, row, rows), :]
        return pair, chip

    def from_below(slot, row):
        pair, chip = both(slot, row)
        return jnp.where(odd, pair, chip)

    def from_above(slot, row):
        pair, chip = both(slot, row)
        return jnp.where(odd, chip, pair)

    return from_below, from_above


WHERE_YZ = {1: 0, 2: 1, 4: 2, 5: 3}


def moments(saved_ref, state, moment_ref, i, rows, lane):
    for row in chunks(rows):
        here = pl.ds(row, ROWS)
        for c in range(3):
            real = saved_ref[0, c, i, here, :].astype(jnp.float32)
            imag = saved_ref[0, c + 3, i, here, :].astype(jnp.float32)
            value = real * rows_at(state, (c + 3, i), row) + imag * rows_at(state, (c, i), row)
            if c < 2:
                value = value + ahead(value, lane)
            put(moment_ref, (c, i), row, value)


def early_kernel(
    medium_ref, scale_ref, one, pair_ref, chip_ref, three, extra_ref, two, held, delta_low, delta_high, delta_two,
):
    planes, rows, width = medium_ref.shape[1:]
    lane = lane_of(width)
    odd, first_scale, last_scale = parity_and_ends()
    for ref in (two, three, held, delta_low, delta_high, delta_two):
        clear_pads(ref)
    from_below, from_above = readers(odd, pair_ref, 0, chip_ref, 0, rows)

    for row in chunks(rows):
        sums = edge_sums(lambda c, s: rows_at(one, (c, planes - 1), row, s), lane)
        scale = (sweep_steps[1] * last_scale) / (4.0 + from_above(4, row))
        for k, c in enumerate((1, 2, 4, 5)):
            put(delta_high, (c,), row, scale * sums[k])
        scale = sweep_steps[1] / (4.0 + from_below(4, row))
        for part in (0, 3):
            ey, ez = rows_at(one, (part + 1, 0), row), rows_at(one, (part + 2, 0), row)
            put(delta_low, (part + 1,), row, scale * ey)
            put(delta_low, (part + 2,), row, scale * ez)
            put(delta_low, (part,), row, scale * ((behind(ez, lane) - ez) + (rows_at(one, (part + 1, 0), row, -1) - ey)))

    sweep_slab(
        planes_of(one), held, two, one, medium_ref, scale_ref, sweep_steps[1],
        lambda part, row: (from_below(2 * (part // 3), row), from_below(2 * (part // 3) + 1, row)),
        lambda c, row: from_above(WHERE_YZ[c], row),
        first_scale, planes, rows, lane,
    )

    none = [0.0] * 6
    for row in chunks(rows):
        values = curl(lambda c, s: rows_at(delta_low, (c,), row, s), lambda c: rows_at(two, (c, 0), row), lane)
        for c in range(6):
            put(held, (c, 0), row, values[c])
    for row in chunks(rows):
        before = {1: -rows_at(delta_low, (2,), row), 2: rows_at(delta_low, (1,), row),
                  4: -rows_at(delta_low, (5,), row), 5: rows_at(delta_low, (4,), row)}
        image = curl_back(lambda c, s: rows_at(held, (c, 0), row, s), lambda c: before[c], lane)
        real, imag = from_below(4, row), from_below(5, row)
        new = updated(
            [rows_at(delta_low, (c,), row) for c in range(6)], image, none, 0.0, real, imag, sweep_steps[2] / (4.0 + real)
        )
        for c in range(6):
            put(delta_two, (c,), row, new[c])
    for row in chunks(rows):
        sums = edge_sums(lambda c, s: rows_at(delta_two, (c,), row, s), lane)
        for k in range(4):
            extra_ref[k, pl.ds(row, ROWS), :] = sums[k]
    for row in chunks(rows):
        for part in (0, 3):
            ey, ez = rows_at(delta_high, (part + 1,), row), rows_at(delta_high, (part + 2,), row)
            put(held, (part, 1), row, (rows_at(delta_high, (part + 2,), row, 1) - ez) - (ahead(ey, lane) - ey))
    for row in chunks(rows):
        here = pl.ds(row, ROWS)
        sums = edge_sums(lambda c, s: rows_at(two, (c, planes - 1), row, s), lane)
        real, imag = from_above(4, row), from_above(5, row)
        scale = (sweep_steps[2] * last_scale) / (4.0 + real)
        center, image = {}, {}
        for part in (0, 3):
            ey, ez = rows_at(delta_high, (part + 1,), row), rows_at(delta_high, (part + 2,), row)
            hx = rows_at(held, (part, 1), row)
            k = 2 * (part // 3)
            center[part + 1], center[part + 2] = ey, ez
            image[part + 1] = 2.0 * ey - sums[k] - (behind(hx, lane) - hx)
            image[part + 2] = (rows_at(held, (part, 1), row, -1) - hx) - sums[k + 1] + 2.0 * ez
        for k, c in enumerate((1, 2)):
            extra_ref[4 + k, here, :] = center[c] - scale * (image[c] + real * center[c] - imag * center[c + 3])
            extra_ref[6 + k, here, :] = center[c + 3] - scale * (
                image[c + 3] + real * center[c + 3] + imag * center[c]
            )

    def low(part, row):
        sums = edge_sums(lambda c, s: rows_at(delta_low, (c,), row, s), lane)
        return sums[2 * (part // 3)], sums[2 * (part // 3) + 1]

    sweep_slab(
        planes_of(two), held, three, one, medium_ref, scale_ref, sweep_steps[2], low,
        lambda c, row: rows_at(delta_high, (c,), row), first_scale, planes, rows, lane,
    )


def last_kernel(
    base_ref, medium_ref, saved_ref, scale_ref, owner_ref, edge_ref, pair_ref, chip_ref, two, extra_ref,
    send_ref, stay_ref, ends, above, three, held, moment, window,
):
    planes, rows, width = medium_ref.shape[1:]
    lane = lane_of(width)
    odd, first_scale, _ = parity_and_ends()
    for ref in (ends, above, held, moment):
        clear_pads(ref)
    last = planes - 1

    from_below, from_above = readers(odd, pair_ref, 6, chip_ref, 0, rows)
    for row in chunks(rows):
        for k in range(4):
            put(above, (k,), row, from_above(k, row))
    for row in chunks(rows):
        here = pl.ds(row, ROWS)
        low_scale = (first_scale * sweep_steps[2]) * scale_ref[0, here, :]
        high_scale = sweep_steps[2] * scale_ref[last, here, :]
        for part in (0, 3):
            k = 2 * (part // 3)
            put(ends, (part, 0), row, rows_at(two, (part, 0), row))
            put(ends, (part + 1, 0), row, rows_at(two, (part + 1, 0), row) + low_scale * from_below(k, row))
            put(ends, (part + 2, 0), row, rows_at(two, (part + 2, 0), row) + low_scale * from_below(k + 1, row))
            ey, ez = rows_at(above, (k,), row), rows_at(above, (k + 1,), row)
            turn = (behind(ez, lane) - ez) + (rows_at(above, (k,), row, -1) - ey)
            put(ends, (part, 1), row, rows_at(two, (part, last), row) + high_scale * turn)
            put(ends, (part + 1, 1), row, rows_at(two, (part + 1, last), row) + high_scale * ey)
            put(ends, (part + 2, 1), row, rows_at(two, (part + 2, last), row) + high_scale * ez)

    def state(c, i, row, shift=0):
        if i == 0:
            return rows_at(ends, (c, 0), row, shift)
        if i == last:
            return rows_at(ends, (c, 1), row, shift)
        return rows_at(two, (c, i), row, shift)

    below_two, above_two = readers(odd, pair_ref, 10, chip_ref, 4, rows)

    def low(part, row):
        k = 2 * (part // 3)
        here = pl.ds(row, ROWS)
        return below_two(k, row) + extra_ref[k, here, :], below_two(k + 1, row) + extra_ref[k + 1, here, :]

    sweep_slab(
        state, held, three, base_ref, medium_ref, scale_ref, sweep_steps[3], low,
        lambda c, row: above_two(WHERE_YZ[c], row) + extra_ref[4 + WHERE_YZ[c], pl.ds(row, ROWS), :],
        first_scale, planes, rows, lane,
    )
    for i in range(planes):
        moments(saved_ref, three, moment, i, rows, lane)

    def moment_rows(c, i, row, shift=0):
        return rows_at(moment, (c, i), row, shift)

    for row in chunks(rows):
        here = pl.ds(row, ROWS)
        sums = [0.0] * (2 * REACH + 2)

        def add(value, offset, low):
            for k in range(2 * REACH + 1):
                slot = k + low
                sums[slot] = sums[slot] + jnp.where(offset == float(slot - REACH - 1), value, 0.0)

        def side(i):
            return moment_rows(1, i, row) + (moment_rows(2, i, row) + moment_rows(2, i, row, 1))

        lower = side(0)
        add(lower, edge_ref[here, :], 0)
        for i in range(planes):
            cell = moment_rows(0, i, row) + moment_rows(0, i, row, 1) + lower
            if i + 1 < planes:
                lower = side(i + 1)
                cell = cell + lower
            add(cell, owner_ref[i, here, :], 1)
        for k in range(2 * REACH + 2):
            window[k, here, :] = sums[k]
    for k in range(2 * REACH + 2):
        both = 0.25 * (window[k, pl.ds(0, rows // 2, stride=2), :] + window[k, pl.ds(1, rows // 2, stride=2), :])
        if k % 2 == 0:
            send_ref[k // 2] = both
        else:
            stay_ref[k // 2] = both


def vmem():
    return pl.BlockSpec(memory_space=pltpu.VMEM)


def call(kernel, out_shape, scratch, arguments, in_specs=None, limit=24 << 20, flops=1 << 20):
    return pl.pallas_call(
        kernel,
        out_shape=[jax.ShapeDtypeStruct(s, jnp.float32) for s in out_shape],
        in_specs=in_specs or [vmem()] * len(arguments),
        out_specs=[vmem()] * len(out_shape),
        scratch_shapes=[s if not isinstance(s, tuple) else pltpu.VMEM(s, jnp.float32) for s in scratch],
        compiler_params=pltpu.CompilerParams(vmem_limit_bytes=limit),
        cost_estimate=pl.CostEstimate(flops=flops, bytes_accessed=1 << 20, transcendentals=0),
    )(*arguments)


def core_swap(value):
    size = lax.axis_size("space")
    return lax.ppermute(value, "space", [(i, i ^ 1) for i in range(size)])


def chip_swap(value):
    size = lax.axis_size("space")
    pairs = []
    for i in range(1, size - 1, 2):
        pairs += [(i, i + 1), (i + 1, i)]
    return lax.ppermute(value, "space", pairs)


def sum_over_groups(value):
    size = lax.axis_size("src")
    if size & (size - 1):
        return lax.psum(value, "src")
    step = 1
    while step < size:
        value = value + lax.ppermute(value, "src", [(i, i ^ step) for i in range(size)])
        step *= 2
    return value


def gather_owned(send, stay):
    size = lax.axis_size("space")
    index = lax.axis_index("space")
    odd = lax.rem(index, 2) == 1
    other = core_swap(send)
    below = stay[0] + jnp.where(odd, other[1], other[0])
    here = stay[1] + jnp.where(odd, other[2], other[1])
    above = stay[2] + jnp.where(odd, 0.0, other[2])
    chip = index // 2
    upward = lax.rem(chip, 2) == 0
    chips = size // 2
    inner, outer = [], []
    for c in range(chips):
        for core in range(2):
            if c ^ 1 < chips:
                inner.append((2 * c + core, 2 * (c ^ 1) + core))
            partner = ((c + 1) ^ 1) - 1
            if 0 <= partner < chips:
                outer.append((2 * c + core, 2 * partner + core))
    from_inner = lax.ppermute(jnp.where(upward, above, below), "space", inner)
    from_outer = lax.ppermute(jnp.where(upward, below, above), "space", outer)
    from_far = lax.ppermute(other[0], "space", [(i, i - 4) for i in range(5, size, 2)])
    return here + from_inner + from_outer + from_far


def transposed_smooth(summed, rough):
    rows_in = summed.shape[-2]
    depth_in = summed.shape[-1]
    total = jnp.zeros_like(summed)
    for vertical in range(3):
        for lateral in range(3):
            product = rough[vertical * 3 + lateral] * summed
            padded = jnp.pad(product, ((0, 0), (1, 1), (1, 1)))
            total = (
                total
                + padded[
                    :, 2 - vertical : 2 - vertical + rows_in, 2 - lateral : 2 - lateral + depth_in
                ]
            )
    return total


def slab(adjoint_source, forward_field, medium, plane_map, depth, rough):
    planes, rows, width = medium.shape[1:]
    index = lax.axis_index("space")
    size = lax.axis_size("space") + REACH
    plane = (rows + 2 * PAD, width)
    state = (6, planes) + plane
    held = (6, planes + 1) + plane
    scale = (planes, rows, width)
    hbm = pl.BlockSpec(memory_space=pltpu.HBM)
    columns = pltpu.VMEM((planes, rows), jnp.int32)
    given = (adjoint_source, medium, depth, plane_map)
    chip, medium, scales, own, meta = call(
        start_kernel,
        [(6 * rows + PAD, width), medium.shape, scale, state, (PAD, width)],
        [(6, planes, rows, width), columns, columns, pltpu.SemaphoreType.DMA((2 * planes + 2,))],
        tuple(pltpu.with_memory_space_constraint(a, pltpu.HBM) for a in given),
        in_specs=[hbm] * 4,
    )
    chip = chip_swap(chip)
    chip_one, pair = call(
        follow_kernel, [(8 * rows, width), (14 * rows + PAD, width)], [state, state, held], (medium, scales, own, meta)
    )
    chip_one = chip_swap(chip_one)
    pair = core_swap(pair)

    here = index.astype(jnp.float32)
    levels = depth[0].astype(jnp.float32)
    owners = plane_map.astype(jnp.float32)
    position = lax.broadcasted_iota(jnp.int32, (planes, rows, width), 2).astype(jnp.float32)
    outside = float(size)
    owner = jnp.where(position < levels[:, :, None], (owners - here)[:, :, None], outside)
    below = jnp.where(lax.rem(index, 2) == 1, pair[14 * rows :], chip[6 * rows :])
    edge = jnp.where(position[0] < below[0, :rows, None], (below[1, :rows] - here)[:, None], outside)
    first, extra = call(
        early_kernel,
        [state, (8, rows, width)],
        [state, held, (6,) + plane, (6,) + plane, (6,) + plane],
        (medium, scales, own, pair, chip),
    )
    send, stay = call(
        last_kernel,
        [(REACH + 1, rows // 2, width), (REACH + 1, rows // 2, width)],
        [(6, 2) + plane, (4,) + plane, state, held, (3, planes) + plane, (2 * REACH + 2, rows, width)],
        (own, medium, forward_field, scales, owner, edge, pair, chip_one, first, extra),
    )
    total = sum_over_groups(gather_owned(send, stay))
    return transposed_smooth(total[None], rough)


def solution(mesh):
    in_specs = (
        P("src", None, "space", None, None),
        P("src", None, "space", None, None),
        P(None, "space", None, None),
        P("space", None),
        P("src", "space", None),
        P(None, "space", None, None),
    )
    out_specs = P("space", None, None)
    return jax.shard_map(slab, mesh=mesh, in_specs=in_specs, out_specs=out_specs, check_vma=False)
```

```python
import functools

import jax
import jax.numpy as jnp
from jax import lax
from jax.experimental import pallas as pl
from jax.experimental.pallas import tpu as pltpu
from jax.sharding import PartitionSpec as P


REACH = 2

sweep_steps = (0.323, 1.658, 0.422, 0.752)

PAD = 8
ROWS = 16


def lane_of(width):
    return lax.broadcasted_iota(jnp.int32, (ROWS, width), 1)


def ahead(value, lane):
    width = value.shape[-1]
    return jnp.where(lane == width - 1, 0.0, pltpu.roll(value, width - 1, 1))


def behind(value, lane):
    return jnp.where(lane == 0, 0.0, pltpu.roll(value, 1, 1))


def rows_at(ref, index, row, shift=0):
    return ref[index + (pl.ds(PAD + row + shift, ROWS), slice(None))]


def put(ref, index, row, value):
    ref[index + (pl.ds(PAD + row, ROWS), slice(None))] = value


def clear_pads(ref):
    rows = ref.shape[-2]
    lead = ref.shape[:-2]
    zero = jnp.zeros((PAD, ref.shape[-1]), jnp.float32)
    for flat in range(functools.reduce(lambda a, b: a * b, lead, 1)):
        index = []
        rest = flat
        for size in reversed(lead):
            index.insert(0, rest % size)
            rest //= size
        ref[tuple(index) + (pl.ds(0, PAD), slice(None))] = zero
        ref[tuple(index) + (pl.ds(rows - PAD, PAD), slice(None))] = zero


def chunks(total):
    return range(0, total, ROWS)


def curl(field, ahead_of, lane):
    out = []
    for part in (0, 3):
        ex, ey, ez = field(part, 0), field(part + 1, 0), field(part + 2, 0)
        hx = (field(part + 2, 1) - ez) - (ahead(ey, lane) - ey)
        hy = (ahead(ex, lane) - ex) - (ahead_of(part + 2) - ez)
        hz = (ahead_of(part + 1) - ey) - (field(part, 1) - ex)
        out += [hx, hy, hz]
    return out


def curl_back(held, before, lane):
    out = []
    for part in (0, 3):
        hx, hy, hz = held(part, 0), held(part + 1, 0), held(part + 2, 0)
        ox = (behind(hy, lane) - hy) - (held(part + 2, -1) - hz)
        oy = (before(part + 2) - hz) - (behind(hx, lane) - hx)
        oz = (held(part, -1) - hx) - (before(part + 1) - hy)
        out += [ox, oy, oz]
    return out


def updated(center, image, base, ratio, real, imag, scale):
    out = []
    for c in range(3):
        applied = image[c] + real * center[c] - imag * center[c + 3]
        out.append(center[c] + ratio * base[c] - scale * applied)
    for c in range(3):
        applied = image[c + 3] + real * center[c + 3] + imag * center[c]
        out.append(center[c + 3] + ratio * base[c + 3] - scale * applied)
    return out


def edge_sums(field, lane):
    out = []
    for part in (0, 3):
        ex = field(part, 0)
        out.append(field(part + 1, 0) + (field(part, 1) - ex))
        out.append(field(part + 2, 0) + (ahead(ex, lane) - ex))
    return out


def planes_of(ref):
    return lambda c, i, row, shift=0: rows_at(ref, (c, i), row, shift)


def sweep_slab(state, held, result, base, medium_ref, scale_ref, weight, low, high, first_scale, planes, rows, lane, wanted=None):
    wanted = range(planes) if wanted is None else wanted
    needed = sorted({i for w in wanted for i in (w - 1, w)})
    for i in needed:
        for row in chunks(rows):
            if i < 0:
                for part in (0, 3):
                    gy, gz = low(part, row)
                    ey, ez = state(part + 1, 0, row), state(part + 2, 0, row)
                    put(held, (part + 1, 0), row, first_scale * (gz - ez))
                    put(held, (part + 2, 0), row, first_scale * (ey - gy))
                continue

            def ahead_of(c, i=i, row=row):
                if i + 1 < planes:
                    return state(c, i + 1, row)
                return high(c, row)

            values = curl(lambda c, s: state(c, i, row, s), ahead_of, lane)
            for c in range(6):
                put(held, (c, i + 1), row, values[c])
    for i in wanted:
        for row in chunks(rows):
            image = curl_back(
                lambda c, s: rows_at(held, (c, i + 1), row, s), lambda c: rows_at(held, (c, i), row), lane
            )
            here = pl.ds(row, ROWS)
            new = updated(
                [state(c, i, row) for c in range(6)],
                image,
                [rows_at(base, (c, i), row) for c in range(6)],
                weight / sweep_steps[0],
                medium_ref[0, i, here, :],
                medium_ref[1, i, here, :],
                weight * scale_ref[i, here, :],
            )
            for c in range(6):
                put(result, (c, i), row, new[c])


def first_sweep(fields, medium_ref, scale_ref, state, i, rows):
    for row in chunks(rows):
        here = pl.ds(row, ROWS)
        scale = 1.0 / (4.0 + medium_ref[0, i, here, :])
        scale_ref[i, here, :] = scale
        for c in range(6):
            put(state, (c, i), row, sweep_steps[0] * scale * fields[c, i, here, :])


def parity_and_ends():
    index = lax.axis_index("space")
    odd = lax.rem(index, 2) == 1
    first_scale = jnp.where(index == 0, 0.0, 1.0)
    last_scale = jnp.where(index == lax.axis_size("space") - 1, 0.0, 1.0)
    return odd, first_scale, last_scale


def even_group():
    return lax.rem(lax.axis_index("src"), 2) == 0


def emit_level(emit, first, state, planes, rows, lane):
    for row in chunks(rows):
        sums = edge_sums(lambda c, s: rows_at(state, (c, planes - 1), row, s), lane)
        bottom = [rows_at(state, (c, 0), row) for c in (1, 2, 4, 5)]
        for k in range(4):
            emit(first + k, row, bottom[k], sums[k])


def message_rows(slot, row, rows):
    return pl.ds(slot * rows + row, ROWS)


def start_kernel(
    source_hbm, medium_hbm, depth_hbm, map_hbm, chip_ref, medium_ref, scale_ref, one, meta_ref,
    fields, levels, owners, sems,
):
    planes, rows, width = medium_ref.shape[1:]
    lane = lane_of(width)
    odd = parity_and_ends()[0]
    last = planes - 1
    order = [last, 0] + list(range(1, last))
    copies = []
    for i in order:
        copies.append(pltpu.make_async_copy(medium_hbm.at[:, i], medium_ref.at[:, i], sems.at[2 * i]))
        copies.append(pltpu.make_async_copy(source_hbm.at[0, :, i], fields.at[:, i], sems.at[2 * i + 1]))
    columns = [
        pltpu.make_async_copy(depth_hbm.at[0], levels, sems.at[2 * planes]),
        pltpu.make_async_copy(map_hbm, owners, sems.at[2 * planes + 1]),
    ]
    for copy in copies + columns:
        copy.start()
    clear_pads(one)
    meta_ref[...] = jnp.zeros_like(meta_ref)

    def emit(slot, row, below, above):
        chip_ref[message_rows(slot, row, rows), :] = jnp.where(odd, above, below)

    for k, i in enumerate(order):
        copies[2 * k].wait()
        copies[2 * k + 1].wait()
        first_sweep(fields, medium_ref, scale_ref, one, i, rows)
        if k == 1:
            emit_level(emit, 0, one, planes, rows, lane)
            first_part = even_group()
            for row in chunks(rows):
                here = pl.ds(row, ROWS)
                ends = [jnp.where(first_part, medium_ref[0, j, here, :], medium_ref[1, j, here, :]) for j in (0, last)]
                emit(4, row, ends[0], ends[1])
    for copy in columns:
        copy.wait()
    meta_ref[pl.ds(0, 1), pl.ds(0, rows)] = levels[pl.ds(last, 1), :].astype(jnp.float32)
    meta_ref[pl.ds(1, 1), pl.ds(0, rows)] = owners[pl.ds(last, 1), :].astype(jnp.float32)
    chip_ref[pl.ds(5 * rows, PAD), :] = meta_ref[...]


def no_plane(c, row):
    return 0.0


def no_sums(part, row):
    return 0.0, 0.0


def follow_kernel(medium_ref, scale_ref, one, meta_ref, chip_ref, pair_ref, two, three, held):
    planes, rows, width = medium_ref.shape[1:]
    lane = lane_of(width)
    odd, first_scale, _ = parity_and_ends()
    clear_pads(two)
    clear_pads(three)
    clear_pads(held)

    def emitter(slots, to_chip):
        def emit(slot, row, below, above):
            pair_ref[message_rows(slots + slot, row, rows), :] = jnp.where(odd, below, above)
            if to_chip is not None:
                chip_ref[message_rows(to_chip + slot, row, rows), :] = jnp.where(odd, above, below)

        return emit

    sweep_slab(
        planes_of(one), held, two, one, medium_ref, scale_ref, sweep_steps[1], no_sums, no_plane, first_scale,
        planes, rows, lane,
    )
    emit_level(emitter(6, 0), 0, two, planes, rows, lane)
    sweep_slab(
        planes_of(two), held, three, one, medium_ref, scale_ref, sweep_steps[2], no_sums, no_plane, first_scale,
        planes, rows, lane, wanted=sorted({0, planes - 1}),
    )
    emit_level(emitter(10, 4), 0, three, planes, rows, lane)
    emit_level(emitter(0, None), 0, one, planes, rows, lane)
    emit = emitter(4, None)
    for row in chunks(rows):
        for k in range(2):
            here = pl.ds(row, ROWS)
            emit(k, row, medium_ref[k, 0, here, :], medium_ref[k, planes - 1, here, :])
    pair_ref[pl.ds(14 * rows, PAD), :] = meta_ref[...]


def readers(odd, pair_ref, pair_first, chip_ref, chip_first, rows):
    def both(slot, row):
        pair = pair_ref[message_rows(pair_first + slot, row, rows), :]
        chip = chip_ref[message_rows(chip_first + slot, row, rows), :]
        return pair, chip

    def from_below(slot, row):
        pair, chip = both(slot, row)
        return jnp.where(odd, pair, chip)

    def from_above(slot, row):
        pair, chip = both(slot, row)
        return jnp.where(odd, chip, pair)

    return from_below, from_above


WHERE_YZ = {1: 0, 2: 1, 4: 2, 5: 3}


def moments(saved_ref, state, moment_ref, i, rows, lane):
    for row in chunks(rows):
        here = pl.ds(row, ROWS)
        for c in range(3):
            real = saved_ref[0, c, i, here, :].astype(jnp.float32)
            imag = saved_ref[0, c + 3, i, here, :].astype(jnp.float32)
            value = real * rows_at(state, (c + 3, i), row) + imag * rows_at(state, (c, i), row)
            if c < 2:
                value = value + ahead(value, lane)
            put(moment_ref, (c, i), row, value)


def early_kernel(medium_ref, scale_ref, one, pair_ref, chip_ref, two, held):
    planes, rows, width = medium_ref.shape[1:]
    lane = lane_of(width)
    odd, first_scale, _ = parity_and_ends()
    for ref in (two, held):
        clear_pads(ref)
    from_below, from_above = readers(odd, pair_ref, 0, chip_ref, 0, rows)
    sweep_slab(
        planes_of(one), held, two, one, medium_ref, scale_ref, sweep_steps[1],
        lambda part, row: (from_below(2 * (part // 3), row), from_below(2 * (part // 3) + 1, row)),
        lambda c, row: from_above(WHERE_YZ[c], row),
        first_scale, planes, rows, lane,
    )


def second_kernel(
    medium_ref, scale_ref, one, two, pair_ref, chip_ref, other_ref, three, extra_ref, held, delta_low, delta_high, delta_two,
):
    planes, rows, width = medium_ref.shape[1:]
    lane = lane_of(width)
    odd, first_scale, last_scale = parity_and_ends()
    for ref in (three, held, delta_low, delta_high, delta_two):
        clear_pads(ref)
    first_part = even_group()

    def medium_next(above, part, row):
        pair = pair_ref[message_rows(4 + part, row, rows), :]
        chip, other = chip_ref[message_rows(4, row, rows), :], other_ref[pl.ds(row, ROWS), :]
        chip = jnp.where(first_part, chip, other) if part == 0 else jnp.where(first_part, other, chip)
        return jnp.where(odd, chip, pair) if above else jnp.where(odd, pair, chip)

    for row in chunks(rows):
        sums = edge_sums(lambda c, s: rows_at(one, (c, planes - 1), row, s), lane)
        scale = (sweep_steps[1] * last_scale) / (4.0 + medium_next(True, 0, row))
        for k, c in enumerate((1, 2, 4, 5)):
            put(delta_high, (c,), row, scale * sums[k])
        scale = sweep_steps[1] / (4.0 + medium_next(False, 0, row))
        for part in (0, 3):
            ey, ez = rows_at(one, (part + 1, 0), row), rows_at(one, (part + 2, 0), row)
            put(delta_low, (part + 1,), row, scale * ey)
            put(delta_low, (part + 2,), row, scale * ez)
            put(delta_low, (part,), row, scale * ((behind(ez, lane) - ez) + (rows_at(one, (part + 1, 0), row, -1) - ey)))

    none = [0.0] * 6
    for row in chunks(rows):
        values = curl(lambda c, s: rows_at(delta_low, (c,), row, s), lambda c: rows_at(two, (c, 0), row), lane)
        for c in range(6):
            put(held, (c, 0), row, values[c])
    for row in chunks(rows):
        before = {1: -rows_at(delta_low, (2,), row), 2: rows_at(delta_low, (1,), row),
                  4: -rows_at(delta_low, (5,), row), 5: rows_at(delta_low, (4,), row)}
        image = curl_back(lambda c, s: rows_at(held, (c, 0), row, s), lambda c: before[c], lane)
        real, imag = medium_next(False, 0, row), medium_next(False, 1, row)
        new = updated(
            [rows_at(delta_low, (c,), row) for c in range(6)], image, none, 0.0, real, imag, sweep_steps[2] / (4.0 + real)
        )
        for c in range(6):
            put(delta_two, (c,), row, new[c])
    for row in chunks(rows):
        sums = edge_sums(lambda c, s: rows_at(delta_two, (c,), row, s), lane)
        for k in range(4):
            extra_ref[k, pl.ds(row, ROWS), :] = sums[k]
    for row in chunks(rows):
        for part in (0, 3):
            ey, ez = rows_at(delta_high, (part + 1,), row), rows_at(delta_high, (part + 2,), row)
            put(held, (part, 1), row, (rows_at(delta_high, (part + 2,), row, 1) - ez) - (ahead(ey, lane) - ey))
    for row in chunks(rows):
        here = pl.ds(row, ROWS)
        sums = edge_sums(lambda c, s: rows_at(two, (c, planes - 1), row, s), lane)
        real, imag = medium_next(True, 0, row), medium_next(True, 1, row)
        scale = (sweep_steps[2] * last_scale) / (4.0 + real)
        center, image = {}, {}
        for part in (0, 3):
            ey, ez = rows_at(delta_high, (part + 1,), row), rows_at(delta_high, (part + 2,), row)
            hx = rows_at(held, (part, 1), row)
            k = 2 * (part // 3)
            center[part + 1], center[part + 2] = ey, ez
            image[part + 1] = 2.0 * ey - sums[k] - (behind(hx, lane) - hx)
            image[part + 2] = (rows_at(held, (part, 1), row, -1) - hx) - sums[k + 1] + 2.0 * ez
        for k, c in enumerate((1, 2)):
            extra_ref[4 + k, here, :] = center[c] - scale * (image[c] + real * center[c] - imag * center[c + 3])
            extra_ref[6 + k, here, :] = center[c + 3] - scale * (
                image[c + 3] + real * center[c + 3] + imag * center[c]
            )

    def low(part, row):
        sums = edge_sums(lambda c, s: rows_at(delta_low, (c,), row, s), lane)
        return sums[2 * (part // 3)], sums[2 * (part // 3) + 1]

    sweep_slab(
        planes_of(two), held, three, one, medium_ref, scale_ref, sweep_steps[2], low,
        lambda c, row: rows_at(delta_high, (c,), row), first_scale, planes, rows, lane,
    )


def last_kernel(
    base_ref, medium_ref, saved_ref, scale_ref, owner_ref, edge_ref, pair_ref, chip_ref, two, extra_ref,
    send_ref, stay_ref, ends, above, three, held, moment, window,
):
    planes, rows, width = medium_ref.shape[1:]
    lane = lane_of(width)
    odd, first_scale, _ = parity_and_ends()
    for ref in (ends, above, held, moment):
        clear_pads(ref)
    last = planes - 1

    from_below, from_above = readers(odd, pair_ref, 6, chip_ref, 0, rows)
    for row in chunks(rows):
        for k in range(4):
            put(above, (k,), row, from_above(k, row))
    for row in chunks(rows):
        here = pl.ds(row, ROWS)
        low_scale = (first_scale * sweep_steps[2]) * scale_ref[0, here, :]
        high_scale = sweep_steps[2] * scale_ref[last, here, :]
        for part in (0, 3):
            k = 2 * (part // 3)
            put(ends, (part, 0), row, rows_at(two, (part, 0), row))
            put(ends, (part + 1, 0), row, rows_at(two, (part + 1, 0), row) + low_scale * from_below(k, row))
            put(ends, (part + 2, 0), row, rows_at(two, (part + 2, 0), row) + low_scale * from_below(k + 1, row))
            ey, ez = rows_at(above, (k,), row), rows_at(above, (k + 1,), row)
            turn = (behind(ez, lane) - ez) + (rows_at(above, (k,), row, -1) - ey)
            put(ends, (part, 1), row, rows_at(two, (part, last), row) + high_scale * turn)
            put(ends, (part + 1, 1), row, rows_at(two, (part + 1, last), row) + high_scale * ey)
            put(ends, (part + 2, 1), row, rows_at(two, (part + 2, last), row) + high_scale * ez)

    def state(c, i, row, shift=0):
        if i == 0:
            return rows_at(ends, (c, 0), row, shift)
        if i == last:
            return rows_at(ends, (c, 1), row, shift)
        return rows_at(two, (c, i), row, shift)

    below_two, above_two = readers(odd, pair_ref, 10, chip_ref, 4, rows)

    def low(part, row):
        k = 2 * (part // 3)
        here = pl.ds(row, ROWS)
        return below_two(k, row) + extra_ref[k, here, :], below_two(k + 1, row) + extra_ref[k + 1, here, :]

    sweep_slab(
        state, held, three, base_ref, medium_ref, scale_ref, sweep_steps[3], low,
        lambda c, row: above_two(WHERE_YZ[c], row) + extra_ref[4 + WHERE_YZ[c], pl.ds(row, ROWS), :],
        first_scale, planes, rows, lane,
    )
    for i in range(planes):
        moments(saved_ref, three, moment, i, rows, lane)

    def moment_rows(c, i, row, shift=0):
        return rows_at(moment, (c, i), row, shift)

    for row in chunks(rows):
        here = pl.ds(row, ROWS)
        sums = [0.0] * (2 * REACH + 2)

        def add(value, offset, low):
            for k in range(2 * REACH + 1):
                slot = k + low
                sums[slot] = sums[slot] + jnp.where(offset == float(slot - REACH - 1), value, 0.0)

        def side(i):
            return moment_rows(1, i, row) + (moment_rows(2, i, row) + moment_rows(2, i, row, 1))

        lower = side(0)
        add(lower, edge_ref[here, :], 0)
        for i in range(planes):
            cell = moment_rows(0, i, row) + moment_rows(0, i, row, 1) + lower
            if i + 1 < planes:
                lower = side(i + 1)
                cell = cell + lower
            add(cell, owner_ref[i, here, :], 1)
        for k in range(2 * REACH + 2):
            window[k, here, :] = sums[k]
    for k in range(2 * REACH + 2):
        both = 0.25 * (window[k, pl.ds(0, rows // 2, stride=2), :] + window[k, pl.ds(1, rows // 2, stride=2), :])
        if k % 2 == 0:
            send_ref[k // 2] = both
        else:
            stay_ref[k // 2] = both


def vmem():
    return pl.BlockSpec(memory_space=pltpu.VMEM)


def call(kernel, out_shape, scratch, arguments, in_specs=None, limit=24 << 20, flops=1 << 20):
    return pl.pallas_call(
        kernel,
        out_shape=[jax.ShapeDtypeStruct(s, jnp.float32) for s in out_shape],
        in_specs=in_specs or [vmem()] * len(arguments),
        out_specs=[vmem()] * len(out_shape),
        scratch_shapes=[s if not isinstance(s, tuple) else pltpu.VMEM(s, jnp.float32) for s in scratch],
        compiler_params=pltpu.CompilerParams(vmem_limit_bytes=limit),
        cost_estimate=pl.CostEstimate(flops=flops, bytes_accessed=1 << 20, transcendentals=0),
    )(*arguments)


def core_swap(value):
    size = lax.axis_size("space")
    return lax.ppermute(value, "space", [(i, i ^ 1) for i in range(size)])


def chip_swap(value):
    size = lax.axis_size("space")
    pairs = []
    for i in range(1, size - 1, 2):
        pairs += [(i, i + 1), (i + 1, i)]
    return lax.ppermute(value, "space", pairs)


def sum_over_groups(value):
    size = lax.axis_size("src")
    if size & (size - 1):
        return lax.psum(value, "src")
    step = 1
    while step < size:
        value = value + lax.ppermute(value, "src", [(i, i ^ step) for i in range(size)])
        step *= 2
    return value


def gather_owned(send, stay):
    size = lax.axis_size("space")
    index = lax.axis_index("space")
    odd = lax.rem(index, 2) == 1
    other = core_swap(send)
    below = stay[0] + jnp.where(odd, other[1], other[0])
    here = stay[1] + jnp.where(odd, other[2], other[1])
    above = stay[2] + jnp.where(odd, 0.0, other[2])
    chip = index // 2
    upward = lax.rem(chip, 2) == 0
    chips = size // 2
    inner, outer = [], []
    for c in range(chips):
        for core in range(2):
            if c ^ 1 < chips:
                inner.append((2 * c + core, 2 * (c ^ 1) + core))
            partner = ((c + 1) ^ 1) - 1
            if 0 <= partner < chips:
                outer.append((2 * c + core, 2 * partner + core))
    from_inner = lax.ppermute(jnp.where(upward, above, below), "space", inner)
    from_outer = lax.ppermute(jnp.where(upward, below, above), "space", outer)
    from_far = lax.ppermute(other[0], "space", [(i, i - 4) for i in range(5, size, 2)])
    return here + from_inner + from_outer + from_far


def transposed_smooth(summed, rough):
    rows_in = summed.shape[-2]
    depth_in = summed.shape[-1]
    total = jnp.zeros_like(summed)
    for vertical in range(3):
        for lateral in range(3):
            product = rough[vertical * 3 + lateral] * summed
            padded = jnp.pad(product, ((0, 0), (1, 1), (1, 1)))
            total = (
                total
                + padded[
                    :, 2 - vertical : 2 - vertical + rows_in, 2 - lateral : 2 - lateral + depth_in
                ]
            )
    return total


def slab(adjoint_source, forward_field, medium, plane_map, depth, rough):
    planes, rows, width = medium.shape[1:]
    index = lax.axis_index("space")
    size = lax.axis_size("space") + REACH
    plane = (rows + 2 * PAD, width)
    state = (6, planes) + plane
    held = (6, planes + 1) + plane
    scale = (planes, rows, width)
    hbm = pl.BlockSpec(memory_space=pltpu.HBM)
    columns = pltpu.VMEM((planes, rows), jnp.int32)
    given = (adjoint_source, medium, depth, plane_map)
    chip, medium, scales, own, meta = call(
        start_kernel,
        [(5 * rows + PAD, width), medium.shape, scale, state, (PAD, width)],
        [(6, planes, rows, width), columns, columns, pltpu.SemaphoreType.DMA((2 * planes + 2,))],
        tuple(pltpu.with_memory_space_constraint(a, pltpu.HBM) for a in given),
        in_specs=[hbm] * 4,
    )
    chip = chip_swap(chip)
    chip_one, pair = call(
        follow_kernel, [(8 * rows, width), (14 * rows + PAD, width)], [state, state, held], (medium, scales, own, meta)
    )
    chip_one = chip_swap(chip_one)
    pair = core_swap(pair)

    here = index.astype(jnp.float32)
    levels = depth[0].astype(jnp.float32)
    owners = plane_map.astype(jnp.float32)
    position = lax.broadcasted_iota(jnp.int32, (planes, rows, width), 2).astype(jnp.float32)
    outside = float(size)
    owner = jnp.where(position < levels[:, :, None], (owners - here)[:, :, None], outside)
    below = jnp.where(lax.rem(index, 2) == 1, pair[14 * rows :], chip[5 * rows :])
    edge = jnp.where(position[0] < below[0, :rows, None], (below[1, :rows] - here)[:, None], outside)
    groups = lax.axis_size("src")
    other = lax.ppermute(chip[4 * rows : 5 * rows], "src", [(i, i ^ 1) for i in range(groups)])
    (first,) = call(early_kernel, [state], [held], (medium, scales, own, pair, chip))
    second, extra = call(
        second_kernel,
        [state, (8, rows, width)],
        [held, (6,) + plane, (6,) + plane, (6,) + plane],
        (medium, scales, own, first, pair, chip, other),
    )
    send, stay = call(
        last_kernel,
        [(REACH + 1, rows // 2, width), (REACH + 1, rows // 2, width)],
        [(6, 2) + plane, (4,) + plane, state, held, (3, planes) + plane, (2 * REACH + 2, rows, width)],
        (own, medium, forward_field, scales, owner, edge, pair, chip_one, second, extra),
    )
    total = sum_over_groups(gather_owned(send, stay))
    return transposed_smooth(total[None], rough)


def solution(mesh):
    in_specs = (
        P("src", None, "space", None, None),
        P("src", None, "space", None, None),
        P(None, "space", None, None),
        P("space", None),
        P("src", "space", None),
        P(None, "space", None, None),
    )
    out_specs = P("space", None, None)
    return jax.shard_map(slab, mesh=mesh, in_specs=in_specs, out_specs=out_specs, check_vma=False)
```

```python
import jax
import jax.numpy as jnp
from jax import lax
from jax.experimental import pallas as pl
from jax.experimental.pallas import tpu as pltpu
from jax.sharding import PartitionSpec as P


REACH = 2

sweep_steps = (0.323, 1.658, 0.422, 0.752)

PAD = 8
ROWS = 32


def lane_of(width):
    return lax.broadcasted_iota(jnp.int32, (ROWS, width), 1)


def ahead(value, lane):
    width = value.shape[-1]
    return jnp.where(lane == width - 1, 0.0, pltpu.roll(value, width - 1, 1))


def behind(value, lane):
    return jnp.where(lane == 0, 0.0, pltpu.roll(value, 1, 1))


def rows_at(ref, index, row, shift=0):
    return ref[index + (pl.ds(PAD + row + shift, ROWS), slice(None))]


def put(ref, index, row, value):
    ref[index + (pl.ds(PAD + row, ROWS), slice(None))] = value


def indices(lead):
    out = [()]
    for size in lead:
        out = [index + (i,) for index in out for i in range(size)]
    return out


def clear_after(ref, components=(0, 2, 3, 5)):
    zero = jnp.zeros((PAD, ref.shape[-1]), jnp.float32)
    for index in indices(ref.shape[:-2]):
        if index[0] in components:
            ref[index + (pl.ds(ref.shape[-2] - PAD, PAD), slice(None))] = zero


def clear_before(ref, components=(0, 2, 3, 5)):
    zero = jnp.zeros((PAD, ref.shape[-1]), jnp.float32)
    for index in indices(ref.shape[:-2]):
        if index[0] in components:
            ref[index + (pl.ds(0, PAD), slice(None))] = zero


def chunks(total):
    return range(0, total, ROWS)


def curl(field, ahead_of, lane):
    out = []
    for part in (0, 3):
        ex, ey, ez = field(part, 0), field(part + 1, 0), field(part + 2, 0)
        hx = (field(part + 2, 1) - ez) - (ahead(ey, lane) - ey)
        hy = (ahead(ex, lane) - ex) - (ahead_of(part + 2) - ez)
        hz = (ahead_of(part + 1) - ey) - (field(part, 1) - ex)
        out += [hx, hy, hz]
    return out


def curl_back(held, before, lane):
    out = []
    for part in (0, 3):
        hx, hy, hz = held(part, 0), held(part + 1, 0), held(part + 2, 0)
        ox = (behind(hy, lane) - hy) - (held(part + 2, -1) - hz)
        oy = (before(part + 2) - hz) - (behind(hx, lane) - hx)
        oz = (held(part, -1) - hx) - (before(part + 1) - hy)
        out += [ox, oy, oz]
    return out


def updated(center, image, base, ratio, real, imag, scale):
    out = []
    for c in range(3):
        applied = image[c] + real * center[c] - imag * center[c + 3]
        out.append(center[c] + ratio * base[c] - scale * applied)
    for c in range(3):
        applied = image[c + 3] + real * center[c + 3] + imag * center[c]
        out.append(center[c + 3] + ratio * base[c + 3] - scale * applied)
    return out


def edge_sums(field, lane):
    out = []
    for part in (0, 3):
        ex = field(part, 0)
        out.append(field(part + 1, 0) + (field(part, 1) - ex))
        out.append(field(part + 2, 0) + (ahead(ex, lane) - ex))
    return out


def planes_of(ref):
    return lambda c, i, row, shift=0: rows_at(ref, (c, i), row, shift)


def sweep_slab(state, held, result, base, medium_ref, scale_ref, weight, low, high, first_scale, planes, rows, lane, wanted=None, skip=()):
    wanted = range(planes) if wanted is None else wanted
    needed = sorted({i for w in wanted for i in (w - 1, w)})
    for i in needed:
        for row in chunks(rows):
            if i < 0:
                for part in (0, 3):
                    gy, gz = low(part, row)
                    ey, ez = state(part + 1, 0, row), state(part + 2, 0, row)
                    put(held, (part + 1, 0), row, first_scale * (gz - ez))
                    put(held, (part + 2, 0), row, first_scale * (ey - gy))
                continue

            def ahead_of(c, i=i, row=row):
                if i + 1 < planes:
                    return state(c, i + 1, row)
                return high(c, row)

            values = curl(lambda c, s: state(c, i, row, s), ahead_of, lane)
            for c in range(6) if i in wanted else (1, 2, 4, 5):
                put(held, (c, i + 1), row, values[c])
    for i in wanted:
        for row in chunks(rows):
            image = curl_back(
                lambda c, s: rows_at(held, (c, i + 1), row, s), lambda c: rows_at(held, (c, i), row), lane
            )
            here = pl.ds(row, ROWS)
            new = updated(
                [state(c, i, row) for c in range(6)],
                image,
                [rows_at(base, (c, i), row) for c in range(6)],
                weight / sweep_steps[0],
                medium_ref[0, i, here, :],
                medium_ref[1, i, here, :],
                weight * scale_ref[i, here, :],
            )
            for c in range(6):
                if (c, i) not in skip:
                    put(result, (c, i), row, new[c])


def first_sweep(fields, medium_ref, scale_ref, state, i, rows):
    for row in chunks(rows):
        here = pl.ds(row, ROWS)
        scale = 1.0 / (4.0 + medium_ref[0, i, here, :])
        scale_ref[i, here, :] = scale
        for c in range(6):
            put(state, (c, i), row, sweep_steps[0] * scale * fields[c, i, here, :])


def parity_and_ends():
    index = lax.axis_index("space")
    odd = lax.rem(index, 2) == 1
    first_scale = jnp.where(index == 0, 0.0, 1.0)
    last_scale = jnp.where(index == lax.axis_size("space") - 1, 0.0, 1.0)
    return odd, first_scale, last_scale


def even_group():
    return lax.rem(lax.axis_index("src"), 2) == 0


def emit_level(emit, first, state, planes, rows, lane):
    for row in chunks(rows):
        sums = edge_sums(lambda c, s: rows_at(state, (c, planes - 1), row, s), lane)
        bottom = [rows_at(state, (c, 0), row) for c in (1, 2, 4, 5)]
        for k in range(4):
            emit(first + k, row, bottom[k], sums[k])


def message_rows(slot, row, rows):
    return pl.ds(slot * rows + row, ROWS)


def start_kernel(
    source_hbm, medium_hbm, depth_hbm, map_hbm, chip_ref, medium_ref, scale_ref, one, meta_ref,
    fields, levels, owners, sems,
):
    planes, rows, width = medium_ref.shape[1:]
    lane = lane_of(width)
    odd = parity_and_ends()[0]
    last = planes - 1
    order = [last, 0] + list(range(1, last))
    copies = []
    for i in order:
        copies.append(pltpu.make_async_copy(medium_hbm.at[:, i], medium_ref.at[:, i], sems.at[2 * i]))
        copies.append(pltpu.make_async_copy(source_hbm.at[0, :, i], fields.at[:, i], sems.at[2 * i + 1]))
    columns = [
        pltpu.make_async_copy(depth_hbm.at[0], levels, sems.at[2 * planes]),
        pltpu.make_async_copy(map_hbm, owners, sems.at[2 * planes + 1]),
    ]
    for copy in copies + columns:
        copy.start()
    clear_after(one)
    clear_before(one, (1, 4))
    meta_ref[...] = jnp.zeros_like(meta_ref)

    def emit(slot, row, below, above):
        chip_ref[message_rows(slot, row, rows), :] = jnp.where(odd, above, below)

    for k, i in enumerate(order):
        copies[2 * k].wait()
        copies[2 * k + 1].wait()
        first_sweep(fields, medium_ref, scale_ref, one, i, rows)
        if k == 1:
            emit_level(emit, 0, one, planes, rows, lane)
            first_part = even_group()
            for row in chunks(rows):
                here = pl.ds(row, ROWS)
                ends = [jnp.where(first_part, medium_ref[0, j, here, :], medium_ref[1, j, here, :]) for j in (0, last)]
                emit(4, row, ends[0], ends[1])
    for copy in columns:
        copy.wait()
    meta_ref[pl.ds(0, 1), pl.ds(0, rows)] = levels[pl.ds(last, 1), :].astype(jnp.float32)
    meta_ref[pl.ds(1, 1), pl.ds(0, rows)] = owners[pl.ds(last, 1), :].astype(jnp.float32)
    chip_ref[pl.ds(5 * rows, PAD), :] = meta_ref[...]


def no_plane(c, row):
    return 0.0


def no_sums(part, row):
    return 0.0, 0.0


def follow_kernel(medium_ref, scale_ref, one, meta_ref, chip_ref, pair_ref, two, three, held):
    planes, rows, width = medium_ref.shape[1:]
    lane = lane_of(width)
    odd, first_scale, _ = parity_and_ends()
    clear_after(two)
    clear_after(three, (0, 3))
    clear_before(held)

    def emitter(slots, to_chip):
        def emit(slot, row, below, above):
            pair_ref[message_rows(slots + slot, row, rows), :] = jnp.where(odd, below, above)
            if to_chip is not None:
                chip_ref[message_rows(to_chip + slot, row, rows), :] = jnp.where(odd, above, below)

        return emit

    last = planes - 1
    sweep_slab(
        planes_of(one), held, two, one, medium_ref, scale_ref, sweep_steps[1], no_sums, no_plane, first_scale,
        planes, rows, lane, wanted=sorted({0, 1, last - 1, last}), skip=[(c, 1) for c in (0, 3) if 1 < last - 1],
    )
    emit_level(emitter(6, 0), 0, two, planes, rows, lane)
    sweep_slab(
        planes_of(two), held, three, one, medium_ref, scale_ref, sweep_steps[2], no_sums, no_plane, first_scale,
        planes, rows, lane, wanted=sorted({0, last}), skip=[(c, 0) for c in (0, 3)],
    )
    emit_level(emitter(10, 4), 0, three, planes, rows, lane)
    emit_level(emitter(0, None), 0, one, planes, rows, lane)
    emit = emitter(4, None)
    for row in chunks(rows):
        for k in range(2):
            here = pl.ds(row, ROWS)
            emit(k, row, medium_ref[k, 0, here, :], medium_ref[k, planes - 1, here, :])
    pair_ref[pl.ds(14 * rows, PAD), :] = meta_ref[...]


def readers(odd, pair_ref, pair_first, chip_ref, chip_first, rows):
    def both(slot, row):
        pair = pair_ref[message_rows(pair_first + slot, row, rows), :]
        chip = chip_ref[message_rows(chip_first + slot, row, rows), :]
        return pair, chip

    def from_below(slot, row):
        pair, chip = both(slot, row)
        return jnp.where(odd, pair, chip)

    def from_above(slot, row):
        pair, chip = both(slot, row)
        return jnp.where(odd, chip, pair)

    return from_below, from_above


WHERE_YZ = {1: 0, 2: 1, 4: 2, 5: 3}


def moments(saved_ref, state, moment_ref, i, rows, lane):
    for row in chunks(rows):
        here = pl.ds(row, ROWS)
        for c in range(3):
            real = saved_ref[0, c, i, here, :].astype(jnp.float32)
            imag = saved_ref[0, c + 3, i, here, :].astype(jnp.float32)
            value = real * rows_at(state, (c + 3, i), row) + imag * rows_at(state, (c, i), row)
            if c < 2:
                value = value + ahead(value, lane)
            put(moment_ref, (c, i), row, value)


def early_kernel(medium_ref, scale_ref, one, pair_ref, chip_ref, two, held):
    planes, rows, width = medium_ref.shape[1:]
    lane = lane_of(width)
    odd, first_scale, _ = parity_and_ends()
    clear_after(two)
    clear_before(held)
    from_below, from_above = readers(odd, pair_ref, 0, chip_ref, 0, rows)
    sweep_slab(
        planes_of(one), held, two, one, medium_ref, scale_ref, sweep_steps[1],
        lambda part, row: (from_below(2 * (part // 3), row), from_below(2 * (part // 3) + 1, row)),
        lambda c, row: from_above(WHERE_YZ[c], row),
        first_scale, planes, rows, lane,
    )


def second_kernel(
    medium_ref, scale_ref, one, two, pair_ref, chip_ref, other_ref, three, extra_ref, held, delta_low, delta_high, delta_two,
):
    planes, rows, width = medium_ref.shape[1:]
    lane = lane_of(width)
    odd, first_scale, last_scale = parity_and_ends()
    for ref in (three, delta_low, delta_high):
        clear_after(ref)
    clear_after(delta_two, (0, 3))
    clear_before(held)
    first_part = even_group()

    def medium_next(above, part, row):
        pair = pair_ref[message_rows(4 + part, row, rows), :]
        chip, other = chip_ref[message_rows(4, row, rows), :], other_ref[pl.ds(row, ROWS), :]
        chip = jnp.where(first_part, chip, other) if part == 0 else jnp.where(first_part, other, chip)
        return jnp.where(odd, chip, pair) if above else jnp.where(odd, pair, chip)

    for row in chunks(rows):
        sums = edge_sums(lambda c, s: rows_at(one, (c, planes - 1), row, s), lane)
        scale = (sweep_steps[1] * last_scale) / (4.0 + medium_next(True, 0, row))
        for k, c in enumerate((1, 2, 4, 5)):
            put(delta_high, (c,), row, scale * sums[k])
        scale = sweep_steps[1] / (4.0 + medium_next(False, 0, row))
        for part in (0, 3):
            ey, ez = rows_at(one, (part + 1, 0), row), rows_at(one, (part + 2, 0), row)
            put(delta_low, (part + 1,), row, scale * ey)
            put(delta_low, (part + 2,), row, scale * ez)
            put(delta_low, (part,), row, scale * ((behind(ez, lane) - ez) + (rows_at(one, (part + 1, 0), row, -1) - ey)))

    none = [0.0] * 6
    for row in chunks(rows):
        values = curl(lambda c, s: rows_at(delta_low, (c,), row, s), lambda c: rows_at(two, (c, 0), row), lane)
        for c in range(6):
            put(held, (c, 0), row, values[c])
    for row in chunks(rows):
        before = {1: -rows_at(delta_low, (2,), row), 2: rows_at(delta_low, (1,), row),
                  4: -rows_at(delta_low, (5,), row), 5: rows_at(delta_low, (4,), row)}
        image = curl_back(lambda c, s: rows_at(held, (c, 0), row, s), lambda c: before[c], lane)
        real, imag = medium_next(False, 0, row), medium_next(False, 1, row)
        new = updated(
            [rows_at(delta_low, (c,), row) for c in range(6)], image, none, 0.0, real, imag, sweep_steps[2] / (4.0 + real)
        )
        for c in range(6):
            put(delta_two, (c,), row, new[c])
    for row in chunks(rows):
        sums = edge_sums(lambda c, s: rows_at(delta_two, (c,), row, s), lane)
        for k in range(4):
            extra_ref[k, pl.ds(row, ROWS), :] = sums[k]
    for row in chunks(rows):
        for part in (0, 3):
            ey, ez = rows_at(delta_high, (part + 1,), row), rows_at(delta_high, (part + 2,), row)
            put(held, (part, 1), row, (rows_at(delta_high, (part + 2,), row, 1) - ez) - (ahead(ey, lane) - ey))
    for row in chunks(rows):
        here = pl.ds(row, ROWS)
        sums = edge_sums(lambda c, s: rows_at(two, (c, planes - 1), row, s), lane)
        real, imag = medium_next(True, 0, row), medium_next(True, 1, row)
        scale = (sweep_steps[2] * last_scale) / (4.0 + real)
        center, image = {}, {}
        for part in (0, 3):
            ey, ez = rows_at(delta_high, (part + 1,), row), rows_at(delta_high, (part + 2,), row)
            hx = rows_at(held, (part, 1), row)
            k = 2 * (part // 3)
            center[part + 1], center[part + 2] = ey, ez
            image[part + 1] = 2.0 * ey - sums[k] - (behind(hx, lane) - hx)
            image[part + 2] = (rows_at(held, (part, 1), row, -1) - hx) - sums[k + 1] + 2.0 * ez
        for k, c in enumerate((1, 2)):
            extra_ref[4 + k, here, :] = center[c] - scale * (image[c] + real * center[c] - imag * center[c + 3])
            extra_ref[6 + k, here, :] = center[c + 3] - scale * (
                image[c + 3] + real * center[c + 3] + imag * center[c]
            )

    def low(part, row):
        sums = edge_sums(lambda c, s: rows_at(delta_low, (c,), row, s), lane)
        return sums[2 * (part // 3)], sums[2 * (part // 3) + 1]

    sweep_slab(
        planes_of(two), held, three, one, medium_ref, scale_ref, sweep_steps[2], low,
        lambda c, row: rows_at(delta_high, (c,), row), first_scale, planes, rows, lane,
    )


def last_kernel(
    base_ref, medium_ref, saved_ref, scale_ref, owner_ref, edge_ref, pair_ref, chip_ref, two, extra_ref,
    send_ref, stay_ref, ends, above, three, held, moment, window,
):
    planes, rows, width = medium_ref.shape[1:]
    lane = lane_of(width)
    odd, first_scale, _ = parity_and_ends()
    clear_after(ends)
    clear_before(above, (0, 2))
    clear_before(held)
    clear_after(moment, (0, 2))
    last = planes - 1

    from_below, from_above = readers(odd, pair_ref, 6, chip_ref, 0, rows)
    for row in chunks(rows):
        for k in range(4):
            put(above, (k,), row, from_above(k, row))
    for row in chunks(rows):
        here = pl.ds(row, ROWS)
        low_scale = (first_scale * sweep_steps[2]) * scale_ref[0, here, :]
        high_scale = sweep_steps[2] * scale_ref[last, here, :]
        for part in (0, 3):
            k = 2 * (part // 3)
            put(ends, (part, 0), row, rows_at(two, (part, 0), row))
            put(ends, (part + 1, 0), row, rows_at(two, (part + 1, 0), row) + low_scale * from_below(k, row))
            put(ends, (part + 2, 0), row, rows_at(two, (part + 2, 0), row) + low_scale * from_below(k + 1, row))
            ey, ez = rows_at(above, (k,), row), rows_at(above, (k + 1,), row)
            turn = (behind(ez, lane) - ez) + (rows_at(above, (k,), row, -1) - ey)
            put(ends, (part, 1), row, rows_at(two, (part, last), row) + high_scale * turn)
            put(ends, (part + 1, 1), row, rows_at(two, (part + 1, last), row) + high_scale * ey)
            put(ends, (part + 2, 1), row, rows_at(two, (part + 2, last), row) + high_scale * ez)

    def state(c, i, row, shift=0):
        if i == 0:
            return rows_at(ends, (c, 0), row, shift)
        if i == last:
            return rows_at(ends, (c, 1), row, shift)
        return rows_at(two, (c, i), row, shift)

    below_two, above_two = readers(odd, pair_ref, 10, chip_ref, 4, rows)

    def low(part, row):
        k = 2 * (part // 3)
        here = pl.ds(row, ROWS)
        return below_two(k, row) + extra_ref[k, here, :], below_two(k + 1, row) + extra_ref[k + 1, here, :]

    sweep_slab(
        state, held, three, base_ref, medium_ref, scale_ref, sweep_steps[3], low,
        lambda c, row: above_two(WHERE_YZ[c], row) + extra_ref[4 + WHERE_YZ[c], pl.ds(row, ROWS), :],
        first_scale, planes, rows, lane,
    )
    for i in range(planes):
        moments(saved_ref, three, moment, i, rows, lane)

    def moment_rows(c, i, row, shift=0):
        return rows_at(moment, (c, i), row, shift)

    for row in chunks(rows):
        here = pl.ds(row, ROWS)
        sums = [0.0] * (2 * REACH + 2)

        def add(value, offset, low):
            for k in range(2 * REACH + 1):
                slot = k + low
                sums[slot] = sums[slot] + jnp.where(offset == float(slot - REACH - 1), value, 0.0)

        def side(i):
            return moment_rows(1, i, row) + (moment_rows(2, i, row) + moment_rows(2, i, row, 1))

        lower = side(0)
        add(lower, edge_ref[here, :], 0)
        for i in range(planes):
            cell = moment_rows(0, i, row) + moment_rows(0, i, row, 1) + lower
            if i + 1 < planes:
                lower = side(i + 1)
                cell = cell + lower
            add(cell, owner_ref[i, here, :], 1)
        for k in range(2 * REACH + 2):
            window[k, here, :] = sums[k]
    for k in range(2 * REACH + 2):
        both = 0.25 * (window[k, pl.ds(0, rows // 2, stride=2), :] + window[k, pl.ds(1, rows // 2, stride=2), :])
        if k % 2 == 0:
            send_ref[k // 2] = both
        else:
            stay_ref[k // 2] = both


def vmem():
    return pl.BlockSpec(memory_space=pltpu.VMEM)


def call(kernel, out_shape, scratch, arguments, in_specs=None, limit=24 << 20, flops=1 << 20):
    return pl.pallas_call(
        kernel,
        out_shape=[jax.ShapeDtypeStruct(s, jnp.float32) for s in out_shape],
        in_specs=in_specs or [vmem()] * len(arguments),
        out_specs=[vmem()] * len(out_shape),
        scratch_shapes=[s if not isinstance(s, tuple) else pltpu.VMEM(s, jnp.float32) for s in scratch],
        compiler_params=pltpu.CompilerParams(vmem_limit_bytes=limit),
        cost_estimate=pl.CostEstimate(flops=flops, bytes_accessed=1 << 20, transcendentals=0),
    )(*arguments)


def core_swap(value):
    size = lax.axis_size("space")
    return lax.ppermute(value, "space", [(i, i ^ 1) for i in range(size)])


def chip_swap(value):
    size = lax.axis_size("space")
    pairs = []
    for i in range(1, size - 1, 2):
        pairs += [(i, i + 1), (i + 1, i)]
    return lax.ppermute(value, "space", pairs)


def sum_over_groups(value):
    size = lax.axis_size("src")
    if size & (size - 1):
        return lax.psum(value, "src")
    step = 1
    while step < size:
        value = value + lax.ppermute(value, "src", [(i, i ^ step) for i in range(size)])
        step *= 2
    return value


def gather_owned(send, stay):
    size = lax.axis_size("space")
    index = lax.axis_index("space")
    odd = lax.rem(index, 2) == 1
    other = core_swap(send)
    below = stay[0] + jnp.where(odd, other[1], other[0])
    here = stay[1] + jnp.where(odd, other[2], other[1])
    above = stay[2] + jnp.where(odd, 0.0, other[2])
    chip = index // 2
    upward = lax.rem(chip, 2) == 0
    chips = size // 2
    inner, outer = [], []
    for c in range(chips):
        for core in range(2):
            if c ^ 1 < chips:
                inner.append((2 * c + core, 2 * (c ^ 1) + core))
            partner = ((c + 1) ^ 1) - 1
            if 0 <= partner < chips:
                outer.append((2 * c + core, 2 * partner + core))
    from_inner = lax.ppermute(jnp.where(upward, above, below), "space", inner)
    from_outer = lax.ppermute(jnp.where(upward, below, above), "space", outer)
    from_far = lax.ppermute(other[0], "space", [(i, i - 4) for i in range(5, size, 2)])
    return here + from_inner + from_outer + from_far


def transposed_smooth(summed, rough):
    rows_in = summed.shape[-2]
    depth_in = summed.shape[-1]
    total = jnp.zeros_like(summed)
    for vertical in range(3):
        for lateral in range(3):
            product = rough[vertical * 3 + lateral] * summed
            padded = jnp.pad(product, ((0, 0), (1, 1), (1, 1)))
            total = (
                total
                + padded[
                    :, 2 - vertical : 2 - vertical + rows_in, 2 - lateral : 2 - lateral + depth_in
                ]
            )
    return total


def slab(adjoint_source, forward_field, medium, plane_map, depth, rough):
    planes, rows, width = medium.shape[1:]
    index = lax.axis_index("space")
    size = lax.axis_size("space") + REACH
    plane = (rows + 2 * PAD, width)
    state = (6, planes) + plane
    held = (6, planes + 1) + plane
    scale = (planes, rows, width)
    hbm = pl.BlockSpec(memory_space=pltpu.HBM)
    columns = pltpu.VMEM((planes, rows), jnp.int32)
    given = (adjoint_source, medium, depth, plane_map)
    chip, medium, scales, own, meta = call(
        start_kernel,
        [(5 * rows + PAD, width), medium.shape, scale, state, (PAD, width)],
        [(6, planes, rows, width), columns, columns, pltpu.SemaphoreType.DMA((2 * planes + 2,))],
        tuple(pltpu.with_memory_space_constraint(a, pltpu.HBM) for a in given),
        in_specs=[hbm] * 4,
    )
    chip = chip_swap(chip)
    chip_one, pair = call(
        follow_kernel, [(8 * rows, width), (14 * rows + PAD, width)], [state, state, held], (medium, scales, own, meta)
    )
    chip_one = chip_swap(chip_one)
    pair = core_swap(pair)

    here = index.astype(jnp.float32)
    levels = depth[0].astype(jnp.float32)
    owners = plane_map.astype(jnp.float32)
    position = lax.broadcasted_iota(jnp.int32, (planes, rows, width), 2).astype(jnp.float32)
    outside = float(size)
    owner = jnp.where(position < levels[:, :, None], (owners - here)[:, :, None], outside)
    below = jnp.where(lax.rem(index, 2) == 1, pair[14 * rows :], chip[5 * rows :])
    edge = jnp.where(position[0] < below[0, :rows, None], (below[1, :rows] - here)[:, None], outside)
    groups = lax.axis_size("src")
    other = lax.ppermute(chip[4 * rows : 5 * rows], "src", [(i, i ^ 1) for i in range(groups)])
    (first,) = call(early_kernel, [state], [held], (medium, scales, own, pair, chip))
    second, extra = call(
        second_kernel,
        [state, (8, rows, width)],
        [held, (6,) + plane, (6,) + plane, (6,) + plane],
        (medium, scales, own, first, pair, chip, other),
    )
    send, stay = call(
        last_kernel,
        [(REACH + 1, rows // 2, width), (REACH + 1, rows // 2, width)],
        [(6, 2) + plane, (4,) + plane, state, held, (3, planes) + plane, (2 * REACH + 2, rows, width)],
        (own, medium, forward_field, scales, owner, edge, pair, chip_one, second, extra),
    )
    total = sum_over_groups(gather_owned(send, stay))
    return transposed_smooth(total[None], rough)


def solution(mesh):
    in_specs = (
        P("src", None, "space", None, None),
        P("src", None, "space", None, None),
        P(None, "space", None, None),
        P("space", None),
        P("src", "space", None),
        P(None, "space", None, None),
    )
    out_specs = P("space", None, None)
    return jax.shard_map(slab, mesh=mesh, in_specs=in_specs, out_specs=out_specs, check_vma=False)
```
